8 devices in a mesh: dp: 1 (over z), tp: 2 (over y), dm: 4 (over x, core).
Axes of the slice: x: 2, y: 2, z: 1, core: 2. Of those that a mesh axis runs over, the one named last changes fastest.
Arguments:
- tokens: bfloat16 [8192, 2304], P('dp', 'dm')
- positions: int32 [2, 4096], P('dp')
- norm_pre_attn: bfloat16 [2304], P('dm')
- w_query: bfloat16 [2304, 8, 256], P('dm', 'tp')
- w_key: bfloat16 [2304, 4, 256], P('dm', 'tp')
- w_value: bfloat16 [2304, 4, 256], P('dm', 'tp')
- w_out: bfloat16 [8, 256, 2304], P('tp', None, 'dm')
- norm_post_attn: bfloat16 [2304], P('dm')
- norm_pre_ffw: bfloat16 [2304], P('dm')
- w_gate: bfloat16 [2304, 9216], P('dm', 'tp')
- w_up: bfloat16 [2304, 9216], P('dm', 'tp')
- w_down: bfloat16 [9216, 2304], P('tp', 'dm')
- norm_post_ffw: bfloat16 [2304], P('dm')
Outputs:
- output 1: bfloat16 [8192, 2304], P('dp', 'dm')
- output 2: bfloat16 [8192, 4, 256], P('dp', 'tp')
- output 3: bfloat16 [8192, 4, 256], P('dp', 'tp')
All inputs are finite; a program needn't handle non-finite values.
Results may differ from the reference program's by a relative error of at most 0.02.
Values are sent between devices in bfloat16 or wider.
A program may use at most 1 GiB of HBM per device.

```python
import jax
import jax.numpy as jnp
from jax import lax

MODEL_DIM = 2304
NUM_HEADS = 8
KV_HEADS = 4
HEAD_DIM = 256
FFW_DIM = 9216
NUM_SEQS = 2
SEQ_LEN = 4096
WINDOW_LEN = 4096
NUM_TOKENS = NUM_SEQS * SEQ_LEN
GROUP_SIZE = NUM_HEADS // KV_HEADS
QUERY_BLOCK = min(SEQ_LEN, 128)
NORM_EPS = 1e-6
SOFT_CAP = 50.0
ROPE_BASE = 10000.0
SCORE_SCALE = (MODEL_DIM / NUM_HEADS) ** -0.5


def draw_normal(key, shape, scale):
    return (jax.random.normal(key, shape, jnp.float32) * scale).astype(jnp.bfloat16)


def draw_gain(key, gain_ramp):
    return (jax.random.normal(key, (MODEL_DIM,), jnp.float32) * 0.3 + gain_ramp).astype(jnp.bfloat16)


def setup_inputs(seed: int = 0, part: int = 0) -> dict:
    shared_key, part_root = jax.random.split(jax.random.key(seed))
    part_key = jax.random.fold_in(part_root, part)
    tok_key, start_key, step_key = jax.random.split(part_key, 3)
    weight_keys = jax.random.split(shared_key, 11)
    seq_start = jax.random.randint(start_key, (NUM_SEQS, 1), 0, SEQ_LEN)
    pos_steps = jax.random.randint(step_key, (NUM_SEQS, SEQ_LEN), 1, 4)
    positions = seq_start + jnp.cumsum(pos_steps, axis=1) - pos_steps[:, :1]
    col_pos = jnp.arange(MODEL_DIM, dtype=jnp.float32) / (MODEL_DIM - 1)
    width_ramp = 2.0 ** (3.0 * col_pos - 1.5)
    out_ramp = 2.0 ** (2.0 * col_pos - 1.0)
    gain_ramp = col_pos - 0.5
    model_scale = MODEL_DIM ** -0.5
    tokens = jax.random.normal(tok_key, (NUM_TOKENS, MODEL_DIM), jnp.float32) * width_ramp[None, :]
    w_out = jax.random.normal(weight_keys[4], (NUM_HEADS, HEAD_DIM, MODEL_DIM), jnp.float32) * ((NUM_HEADS * HEAD_DIM) ** -0.5) * out_ramp
    w_down = jax.random.normal(weight_keys[9], (FFW_DIM, MODEL_DIM), jnp.float32) * (FFW_DIM ** -0.5) * out_ramp[None, :]
    return {
        'tokens': tokens.astype(jnp.bfloat16),
        'positions': positions.astype(jnp.int32),
        'norm_pre_attn': draw_gain(weight_keys[0], gain_ramp),
        'w_query': draw_normal(weight_keys[1], (MODEL_DIM, NUM_HEADS, HEAD_DIM), model_scale),
        'w_key': draw_normal(weight_keys[2], (MODEL_DIM, KV_HEADS, HEAD_DIM), model_scale),
        'w_value': draw_normal(weight_keys[3], (MODEL_DIM, KV_HEADS, HEAD_DIM), model_scale),
        'w_out': w_out.astype(jnp.bfloat16),
        'norm_post_attn': draw_gain(weight_keys[5], gain_ramp),
        'norm_pre_ffw': draw_gain(weight_keys[6], gain_ramp),
        'w_gate': draw_normal(weight_keys[7], (MODEL_DIM, FFW_DIM), model_scale),
        'w_up': draw_normal(weight_keys[8], (MODEL_DIM, FFW_DIM), model_scale),
        'w_down': w_down.astype(jnp.bfloat16),
        'norm_post_ffw': draw_gain(weight_keys[10], gain_ramp),
    }


def rms_scale(values, gain_vec):
    vals32 = values.astype(jnp.float32)
    mean_sq = jnp.mean(vals32 * vals32, axis=-1, keepdims=True)
    return vals32 * lax.rsqrt(mean_sq + NORM_EPS) * (1.0 + gain_vec.astype(jnp.float32))


def rotary_tables(positions):
    half_dim = HEAD_DIM // 2
    inv_freq = ROPE_BASE ** (-2.0 * jnp.arange(half_dim, dtype=jnp.float32) / HEAD_DIM)
    angles = positions.reshape(-1).astype(jnp.float32)[:, None] * inv_freq[None, :]
    return jnp.cos(angles)[:, None, :], jnp.sin(angles)[:, None, :]


def apply_rotary(head_vals, cos_tab, sin_tab):
    half_dim = head_vals.shape[-1] // 2
    lower_half = head_vals[..., :half_dim].astype(jnp.float32)
    upper_half = head_vals[..., half_dim:].astype(jnp.float32)
    rotated = jnp.concatenate([lower_half * cos_tab - upper_half * sin_tab, upper_half * cos_tab + lower_half * sin_tab], axis=-1)
    return rotated.astype(jnp.bfloat16)


def attend(query_rows, key_rows, value_rows, positions):
    keys32 = key_rows.astype(jnp.float32)
    values32 = value_rows.astype(jnp.float32)
    key_index = jnp.arange(SEQ_LEN)

    def one_block(block_index):
        row_start = block_index * QUERY_BLOCK
        q_blk = lax.dynamic_slice_in_dim(query_rows, row_start, QUERY_BLOCK, axis=1).astype(jnp.float32)
        q_pos = lax.dynamic_slice_in_dim(positions, row_start, QUERY_BLOCK, axis=1)
        scores = jnp.einsum('bqkgd,bskd->bkgqs', q_blk, keys32) * SCORE_SCALE
        scores = SOFT_CAP * jnp.tanh(scores / SOFT_CAP)
        q_index = row_start + jnp.arange(QUERY_BLOCK)
        allowed = (key_index[None, :] <= q_index[:, None])[None] & (q_pos[:, :, None] - positions[:, None, :] < WINDOW_LEN)
        scores = jnp.where(allowed[:, None, None], scores, -1e30)
        attn_probs = jax.nn.softmax(scores, axis=-1).astype(jnp.bfloat16).astype(jnp.float32)
        return jnp.einsum('bkgqs,bskd->bqkgd', attn_probs, values32).astype(jnp.bfloat16)

    blocks = lax.map(one_block, jnp.arange(SEQ_LEN // QUERY_BLOCK))
    return jnp.moveaxis(blocks, 0, 1).reshape(NUM_TOKENS, NUM_HEADS * HEAD_DIM)


def reference(tokens, positions, norm_pre_attn, w_query, w_key, w_value, w_out, norm_post_attn, norm_pre_ffw, w_gate, w_up, w_down, norm_post_ffw):
    cos_tab, sin_tab = rotary_tables(positions)
    normed = rms_scale(tokens, norm_pre_attn).astype(jnp.bfloat16)
    query_rows = jnp.dot(normed, w_query.reshape(MODEL_DIM, NUM_HEADS * HEAD_DIM), preferred_element_type=jnp.float32).astype(jnp.bfloat16)
    key_rows = jnp.dot(normed, w_key.reshape(MODEL_DIM, KV_HEADS * HEAD_DIM), preferred_element_type=jnp.float32).astype(jnp.bfloat16)
    value_rows = jnp.dot(normed, w_value.reshape(MODEL_DIM, KV_HEADS * HEAD_DIM), preferred_element_type=jnp.float32).astype(jnp.bfloat16)
    query_rows = apply_rotary(query_rows.reshape(NUM_TOKENS, NUM_HEADS, HEAD_DIM), cos_tab, sin_tab)
    key_rows = apply_rotary(key_rows.reshape(NUM_TOKENS, KV_HEADS, HEAD_DIM), cos_tab, sin_tab)
    value_rows = value_rows.reshape(NUM_TOKENS, KV_HEADS, HEAD_DIM)
    attn_rows = attend(query_rows.reshape(NUM_SEQS, SEQ_LEN, KV_HEADS, GROUP_SIZE, HEAD_DIM), key_rows.reshape(NUM_SEQS, SEQ_LEN, KV_HEADS, HEAD_DIM), value_rows.reshape(NUM_SEQS, SEQ_LEN, KV_HEADS, HEAD_DIM), positions)
    attn_out = jnp.dot(attn_rows, w_out.reshape(NUM_HEADS * HEAD_DIM, MODEL_DIM), preferred_element_type=jnp.float32).astype(jnp.bfloat16)
    hidden = (tokens.astype(jnp.float32) + rms_scale(attn_out, norm_post_attn)).astype(jnp.bfloat16)
    ffw_in = rms_scale(hidden, norm_pre_ffw).astype(jnp.bfloat16)
    gate_proj = jnp.dot(ffw_in, w_gate, preferred_element_type=jnp.float32).astype(jnp.bfloat16)
    up_proj = jnp.dot(ffw_in, w_up, preferred_element_type=jnp.float32).astype(jnp.bfloat16)
    gated_act = (jax.nn.gelu(gate_proj.astype(jnp.float32), approximate=True) * up_proj.astype(jnp.float32)).astype(jnp.bfloat16)
    down_proj = jnp.dot(gated_act, w_down, preferred_element_type=jnp.float32).astype(jnp.bfloat16)
    tokens_out = (hidden.astype(jnp.float32) + rms_scale(down_proj, norm_post_ffw)).astype(jnp.bfloat16)
    return (tokens_out, key_rows, value_rows)
```

```python
import functools

import jax
import jax.numpy as jnp
from jax import lax
from jax.experimental import pallas as pl
from jax.experimental.pallas import tpu as pltpu
from jax.sharding import PartitionSpec as P


NORM_EPS = 1e-6
SOFT_CAP = 50.0
ROPE_BASE = 10000.0
WINDOW_LEN = 4096
LOG2E = 1.4426950408889634
BF = jnp.bfloat16
F32 = jnp.float32
VM = 56 * 1024 * 1024
CH = 128
MT = 256
ANY = pl.BlockSpec(memory_space=pl.ANY)


def dot(a, b):
    return jnp.dot(a, b, preferred_element_type=F32)


def dot_nt(a, b):
    return lax.dot_general(a, b, (((1,), (1,)), ((), ())), preferred_element_type=F32)


def whole(*shape):
    return pl.BlockSpec(shape, lambda *_: (0,) * len(shape))


def inv_rms(blocks, width):
    sq = sum(jnp.sum(jnp.square(b.astype(F32)), axis=0, keepdims=True) for b in blocks)
    return lax.rsqrt(sq / width + NORM_EPS)


def part_of(ref, j, size):
    return ref.at[j * size:(j + 1) * size, :]


def call(kernel, grid, in_specs, out_specs, out_shape, scratch=(), prefetch=1, flops=0, nbytes=0, aliases=None):
    return pl.pallas_call(
        kernel,
        out_shape=out_shape,
        grid_spec=pltpu.PrefetchScalarGridSpec(num_scalar_prefetch=prefetch, grid=grid, in_specs=in_specs, out_specs=out_specs, scratch_shapes=list(scratch)),
        cost_estimate=pl.CostEstimate(flops=flops, bytes_accessed=nbytes, transcendentals=0),
        compiler_params=pltpu.CompilerParams(vmem_limit_bytes=VM),
        input_output_aliases=aliases or {},
    )


def norm_kernel(s_ref, own, own_c, rx, rxc, ry, ryc, g_ref, a_ref, *, width, per_half):
    w4 = own.shape[0]
    mine = (pl.program_id(0) // per_half) == s_ref[1]
    blocks = [own[...], own_c[...], jnp.where(mine, rx[...], ry[...]), jnp.where(mine, rxc[...], ryc[...])]
    r = inv_rms(blocks, width)
    for j, b in enumerate(blocks):
        part_of(a_ref, j, w4)[...] = (b.astype(F32) * r * part_of(g_ref, j, w4)[:, 0:1]).astype(BF)


def qkv_kernel(s_ref, a_ref, w0, w1, w2, w3, cos_ref, sin_ref, *rest, hd, aliased):
    if aliased:
        rest = rest[2:]
    qv_ref, kv_ref, w_t, w_all = rest
    w4 = w0.shape[0]

    @pl.when(pl.program_id(0) == 0)
    def _():
        for j, w in enumerate((w0, w1, w2, w3)):
            part_of(w_all, j, w4)[...] = w[...]
        for r in range(0, w_all.shape[0], MT):
            w_t[:, r:r + MT] = w_all[r:r + MT, :].T

    qkv = dot(w_t[...], a_ref[...]).astype(BF).astype(F32)
    ct, st = cos_ref[...], sin_ref[...]
    hh = hd // 2

    def rot(base):
        u1, u2 = qkv[base:base + hh], qkv[base + hh:base + hd]
        return u1 * ct - u2 * st, u2 * ct + u1 * st

    for g in range(2):
        lo, hi = rot(g * hd)
        qv_ref[g * hd:g * hd + hh, :] = lo.astype(BF)
        qv_ref[g * hd + hh:(g + 1) * hd, :] = hi.astype(BF)
    v = qkv[3 * hd:]
    qv_ref[2 * hd:, :] = v.astype(BF)
    klo, khi = rot(2 * hd)
    kv_ref[:, :hh] = klo.T.astype(BF)
    kv_ref[:, hh:hd] = khi.T.astype(BF)
    kv_ref[:, hd:] = v.T.astype(BF)


def attn_kernel(lo_ref, full_ref, q_ref, k_ref, v_ref, pq_ref, pk_ref, o_ref, acc_ref, m_ref, l_ref, *, bq, bk, q_block0, scale):
    qb = q_block0 + pl.program_id(0)
    hd = k_ref.shape[1]
    groups = q_ref.shape[0] // hd
    lo, full = lo_ref[qb], full_ref[qb]
    diag = (qb * bq) // bk
    last = ((qb + 1) * bq + bk - 1) // bk
    m_ref[...] = jnp.full_like(m_ref, -1e30)
    l_ref[...] = jnp.zeros_like(l_ref)
    acc_ref[...] = jnp.zeros_like(acc_ref)

    def step(j, masked):
        rows = pl.ds(pl.multiple_of(j * bk, bk), bk)
        kb = k_ref[rows, :]
        vb = v_ref[:, rows]
        if masked:
            dif = pq_ref[...] - pk_ref[rows, :]
            ok = (dif >= 0) & (dif < WINDOW_LEN)
        for g in range(groups):
            s = dot(kb, q_ref[g * hd:(g + 1) * hd, :])
            s = jnp.tanh(s * (scale / SOFT_CAP)) * (SOFT_CAP * LOG2E)
            if masked:
                s = jnp.where(ok, s, -1e30)
            m_old = m_ref[g]
            m_new = jnp.maximum(m_old, jnp.max(s, axis=0, keepdims=True))
            p = jnp.exp2(s - m_new)
            alpha = jnp.exp2(m_old - m_new)
            l_ref[g] = l_ref[g] * alpha + jnp.sum(p, axis=0, keepdims=True)
            m_ref[g] = m_new
            acc_ref[g] = acc_ref[g] * alpha + dot(vb, p.astype(BF))

    mid = jnp.maximum(jnp.minimum(full, diag), lo)

    def masked_step(j, _):
        step(j, True)
        return 0

    def full_step(j, _):
        step(j, False)
        return 0

    lax.fori_loop(lo, mid, masked_step, 0)
    lax.fori_loop(mid, diag, full_step, 0)
    lax.fori_loop(jnp.maximum(diag, mid), last, masked_step, 0)
    for g in range(groups):
        o_ref[g * hd:(g + 1) * hd, :] = (acc_ref[g] / l_ref[g]).astype(BF)


def norm_to_m(m_ref, blocks, r, g_ref, col, mt_ref):
    w4 = blocks[0].shape[0]
    for j, b in enumerate(blocks):
        part_of(mt_ref, j, w4)[...] = (b * r * part_of(g_ref, j, w4)[:, col:col + 1]).astype(BF)
    for i in range(0, mt_ref.shape[0], MT):
        m_ref[:, i:i + MT] = mt_ref[i:i + MT, :].T


def proj_kernel(s_ref, o_own, o_c, o_y, o_yc, b0, b0c, b1, b1c, b2, b2c, b3, b3c, x0, x1, x2, x3, g_ref, h_ref, m_ref, o_all, mt_ref, *, width):
    c = s_ref[2]
    gw = o_own.shape[0]
    first = c == 0
    o_all[0:gw, :] = jnp.where(first, o_own[...], o_c[...])
    o_all[gw:2 * gw, :] = jnp.where(first, o_c[...], o_own[...])
    o_all[2 * gw:3 * gw, :] = jnp.where(first, o_y[...], o_yc[...])
    o_all[3 * gw:, :] = jnp.where(first, o_yc[...], o_y[...])
    w4 = x0.shape[0]
    heads = b0.shape[0]
    o = o_all[...]
    att = []
    for wy, wo in ((b0, b2), (b0c, b2c), (b1, b3), (b1c, b3c)):
        w = jnp.concatenate([wy[h] for h in range(heads)] + [wo[h] for h in range(heads)], axis=1)
        att.append(dot(w, o).astype(BF).astype(F32))
    r = inv_rms(att, width)
    hs = []
    for j, (t, xr) in enumerate(zip(att, (x0, x1, x2, x3))):
        h = (xr[...].astype(F32) + t * r * part_of(g_ref, j, w4)[:, 1:2]).astype(BF)
        part_of(h_ref, j, w4)[...] = h
        hs.append(h.astype(F32))
    norm_to_m(m_ref, hs, inv_rms(hs, width), g_ref, 2, mt_ref)


def renorm_kernel(s_ref, h_ref, g_ref, m_ref, mt_ref, *, width):
    w4 = h_ref.shape[0] // 4
    hs = [part_of(h_ref, j, w4)[...].astype(F32) for j in (2, 3, 0, 1)]
    norm_to_m(m_ref, hs, inv_rms(hs, width), g_ref, 2, mt_ref)


def gate_up_kernel(s_ref, ma, mb, g0, g1, g2, g3, u0, u1, u2, u3, z_ref):
    n = z_ref.shape[1]
    w = jnp.concatenate([jnp.concatenate([g[...] for g in (g0, g1, g2, g3)], axis=0), jnp.concatenate([u[...] for u in (u0, u1, u2, u3)], axis=0)], axis=1)
    base = 0
    for m in (ma, mb):
        for r in range(0, m.shape[0], MT):
            t = dot(m[r:r + MT, :], w)
            g, u = t[:, :n].astype(BF).astype(F32), t[:, n:].astype(BF).astype(F32)
            z_ref[base:base + MT, :] = (jax.nn.gelu(g, approximate=True) * u).astype(BF)
            base += MT


def down_y_kernel(s_ref, zw, zf, d0, d1, d2, d3, acc_ref, d_ref):
    w4 = d0.shape[0]
    n = zw.shape[0]

    @pl.when(pl.program_id(0) == 0)
    def _():
        for j, dd in enumerate((d0, d1, d2, d3)):
            part_of(d_ref, j, w4)[...] = dd[...]

    z = jnp.concatenate([zw[...], zf[...]], axis=0)
    for j in range(4):
        t = dot_nt(d_ref[j * w4:(j + 1) * w4, :], z)
        for q in range(n // CH):
            acc_ref[q, j * w4:(j + 1) * w4, :CH] = t[:, q * CH:(q + 1) * CH]
            acc_ref[q, j * w4:(j + 1) * w4, CH:] = t[:, n + q * CH:n + (q + 1) * CH]


def tail_kernel(part, zw, zf, d0, d1, d2, d3, hw0, hw1, hf0, hf1, g_ref, out,
                d_ref, z_ref, p_ref, lo_ref, hi_ref, rec_ref, h_ref, sqs_ref, sqr_ref, sqo_ref,
                d_sem, z_sem, p_sem, h_sem, loc_sem, rs_s, rs_r, sq_s, sq_r, out_s, out_r, *, width, chunks):
    w4 = d0.shape[0]
    w2 = 2 * w4
    y = lax.axis_index('tp')
    dm = lax.axis_index('dm')
    x, c = dm // 2, lax.rem(dm, 2)
    px = {'dp': 0, 'tp': y, 'dm': (1 - x) * 2 + c}
    pc = {'dp': 0, 'tp': y, 'dm': x * 2 + 1 - c}
    py = {'dp': 0, 'tp': 1 - y, 'dm': dm}
    pyc = {'dp': 0, 'tp': 1 - y, 'dm': x * 2 + 1 - c}

    def local(src, dst, sem):
        return pltpu.make_async_copy(src, dst, sem)

    def remote(src, dst, s_sem, r_sem, dev):
        return pltpu.make_async_remote_copy(src_ref=src, dst_ref=dst, send_sem=s_sem, recv_sem=r_sem, device_id=dev, device_id_type=pl.DeviceIdType.MESH)

    d_cp = [local(dd, part_of(d_ref, j, w4), d_sem.at[j]) for j, dd in enumerate((d0, d1, d2, d3))]

    def z_cp(p):
        return [local(src.at[pl.ds(p * CH, CH), :], z_ref.at[p, i * CH:(i + 1) * CH, :], z_sem.at[p, i]) for i, src in enumerate((zw, zf))]

    def p_cp(p):
        return local(part.at[p], p_ref.at[lax.rem(p, 2)], p_sem.at[lax.rem(p, 2)])

    per = hw0.shape[1] // CH
    h_cp = []
    for q in range(chunks):
        k, l = q // per, (q % per) * CH
        h_cp.append(local((hw0, hw1)[k].at[0:w2, l:l + CH], h_ref.at[q, :, 0:CH], h_sem.at[q, 0]))
        h_cp.append(local((hf0, hf1)[k].at[w2:2 * w2, l:l + CH], h_ref.at[q, :, CH:2 * CH], h_sem.at[q, 1]))

    for cp in z_cp(0):
        cp.start()
    d_cp[2].start()
    p_cp(0).start()
    d_cp[3].start()
    d_cp[0].start()
    d_cp[1].start()
    for q in range(1, chunks):
        for cp in z_cp(q):
            cp.start()
    for cp in h_cp:
        cp.start()

    bar = pltpu.get_barrier_semaphore()
    for dev in (px, pc, py, pyc):
        pl.semaphore_signal(bar, inc=1, device_id=dev, device_id_type=pl.DeviceIdType.MESH)
    pl.semaphore_wait(bar, 4)

    def rs(p):
        return remote(hi_ref.at[p], rec_ref.at[p], rs_s.at[p], rs_r.at[p], px)

    def sq(p):
        return remote(sqs_ref.at[p], sqr_ref.at[p], sq_s.at[p], sq_r.at[p], px)

    def outs(p):
        k, l = p // per, lax.rem(p, per)
        res = []
        for i, pr in enumerate((x, 1 - x)):
            col = pl.multiple_of(((pr * 2 + k) * 4 + 2 * y + c) * (per * CH) + l * CH, CH)
            mine = rec_ref.at[p, 0:w4, i * CH:(i + 1) * CH]
            give = rec_ref.at[p, w4:w2, i * CH:(i + 1) * CH]
            dst = out.at[:, pl.ds(col, CH)]
            res.append((local(mine, dst, loc_sem.at[p, i]), remote(mine, dst, out_s.at[p, i, 0], out_r.at[p, i, 0], py),
                        remote(give, dst, out_s.at[p, i, 1], out_r.at[p, i, 1], pyc), remote(give, dst, out_s.at[p, i, 2], out_r.at[p, i, 2], pc)))
        return res

    def product(p, first=False):
        p_cp(p).wait()
        for cp in z_cp(p):
            cp.wait()
        if first:
            p_cp(1).start()
        else:
            @pl.when(p + 1 < chunks)
            def _():
                p_cp(p + 1).start()
        slot = lax.rem(p, 2)
        for j in (2, 3, 0, 1):
            if first:
                d_cp[j].wait()
            t = dot_nt(d_ref[j * w4:(j + 1) * w4, :], z_ref[p]) + p_ref[slot, j * w4:(j + 1) * w4, :]
            if j < 2:
                lo_ref[p, j * w4:(j + 1) * w4, :] = t
            else:
                t = t.astype(BF)
                hi_ref[p, (j - 2) * w4:(j - 1) * w4, :CH] = t[:, CH:]
                hi_ref[p, (j - 2) * w4:(j - 1) * w4, CH:] = t[:, :CH]
                if j == 3:
                    rs(p).start()

    def add(p):
        rs(p).wait_recv()
        t = (lo_ref[p] + rec_ref[p].astype(F32)).astype(BF)
        rec_ref[p] = t
        t = t.astype(F32)
        v = jnp.broadcast_to(jnp.sum(t * t, axis=0, keepdims=True), (8, 2 * CH))
        sqo_ref[...] = v
        sqs_ref[p, :, :CH] = v[:, CH:]
        sqs_ref[p, :, CH:] = v[:, :CH]
        sq(p).start()

    def finish(p, v):
        sq(p).wait_recv()
        r = lax.rsqrt((v + sqr_ref[p]) / width + NORM_EPS)[0:1]
        g = g_ref[...]
        g = jnp.concatenate([g] * (2 * CH // 128), axis=1)
        rec_ref[p] = (h_ref[p].astype(F32) + rec_ref[p].astype(F32) * r * g).astype(BF)
        for group in outs(p):
            for cp in group[1:] + group[:1]:
                cp.start()

    product(0, True)
    product(1)
    for cp in h_cp:
        cp.wait()

    def body(p, _):
        add(p)
        v = sqo_ref[...]
        product(p + 2)
        finish(p, v)
        return 0

    lax.fori_loop(0, chunks - 2, body, 0)
    for p in (chunks - 2, chunks - 1):
        add(p)
        finish(p, sqo_ref[...])

    def drain(p, _):
        rs(p).wait_send()
        sq(p).wait_send()
        for group in outs(p):
            group[0].wait()
            for cp in group[1:]:
                cp.wait()
        return 0

    lax.fori_loop(0, chunks, drain, 0)


def kv_out_kernel(s_ref, kv0, kv1, *rest):
    k_ref, v_ref = rest[-2:]
    hd = k_ref.shape[2]
    first = s_ref[2] == 0
    a, b = kv0[...], kv1[...]
    lo, hi = jnp.where(first, a, b), jnp.where(first, b, a)
    k_ref[...] = jnp.stack([lo[:, :hd], hi[:, :hd]], axis=1)
    v_ref[...] = jnp.stack([lo[:, hd:], hi[:, hd:]], axis=1)


def solution(mesh):
    tp_size, dm_size = mesh.shape['tp'], mesh.shape['dm']

    def flip(fy, fx, fc):
        return [(y * 4 + x * 2 + c, (y ^ fy) * 4 + (x ^ fx) * 2 + (c ^ fc)) for y in range(2) for x in range(2) for c in range(2)]

    PX, PY, PC, PXC, PYC = flip(0, 1, 0), flip(1, 0, 0), flip(0, 0, 1), flip(0, 1, 1), flip(1, 0, 1)

    def send(a, perm):
        return lax.ppermute(a, ('tp', 'dm'), perm)

    def layer(tokens, positions, n1, wq, wk, wv, wo, n2, n3, wg, wu, wd, n4):
        y = lax.axis_index('tp')
        d = lax.axis_index('dm')
        x, c = d // 2, d % 2
        xo, yo, co = 1 - x, 1 - y, 1 - c
        rows, w4 = tokens.shape
        D = w4 * dm_size
        S = positions.shape[1]
        hd = wq.shape[2]
        scale = (D / (wq.shape[1] * tp_size)) ** -0.5
        gw = 2 * hd
        half = S // 2
        quarter = half // 4
        F4 = wg.shape[1] // 2
        scal = jnp.stack([x, y, c]).astype(jnp.int32)

        def take(a, start, size, axis=0):
            return lax.dynamic_slice_in_dim(a, start, size, axis)

        xt = tokens.T

        gains = jnp.stack([n1, n2, n3, n4])
        gall = jnp.concatenate([gains, send(gains, PC), send(gains, PX), send(gains, PXC)], axis=1)
        gcol = (1.0 + gall.astype(F32)).T

        rx = [send(take(xt, xo * S + k * half + y * (half // 2), half // 2, 1), PX) for k in range(2)]
        own_c = send(take(xt, x * S, S, 1), PC)
        ry = [send(rx[k], PY) for k in range(2)]
        rxc = [send(rx[k], PC) for k in range(2)]
        ryc = [send(ry[k], PC) for k in range(2)]

        def group_cols(g):
            return jnp.concatenate([take(wq, 2 * g, 2, 1).reshape(w4, gw), take(wk, g, 1, 1).reshape(w4, hd), take(wv, g, 1, 1).reshape(w4, hd)], axis=1)

        wq_own, wq_oth = group_cols(c), group_cols(co)
        wqs = [wq_own, send(wq_oth, PC), send(wq_own, PX), send(wq_oth, PXC)]

        wot = jnp.transpose(wo, (0, 2, 1))
        B0 = wot
        B1 = send(B0, PX)
        B2 = send(B0, PY)
        B3 = send(B1, PY)
        Bs = []
        for b in (B0, B1, B2, B3):
            Bs += [b, send(b, PC)]

        def gather(own, oth):
            r1 = send(oth, PX)
            s0 = send(own, PY)
            s1 = send(r1, PY)
            ty = [own, send(own, PC), r1, send(r1, PC)]
            to = [s0, send(s0, PC), s1, send(s1, PC)]
            return ty, to

        def gu_half(xx):
            return jnp.concatenate([take(wg, xx * F4, F4, 1), take(wu, xx * F4, F4, 1)], axis=1)

        gu_y, gu_o = gather(gu_half(x), gu_half(xo))
        wdt = wd.T
        dn_y, dn_o = gather(take(wdt, x * F4, F4, 1), take(wdt, xo * F4, F4, 1))

        pos = take(positions, x, 1)[0]
        inv_freq = ROPE_BASE ** (-2.0 * jnp.arange(hd // 2, dtype=F32) / hd)
        ang = inv_freq[:, None] * pos.astype(F32)[None, :]
        cos_t, sin_t = jnp.cos(ang), jnp.sin(ang)

        tile = 512
        nt = half // tile
        per_half = nt // 2
        nb = S // tile
        a_sets = []
        for k in range(2):
            a_sets.append(call(
                functools.partial(norm_kernel, width=D, per_half=per_half), (nt,),
                [pl.BlockSpec((w4, tile), lambda i, s, k=k: (0, s[0] * nb + k * nt + i)), pl.BlockSpec((w4, tile), lambda i, s, k=k: (0, k * nt + i))]
                + [pl.BlockSpec((w4, tile), lambda i, s: (0, i % per_half))] * 4 + [whole(D, 4)],
                pl.BlockSpec((D, tile), lambda i, s: (0, i)), jax.ShapeDtypeStruct((D, half), BF),
                flops=100 * D * half)(scal, xt, own_c, rx[k], rxc[k], ry[k], ryc[k], gcol))
        qv = kv = None
        for k in range(2):
            ins = [a_sets[k], *wqs, cos_t, sin_t]
            specs = [pl.BlockSpec((D, tile), lambda i, s: (0, i))] + [whole(w4, 2 * gw)] * 4 + [pl.BlockSpec((hd // 2, tile), lambda i, s, k=k: (0, k * nt + i))] * 2
            aliases = None
            if k == 1:
                ins += [qv, kv]
                specs += [ANY, ANY]
                aliases = {8: 0, 9: 1}
            qv, kv = call(
                functools.partial(qkv_kernel, hd=hd, aliased=k == 1), (nt,), specs,
                [pl.BlockSpec((gw + hd, tile), lambda i, s, k=k: (0, k * nt + i)), pl.BlockSpec((tile, gw), lambda i, s, k=k: (k * nt + i, 0))],
                [jax.ShapeDtypeStruct((gw + hd, S), BF), jax.ShapeDtypeStruct((S, gw), BF)],
                [pltpu.VMEM((2 * gw, D), BF), pltpu.VMEM((D, 2 * gw), BF)],
                flops=2 * D * 2 * gw * half, aliases=aliases)(scal, *ins)

        bq = bk = 512
        first_q, last_q = pos[0::bq][:, None], pos[bq - 1::bq][:, None]
        first_k, last_k = pos[0::bk][None, :], pos[bk - 1::bk][None, :]
        lo_t = jnp.sum((first_q - last_k >= WINDOW_LEN).astype(jnp.int32), axis=1)
        full_t = jnp.sum((last_q - first_k >= WINDOW_LEN).astype(jnp.int32), axis=1)
        pos_row, pos_col = pos.reshape(1, S), pos.reshape(S, 1)
        h_own, m_own = [], []
        for k in range(2):
            q0 = k * half // bq
            kl = (k + 1) * half
            o = call(
                functools.partial(attn_kernel, bq=bq, bk=bk, q_block0=q0, scale=scale), (half // bq,),
                [
                    pl.BlockSpec((gw, bq), lambda i, *_, q0=q0: (0, q0 + i)),
                    pl.BlockSpec((kl, hd), lambda i, *_: (0, 0)),
                    pl.BlockSpec((hd, kl), lambda i, *_: (2, 0)),
                    pl.BlockSpec((1, bq), lambda i, *_, q0=q0: (0, q0 + i)),
                    pl.BlockSpec((kl, 1), lambda i, *_: (0, 0)),
                ],
                pl.BlockSpec((gw, bq), lambda i, *_: (0, i)),
                jax.ShapeDtypeStruct((gw, half), BF),
                [pltpu.VMEM((2, hd, bq), F32), pltpu.VMEM((2, 1, bq), F32), pltpu.VMEM((2, 1, bq), F32)],
                prefetch=2, flops=4 * hd * 2 * half * (k * half + half // 2))(lo_t, full_t, qv, kv, qv, pos_row, pos_col)
            mc = 2 * y + co
            my, myc = 2 * yo + c, 2 * yo + co
            o_c = send(take(o, mc * quarter, quarter, 1), PC)
            o_y = send(take(o, my * quarter, quarter, 1), PY)
            o_yc = send(take(o, myc * quarter, quarter, 1), PYC)
            heads = wo.shape[0]
            qn = half // quarter
            h, m = call(
                functools.partial(proj_kernel, width=D), (1,),
                [pl.BlockSpec((gw, quarter), lambda i, s: (0, 2 * s[1] + s[2]))] + [whole(gw, quarter)] * 3 + [whole(heads, w4, hd)] * 8 + [
                    pl.BlockSpec((w4, quarter), lambda i, s, k=k: (0, s[0] * 2 * qn + k * qn + 2 * s[1] + s[2])),
                    pl.BlockSpec((w4, quarter), lambda i, s, k=k: (0, k * qn + 2 * s[1] + s[2])),
                    pl.BlockSpec((w4, quarter), lambda i, s: (0, s[2])),
                    pl.BlockSpec((w4, quarter), lambda i, s: (0, s[2])),
                    whole(D, 4)],
                [whole(D, quarter), whole(quarter, D)],
                [jax.ShapeDtypeStruct((D, quarter), BF), jax.ShapeDtypeStruct((quarter, D), BF)],
                [pltpu.VMEM((4 * gw, quarter), BF), pltpu.VMEM((D, quarter), BF)],
                flops=2 * D * 4 * gw * quarter)(scal, o, o_c, o_y, o_yc, *Bs, xt, own_c, rx[k], rxc[k], gcol)
            h_own.append(h)
            m_own.append(m)
        h_for = [send(h_own[k], PX) for k in range(2)]
        m_for = []
        for k in range(2):
            m_for.append(call(
                functools.partial(renorm_kernel, width=D), (1,), [whole(D, quarter), whole(D, 4)], whole(quarter, D),
                jax.ShapeDtypeStruct((quarter, D), BF), [pltpu.VMEM((D, quarter), BF)], flops=100 * D * quarter)(scal, h_for[k], gcol))

        ft = 384
        nf = F4 // ft

        def gated(ms, w):
            return call(
                gate_up_kernel, (nf,),
                [whole(quarter, D)] * 2 + [pl.BlockSpec((w4, ft), lambda i, s: (0, i))] * 4 + [pl.BlockSpec((w4, ft), lambda i, s: (0, nf + i))] * 4,
                pl.BlockSpec((2 * quarter, ft), lambda i, s: (0, i)), jax.ShapeDtypeStruct((2 * quarter, F4), BF),
                flops=2 * D * 2 * F4 * 2 * quarter)(scal, *ms, *w, *w)

        z = {(t, hf): gated(ms, w) for hf, w in (('y', gu_y), ('o', gu_o)) for t, ms in (('own', m_own), ('for', m_for))}

        w2 = 2 * w4
        chunks = 2 * quarter // CH
        yt = 2 * CH
        part = call(
            down_y_kernel, (2 * quarter // yt,), [pl.BlockSpec((yt, F4), lambda i, s: (i, 0))] * 2 + [whole(w4, F4)] * 4,
            pl.BlockSpec((yt // CH, D, 2 * CH), lambda i, s: (i, 0, 0)), jax.ShapeDtypeStruct((chunks, D, 2 * CH), F32),
            [pltpu.VMEM((D, F4), BF)], flops=2 * D * F4 * 2 * quarter * 2)(scal, z['own', 'y'], z['for', 'y'], *dn_y)
        dma = pltpu.SemaphoreType.DMA
        out = pl.pallas_call(
            functools.partial(tail_kernel, width=D, chunks=chunks),
            out_shape=jax.ShapeDtypeStruct((w4, rows), BF),
            in_specs=[ANY] * 11 + [pl.BlockSpec(memory_space=pltpu.VMEM)],
            out_specs=ANY,
            scratch_shapes=[
                pltpu.VMEM((D, F4), BF), pltpu.VMEM((chunks, 2 * CH, F4), BF), pltpu.VMEM((2, D, 2 * CH), F32),
                pltpu.VMEM((chunks, w2, 2 * CH), F32), pltpu.VMEM((chunks, w2, 2 * CH), BF), pltpu.VMEM((chunks, w2, 2 * CH), BF),
                pltpu.VMEM((chunks, w2, 2 * CH), BF), pltpu.VMEM((chunks, 8, 2 * CH), F32), pltpu.VMEM((chunks, 8, 2 * CH), F32), pltpu.VMEM((8, 2 * CH), F32),
                dma((4,)), dma((chunks, 2)), dma((2,)), dma((chunks, 2)), dma((chunks, 2)),
                dma((chunks,)), dma((chunks,)), dma((chunks,)), dma((chunks,)), dma((chunks, 2, 3)), dma((chunks, 2, 3))],
            cost_estimate=pl.CostEstimate(flops=2 * D * F4 * 4 * quarter, bytes_accessed=4 * D * rows, transcendentals=0),
            compiler_params=pltpu.CompilerParams(vmem_limit_bytes=60 * 1024 * 1024, collective_id=0, has_side_effects=True),
            name='tail',
        )(part, z['own', 'o'], z['for', 'o'], *dn_o, *h_own, *h_for, jnp.broadcast_to(gcol[:w2, 3:4], (w2, 128)))
        tokens_out = out.T

        kv_c = send(kv, PC)
        kv_x = send(kv, PX)
        kv_xc = send(kv_x, PC)
        nk = S // tile
        kv_outs = []
        for i, (t, tc) in enumerate(((kv, kv_c), (kv_x, kv_xc))):
            kv_outs = call(
                kv_out_kernel, (nk,), [pl.BlockSpec((tile, gw), lambda i, s: (i, 0))] * 2 + [ANY] * len(kv_outs),
                [pl.BlockSpec((tile, 2, hd), lambda j, s, i=i: ((s[0] if i == 0 else 1 - s[0]) * nk + j, 0, 0))] * 2, [jax.ShapeDtypeStruct((rows, 2, hd), BF)] * 2,
                flops=100 * rows * hd, aliases={3: 0, 4: 1} if i else None)(scal, t, tc, *kv_outs)
        k_out, v_out = kv_outs
        return tokens_out, k_out, v_out

    width_spec = P('dm')
    in_specs = (P('dp', 'dm'), P('dp', None), width_spec, P('dm', 'tp', None), P('dm', 'tp', None), P('dm', 'tp', None), P('tp', None, 'dm'), width_spec, width_spec, P('dm', 'tp'), P('dm', 'tp'), P('tp', 'dm'), width_spec)
    out_specs = (P('dp', 'dm'), P('dp', 'tp', None), P('dp', 'tp', None))
    return jax.shard_map(layer, mesh=mesh, in_specs=in_specs, out_specs=out_specs, check_vma=False)
```

```python
import functools

import jax
import jax.numpy as jnp
from jax import lax
from jax.experimental import pallas as pl
from jax.experimental.pallas import tpu as pltpu
from jax.sharding import PartitionSpec as P


NORM_EPS = 1e-6
SOFT_CAP = 50.0
ROPE_BASE = 10000.0
WINDOW_LEN = 4096
LOG2E = 1.4426950408889634
BF = jnp.bfloat16
F32 = jnp.float32
VM = 63 * 1024 * 1024
CH = 128
BIG = 2.0 ** 40
SHRINK = 2.0 ** -88
MT = 256
ANY = pl.BlockSpec(memory_space=pl.ANY)


vcat = functools.partial(jnp.concatenate, axis=0)
hcat = functools.partial(jnp.concatenate, axis=1)
by_col = lambda i, *_: (0, i)
by_row = lambda i, *_: (i, 0)


def dot(a, b):
    return jnp.dot(a, b, preferred_element_type=F32)


def dot_nt(a, b):
    return lax.dot_general(a, b, (((1,), (1,)), ((), ())), preferred_element_type=F32)


def whole(*shape):
    return pl.BlockSpec(shape, lambda *_: (0,) * len(shape))


def inv_rms(blocks, width):
    sq = sum(jnp.sum(jnp.square(b.astype(F32)), axis=0, keepdims=True) for b in blocks)
    return lax.rsqrt(sq / width + NORM_EPS)


def part_of(ref, j, size):
    return ref.at[j * size:(j + 1) * size, :]


def call(kernel, grid, in_specs, out_specs, out_shape, scratch=(), prefetch=1, flops=0, nbytes=0, aliases=None):
    return pl.pallas_call(
        kernel,
        out_shape=out_shape,
        grid_spec=pltpu.PrefetchScalarGridSpec(num_scalar_prefetch=prefetch, grid=grid, in_specs=in_specs, out_specs=out_specs, scratch_shapes=list(scratch)),
        cost_estimate=pl.CostEstimate(flops=flops, bytes_accessed=nbytes, transcendentals=0),
        compiler_params=pltpu.CompilerParams(vmem_limit_bytes=VM),
        input_output_aliases=aliases or {},
    )


def norm_kernel(s_ref, own, own_c, rx, rxc, ry, ryc, g_ref, *rest, width, per_half):
    a_ref = rest[-1]
    w4 = own.shape[0]
    mine = (pl.program_id(0) // per_half) == s_ref[1]
    blocks = [own[...], own_c[...], jnp.where(mine, rx[...], ry[...]), jnp.where(mine, rxc[...], ryc[...])]
    r = inv_rms(blocks, width)
    for j, b in enumerate(blocks):
        part_of(a_ref, j, w4)[...] = (b.astype(F32) * r * part_of(g_ref, j, w4)[:, 0:1]).astype(BF)


def qkv_kernel(s_ref, a_ref, w0, w1, w2, w3, cos_ref, sin_ref, qv_ref, kv_ref, w_t, w_all, *, hd):
    w4 = w0.shape[0]

    @pl.when(pl.program_id(0) == 0)
    def _():
        for j, w in enumerate((w0, w1, w2, w3)):
            part_of(w_all, j, w4)[...] = w[...]
        for r in range(0, w_all.shape[0], MT):
            w_t[:, r:r + MT] = w_all[r:r + MT, :].T

    qkv = dot(w_t[...], a_ref[...]).astype(BF).astype(F32)
    ct, st = cos_ref[...], sin_ref[...]
    hh = hd // 2

    def rot(base):
        u1, u2 = qkv[base:base + hh], qkv[base + hh:base + hd]
        return u1 * ct - u2 * st, u2 * ct + u1 * st

    for g in range(2):
        lo, hi = rot(g * hd)
        qv_ref[g * hd:g * hd + hh, :] = lo.astype(BF)
        qv_ref[g * hd + hh:(g + 1) * hd, :] = hi.astype(BF)
    v = qkv[3 * hd:]
    qv_ref[2 * hd:, :] = v.astype(BF)
    klo, khi = rot(2 * hd)
    kv_ref[:, :hh] = klo.T.astype(BF)
    kv_ref[:, hh:hd] = khi.T.astype(BF)
    kv_ref[:, hd:] = v.T.astype(BF)


def attn_kernel(lo_ref, full_ref, q_ref, k_ref, v_ref, pq_ref, pk_ref, o_ref, acc_ref, qq_ref, l_ref, vs_ref, f_ref, *, bq, bk, q_block0, scale):
    qb = q_block0 + pl.program_id(0)
    hd = k_ref.shape[1]
    groups = q_ref.shape[0] // hd
    lo, full = lo_ref[qb], full_ref[qb]
    diag = (qb * bq) // bk
    last = ((qb + 1) * bq + bk - 1) // bk

    @pl.when(pl.program_id(0) == 0)
    def _():
        top = jnp.max(jnp.abs(v_ref[...].astype(F32)), axis=0, keepdims=True)
        top = jnp.max(top, axis=1, keepdims=True)
        f_ref[...] = jnp.broadcast_to(jnp.where(top > BIG, SHRINK, 1.0), f_ref.shape)
        vs_ref[...] = (v_ref[...].astype(F32) * f_ref[0:1, 0:1]).astype(BF)

    for g in range(groups):
        qq_ref[:, g * bq:(g + 1) * bq] = q_ref[g * hd:(g + 1) * hd, :]
    l_ref[...] = jnp.zeros_like(l_ref)
    acc_ref[...] = jnp.zeros_like(acc_ref)

    def step(j, masked):
        rows = pl.ds(pl.multiple_of(j * bk, bk), bk)
        kb = k_ref[rows, :]
        vb = vs_ref[:, rows]
        for n in range(0, groups * bq, MT):
            cols = slice(n, n + MT)
            s = dot(kb, qq_ref[:, cols])
            p = jnp.exp2(jnp.tanh(s * (scale / SOFT_CAP)) * (SOFT_CAP * LOG2E))
            if masked:
                dif = pq_ref[:, n % bq:n % bq + MT] - pk_ref[rows, :]
                p = jnp.where((dif >= 0) & (dif < WINDOW_LEN), p, 0.0)
            l_ref[:, cols] += jnp.sum(p, axis=0, keepdims=True)
            acc_ref[:, cols] += dot(vb, p.astype(BF))

    mid = jnp.maximum(jnp.minimum(full, diag), lo)

    def masked_step(j, _):
        step(j, True)
        return 0

    def full_step(j, _):
        step(j, False)
        return 0

    lax.fori_loop(lo, mid, masked_step, 0)
    lax.fori_loop(mid, diag, full_step, 0)
    lax.fori_loop(jnp.maximum(diag, mid), last, masked_step, 0)
    for g in range(groups):
        cols = slice(g * bq, (g + 1) * bq)
        o_ref[g * hd:(g + 1) * hd, :] = (acc_ref[:, cols] / l_ref[:, cols] / f_ref[0:1, 0:1]).astype(BF)


def norm_to_m(m_ref, blocks, r, g_ref, col, mt_ref):
    w4 = blocks[0].shape[0]
    for j, b in enumerate(blocks):
        part_of(mt_ref, j, w4)[...] = (b * r * part_of(g_ref, j, w4)[:, col:col + 1]).astype(BF)
    for i in range(0, mt_ref.shape[0], MT):
        m_ref[:, i:i + MT] = mt_ref[i:i + MT, :].T


def proj_kernel(s_ref, o_own, o_c, o_y, o_yc, b0, b0c, b1, b1c, b2, b2c, b3, b3c, x0, x1, x2, x3, g_ref, h_ref, m_ref, o_all, mt_ref, w_ref, w_sem, *, width):
    cps = [pltpu.make_async_copy(b, w_ref.at[i], w_sem.at[i]) for i, b in enumerate((b0, b2, b0c, b2c, b1, b3, b1c, b3c))]
    for cp in cps:
        cp.start()
    c = s_ref[2]
    gw = o_own.shape[0]
    first = c == 0
    for i, (a, b) in enumerate(((o_own, o_c), (o_c, o_own), (o_y, o_yc), (o_yc, o_y))):
        part_of(o_all, i, gw)[...] = jnp.where(first, a[...], b[...])
    w4 = x0.shape[0]
    heads = b0.shape[0]
    o = o_all[...]
    att = []
    for j in range(4):
        two = (2 * j, 2 * j + 1)
        for i in two:
            cps[i].wait()
        w = hcat([w_ref[i, h] for i in two for h in range(heads)])
        att.append(dot(w, o).astype(BF).astype(F32))
    r = inv_rms(att, width)
    hs = []
    for j, (t, xr) in enumerate(zip(att, (x0, x1, x2, x3))):
        h = (xr[...].astype(F32) + t * r * part_of(g_ref, j, w4)[:, 1:2]).astype(BF)
        part_of(h_ref, j, w4)[...] = h
        hs.append(h.astype(F32))
    norm_to_m(m_ref, hs, inv_rms(hs, width), g_ref, 2, mt_ref)


def renorm_kernel(s_ref, h_ref, g_ref, m_ref, mt_ref, *, width):
    w4 = h_ref.shape[0] // 4
    hs = [part_of(h_ref, j, w4)[...].astype(F32) for j in (2, 3, 0, 1)]
    norm_to_m(m_ref, hs, inv_rms(hs, width), g_ref, 2, mt_ref)


def gate_up_kernel(s_ref, ma, mb, g0, g1, g2, g3, u0, u1, u2, u3, z_ref):
    n = z_ref.shape[1]
    w = hcat([vcat([g[...] for g in (g0, g1, g2, g3)]), vcat([u[...] for u in (u0, u1, u2, u3)])])
    base = 0
    for m in (ma, mb):
        for r in range(0, m.shape[0], MT):
            t = dot(m[r:r + MT, :], w)
            g, u = t[:, :n].astype(BF).astype(F32), t[:, n:].astype(BF).astype(F32)
            z_ref[base:base + MT, :] = (jax.nn.gelu(g, approximate=True) * u).astype(BF)
            base += MT


def down_y_kernel(s_ref, zwa, zwb, zfa, zfb, d0, d1, d2, d3, acc_ref, d_ref):
    w4 = d0.shape[0]
    n = zwa.shape[0]

    @pl.when(pl.program_id(0) == 0)
    def _():
        for j, dd in enumerate((d0, d1, d2, d3)):
            part_of(d_ref, j, w4)[...] = dd[...]

    z = vcat([hcat([a[...], b[...]]) for a, b in ((zwa, zwb), (zfa, zfb))])
    for j in range(4):
        t = dot_nt(d_ref[j * w4:(j + 1) * w4, :], z)
        for q in range(n // CH):
            acc_ref[q, j * w4:(j + 1) * w4, :CH] = t[:, q * CH:(q + 1) * CH]
            acc_ref[q, j * w4:(j + 1) * w4, CH:] = t[:, n + q * CH:n + (q + 1) * CH]


def tail_kernel(part, zwa, zwb, zfa, zfb, d0, d1, d2, d3, hw0, hw1, hf0, hf1, g_ref, out,
                d_ref, z_ref, p_ref, lo_ref, hi_ref, rec_ref, h_ref, sqs_ref, sqr_ref, sqo_ref,
                d_sem, z_sem, p_sem, h_sem, loc_sem, rs_s, rs_r, sq_s, sq_r, out_s, out_r, *, width, chunks):
    w4 = d0.shape[0]
    w2 = 2 * w4
    f8 = zwa.shape[1]
    y = lax.axis_index('tp')
    dm = lax.axis_index('dm')
    x, c = dm // 2, lax.rem(dm, 2)
    px = {'dp': 0, 'tp': y, 'dm': (1 - x) * 2 + c}
    pc = {'dp': 0, 'tp': y, 'dm': x * 2 + 1 - c}
    py = {'dp': 0, 'tp': 1 - y, 'dm': dm}
    pyc = {'dp': 0, 'tp': 1 - y, 'dm': x * 2 + 1 - c}

    def local(src, dst, sem):
        return pltpu.make_async_copy(src, dst, sem)

    def remote(src, dst, s_sem, r_sem, dev):
        return pltpu.make_async_remote_copy(src_ref=src, dst_ref=dst, send_sem=s_sem, recv_sem=r_sem, device_id=dev, device_id_type=pl.DeviceIdType.MESH)

    d_cp = [local(dd, part_of(d_ref, j, w4), d_sem.at[j]) for j, dd in enumerate((d0, d1, d2, d3))]

    def z_cp(p):
        return [local(src.at[pl.ds(p * CH, CH), :], z_ref.at[p, i // 2 * CH:(i // 2 + 1) * CH, i % 2 * f8:(i % 2 + 1) * f8], z_sem.at[p, i]) for i, src in enumerate((zwa, zwb, zfa, zfb))]

    def p_cp(p):
        return local(part.at[p], p_ref.at[lax.rem(p, 2)], p_sem.at[lax.rem(p, 2)])

    per = hw0.shape[1] // CH
    h_cp = []
    for q in range(chunks):
        k, l = q // per, (q % per) * CH
        h_cp.append(local((hw0, hw1)[k].at[0:w2, l:l + CH], h_ref.at[q, :, 0:CH], h_sem.at[q, 0]))
        h_cp.append(local((hf0, hf1)[k].at[w2:2 * w2, l:l + CH], h_ref.at[q, :, CH:2 * CH], h_sem.at[q, 1]))

    def start(cps):
        for cp in cps:
            cp.start()

    start(z_cp(0) + [d_cp[2], p_cp(0), d_cp[3]])

    bar = pltpu.get_barrier_semaphore()
    for dev in (px, pc, py, pyc):
        pl.semaphore_signal(bar, inc=1, device_id=dev, device_id_type=pl.DeviceIdType.MESH)
    pl.semaphore_wait(bar, 4)

    def rs(p, i):
        rws = slice(i * w4, (i + 1) * w4)
        return remote(hi_ref.at[p, rws], rec_ref.at[p, rws], rs_s.at[p, i], rs_r.at[p, i], px)

    def sq(p):
        return remote(sqs_ref.at[p], sqr_ref.at[p], sq_s.at[p], sq_r.at[p], px)

    def outs(p):
        k, l = p // per, lax.rem(p, per)
        res = []
        for i, pr in enumerate((x, 1 - x)):
            col = pl.multiple_of(((pr * 2 + k) * 4 + 2 * y + c) * (per * CH) + l * CH, CH)
            mine = rec_ref.at[p, 0:w4, i * CH:(i + 1) * CH]
            give = rec_ref.at[p, w4:w2, i * CH:(i + 1) * CH]
            dst = out.at[:, pl.ds(col, CH)]
            res.append((local(mine, dst, loc_sem.at[p, i]), remote(mine, dst, out_s.at[p, i, 0], out_r.at[p, i, 0], py),
                        remote(give, dst, out_s.at[p, i, 1], out_r.at[p, i, 1], pyc), remote(give, dst, out_s.at[p, i, 2], out_r.at[p, i, 2], pc)))
        return res

    def block(p, j):
        return dot_nt(part_of(d_ref, j, w4)[...], z_ref[p]) + p_ref[lax.rem(p, 2), j * w4:(j + 1) * w4, :]

    def upper(p, first=False):
        p_cp(p).wait()
        for cp in z_cp(p):
            cp.wait()
        if first:
            p_cp(1).start()
        else:
            @pl.when(p + 1 < chunks)
            def _():
                p_cp(p + 1).start()
        for i in range(2):
            if first:
                d_cp[2 + i].wait()
            t = block(p, 2 + i).astype(BF)
            hi_ref[p, i * w4:(i + 1) * w4, :CH] = t[:, CH:]
            hi_ref[p, i * w4:(i + 1) * w4, CH:] = t[:, :CH]
            if first or i == 0:
                rs(p, i).start()

    def lower(p, first=False):
        for j in range(2):
            if first:
                d_cp[j].wait()
            lo_ref[p, j * w4:(j + 1) * w4, :] = block(p, j)

    def add(p):
        for i in range(2):
            rs(p, i).wait_recv()
        t = (lo_ref[p] + rec_ref[p].astype(F32)).astype(BF)
        rec_ref[p] = t
        t = t.astype(F32)
        v = jnp.broadcast_to(jnp.sum(t * t, axis=0, keepdims=True), sqo_ref.shape)
        sqo_ref[...] = v
        sqs_ref[p, :, :CH] = v[:, CH:]
        sqs_ref[p, :, CH:] = v[:, :CH]
        sq(p).start()

    def finish(p):
        sq(p).wait_recv()
        r = lax.rsqrt((sqo_ref[...] + sqr_ref[p]) / width + NORM_EPS)[0:1]
        g = g_ref[...]
        g = hcat([g] * (2 * CH // 128))
        rec_ref[p] = (h_ref[p].astype(F32) + rec_ref[p].astype(F32) * r * g).astype(BF)
        for group in outs(p):
            for cp in group[1:] + group[:1]:
                cp.start()

    upper(0, True)
    start(d_cp[:2] + z_cp(1))
    lower(0, True)
    start(h_cp)
    for q in range(2, chunks):
        start(z_cp(q))
    upper(1)
    lower(1)
    for cp in h_cp:
        cp.wait()

    def body(p, _):
        add(p)
        rs(p + 1, 1).start()
        upper(p + 2)
        finish(p)
        lower(p + 2)
        return 0

    lax.fori_loop(0, chunks - 2, body, 0)
    add(chunks - 2)
    rs(chunks - 1, 1).start()
    finish(chunks - 2)
    add(chunks - 1)
    finish(chunks - 1)

    def drain(p, _):
        for i in range(2):
            rs(p, i).wait_send()
        sq(p).wait_send()
        for group in outs(p):
            group[0].wait()
            for cp in group[1:]:
                cp.wait()
        return 0

    lax.fori_loop(0, chunks, drain, 0)


def kv_out_kernel(s_ref, kv0, kv1, *rest, extra):
    if extra:
        rest[-1][...] = rest[0][...]
    k_ref, v_ref = rest[-2 - extra:][:2]
    hd = k_ref.shape[2]
    first = s_ref[2] == 0
    a, b = kv0[...], kv1[...]
    two = jnp.where(first, a, b), jnp.where(first, b, a)
    for ref, at in ((k_ref, 0), (v_ref, hd)):
        ref[...] = jnp.stack([t[:, at:at + hd] for t in two], axis=1)


def solution(mesh):
    tp_size, dm_size = mesh.shape['tp'], mesh.shape['dm']

    def flip(bits):
        return [(i, i ^ bits) for i in range(mesh.size)]

    C, X, Y = 1, 2, dm_size
    PX, PY, PC, PXC, PYC = flip(X), flip(Y), flip(C), flip(X | C), flip(Y | C)

    def send(a, perm):
        return lax.ppermute(a, ('tp', 'dm'), perm)

    def layer(tokens, positions, n1, wq, wk, wv, wo, n2, n3, wg, wu, wd, n4):
        y = lax.axis_index('tp')
        d = lax.axis_index('dm')
        x, c = d // 2, d % 2
        xo, yo, co = 1 - x, 1 - y, 1 - c
        rows, w4 = tokens.shape
        D = w4 * dm_size
        S = positions.shape[1]
        hd = wq.shape[2]
        scale = (D / (wq.shape[1] * tp_size)) ** -0.5
        gw = 2 * hd
        half = S // 2
        quarter = half // 4
        F4 = wg.shape[1] // 2
        scal = jnp.stack([x, y, c]).astype(jnp.int32)

        def take(a, start, size, axis=0):
            return lax.dynamic_slice_in_dim(a, start, size, axis)

        xt = tokens.T

        gains = jnp.stack([n1, n2, n3, n4])
        gall = hcat([gains, send(gains, PC), send(gains, PX), send(gains, PXC)])
        gcol = (1.0 + gall.astype(F32)).T

        rx = [send(take(xt, xo * S + k * half + y * (half // 2), half // 2, 1), PX) for k in range(2)]
        own_p = take(xt, x * S, S, 1)
        own_c = send(own_p, PC)
        ry = [send(rx[k], PY) for k in range(2)]
        rxc = [send(rx[k], PC) for k in range(2)]
        ryc = [send(ry[k], PC) for k in range(2)]

        def group_cols(g):
            return hcat([take(w, n * g, n, 1).reshape(w4, n * hd) for w, n in ((wq, 2), (wk, 1), (wv, 1))])

        wq_own, wq_oth = group_cols(c), group_cols(co)
        wqs = [wq_own, send(wq_oth, PC), send(wq_own, PX), send(wq_oth, PXC)]

        wot = jnp.transpose(wo, (0, 2, 1))
        B0 = wot
        B1 = send(B0, PX)
        B2 = send(B0, PY)
        B3 = send(B1, PY)
        Bs = []
        for b in (B0, B1, B2, B3):
            Bs += [b, send(b, PC)]

        def gather(own, oth):
            r1 = send(oth, PX)
            s0 = send(own, PY)
            s1 = send(r1, PY)
            ty = [own, send(own, PC), r1, send(r1, PC)]
            to = [s0, send(s0, PC), s1, send(s1, PC)]
            return ty, to

        F8 = F4 // 2

        def gu_half(xx, at):
            return hcat([take(w, xx * F4 + at, F8, 1) for w in (wg, wu)])

        gu = {ab: gather(gu_half(x, at), gu_half(xo, at)) for ab, at in (('a', 0), ('b', F8))}
        wdt = wd.T
        dw_own, dw_oth = (take(wdt, xx * F4, F4, 1) for xx in (x, xo))
        dn_y, dn_o = gather(dw_own, dw_oth)

        pos = take(positions, x, 1)[0]
        inv_freq = ROPE_BASE ** (-2.0 * jnp.arange(hd // 2, dtype=F32) / hd)
        ang = inv_freq[:, None] * pos.astype(F32)[None, :]
        cos_t, sin_t = jnp.cos(ang), jnp.sin(ang)

        tile = 512
        nt = half // tile
        per_half = nt // 2
        nb = S // tile
        a_all = []
        for k in range(2):
            a_all = [call(
                functools.partial(norm_kernel, width=D, per_half=per_half), (nt,),
                [pl.BlockSpec((w4, tile), lambda i, s, k=k: (0, s[0] * nb + k * nt + i)), pl.BlockSpec((w4, tile), lambda i, s, k=k: (0, k * nt + i))]
                + [pl.BlockSpec((w4, tile), lambda i, s: (0, i % per_half))] * 4 + [whole(D, 4)] + [ANY] * k,
                pl.BlockSpec((D, tile), lambda i, s, k=k: (0, k * nt + i)), jax.ShapeDtypeStruct((D, S), BF),
                flops=100 * D * half, aliases={8: 0} if k else None)(scal, xt, own_c, rx[k], rxc[k], ry[k], ryc[k], gcol, *a_all)]
        qv, kv = call(
            functools.partial(qkv_kernel, hd=hd), (nb,),
            [pl.BlockSpec((D, tile), by_col)] + [whole(w4, 2 * gw)] * 4 + [pl.BlockSpec((hd // 2, tile), by_col)] * 2,
            [pl.BlockSpec((gw + hd, tile), by_col), pl.BlockSpec((tile, gw), by_row)],
            [jax.ShapeDtypeStruct((gw + hd, S), BF), jax.ShapeDtypeStruct((S, gw), BF)],
            [pltpu.VMEM((2 * gw, D), BF), pltpu.VMEM((D, 2 * gw), BF)],
            flops=2 * D * 2 * gw * S)(scal, *a_all, *wqs, cos_t, sin_t)

        bq = bk = 512
        first_q, last_q = pos[0::bq][:, None], pos[bq - 1::bq][:, None]
        first_k, last_k = pos[0::bk][None, :], pos[bk - 1::bk][None, :]
        lo_t = jnp.sum((first_q - last_k >= WINDOW_LEN).astype(jnp.int32), axis=1)
        full_t = jnp.sum((last_q - first_k >= WINDOW_LEN).astype(jnp.int32), axis=1)
        pos_row, pos_col = pos.reshape(1, S), pos.reshape(S, 1)
        h_own, m_own = [], []
        for k in range(2):
            q0 = k * half // bq
            kl = (k + 1) * half
            o = call(
                functools.partial(attn_kernel, bq=bq, bk=bk, q_block0=q0, scale=scale), (half // bq,),
                [
                    pl.BlockSpec((gw, bq), lambda i, *_, q0=q0: (0, q0 + i)),
                    pl.BlockSpec((kl, hd), lambda i, *_: (0, 0)),
                    pl.BlockSpec((hd, kl), lambda i, *_: (2, 0)),
                    pl.BlockSpec((1, bq), lambda i, *_, q0=q0: (0, q0 + i)),
                    pl.BlockSpec((kl, 1), lambda i, *_: (0, 0)),
                ],
                pl.BlockSpec((gw, bq), by_col),
                jax.ShapeDtypeStruct((gw, half), BF),
                [pltpu.VMEM((hd, 2 * bq), F32), pltpu.VMEM((hd, 2 * bq), BF), pltpu.VMEM((1, 2 * bq), F32), pltpu.VMEM((hd, kl), BF), pltpu.VMEM((8, CH), F32)],
                prefetch=2, flops=4 * hd * 2 * half * (k * half + half // 2))(lo_t, full_t, qv, kv, qv, pos_row, pos_col)
            mc = 2 * y + co
            my, myc = 2 * yo + c, 2 * yo + co
            o_c = send(take(o, mc * quarter, quarter, 1), PC)
            o_y = send(take(o, my * quarter, quarter, 1), PY)
            o_yc = send(take(o, myc * quarter, quarter, 1), PYC)
            heads = wo.shape[0]
            qn = half // quarter
            h, m = call(
                functools.partial(proj_kernel, width=D), (1,),
                [pl.BlockSpec((gw, quarter), lambda i, s: (0, 2 * s[1] + s[2]))] + [whole(gw, quarter)] * 3 + [ANY] * 8 + [
                    pl.BlockSpec((w4, quarter), lambda i, s, k=k: (0, s[0] * 2 * qn + k * qn + 2 * s[1] + s[2])),
                    pl.BlockSpec((w4, quarter), lambda i, s, k=k: (0, k * qn + 2 * s[1] + s[2])),
                    pl.BlockSpec((w4, quarter), lambda i, s: (0, s[2])),
                    pl.BlockSpec((w4, quarter), lambda i, s: (0, s[2])),
                    whole(D, 4)],
                [whole(D, quarter), whole(quarter, D)],
                [jax.ShapeDtypeStruct((D, quarter), BF), jax.ShapeDtypeStruct((quarter, D), BF)],
                [pltpu.VMEM((4 * gw, quarter), BF), pltpu.VMEM((D, quarter), BF), pltpu.VMEM((8, heads, w4, hd), BF), pltpu.SemaphoreType.DMA((8,))],
                flops=2 * D * 4 * gw * quarter)(scal, o, o_c, o_y, o_yc, *Bs, xt, own_c, rx[k], rxc[k], gcol)
            h_own.append(h)
            m_own.append(m)
        h_for = [send(h_own[k], PX) for k in range(2)]
        m_for = []
        for k in range(2):
            m_for.append(call(
                functools.partial(renorm_kernel, width=D), (1,), [whole(D, quarter), whole(D, 4)], whole(quarter, D),
                jax.ShapeDtypeStruct((quarter, D), BF), [pltpu.VMEM((D, quarter), BF)], flops=100 * D * quarter)(scal, h_for[k], gcol))

        ft = 384
        nf = F8 // ft

        def gated(ms, w):
            return call(
                gate_up_kernel, (nf,),
                [whole(quarter, D)] * 2 + [pl.BlockSpec((w4, ft), by_col)] * 4 + [pl.BlockSpec((w4, ft), lambda i, s: (0, nf + i))] * 4,
                pl.BlockSpec((2 * quarter, ft), by_col), jax.ShapeDtypeStruct((2 * quarter, F8), BF),
                flops=2 * D * 2 * F8 * 2 * quarter)(scal, *ms, *w, *w)

        z = {t + hf: [gated(ms, gu[ab][i]) for ab in gu] for i, hf in enumerate('yo') for t, ms in (('own', m_own), ('for', m_for))}

        w2 = 2 * w4
        chunks = 2 * quarter // CH
        yt = 2 * CH
        part = call(
            down_y_kernel, (2 * quarter // yt,), [pl.BlockSpec((yt, F8), by_row)] * 4 + [whole(w4, F4)] * 4,
            pl.BlockSpec((2, D, yt), lambda i, s: (i, 0, 0)), jax.ShapeDtypeStruct((chunks, D, yt), F32),
            [pltpu.VMEM((D, F4), BF)], flops=2 * D * F4 * 2 * quarter * 2)(scal, *z['owny'], *z['fory'], *dn_y)
        dma = pltpu.SemaphoreType.DMA
        out = pl.pallas_call(
            functools.partial(tail_kernel, width=D, chunks=chunks),
            out_shape=jax.ShapeDtypeStruct((w4, rows), BF),
            in_specs=[ANY] * 13 + [pl.BlockSpec(memory_space=pltpu.VMEM)],
            out_specs=ANY,
            scratch_shapes=[
                pltpu.VMEM((D, F4), BF), pltpu.VMEM((chunks, yt, F4), BF), pltpu.VMEM((2, D, yt), F32), pltpu.VMEM((chunks, w2, yt), F32),
                *[pltpu.VMEM((chunks, w2, yt), BF)] * 3, *[pltpu.VMEM((chunks, 8, yt), F32)] * 2, pltpu.VMEM((8, yt), F32),
                dma((4,)), dma((chunks, 4)), dma((2,)), *[dma((chunks, 2))] * 4, *[dma((chunks,))] * 2, *[dma((chunks, 2, 3))] * 2],
            cost_estimate=pl.CostEstimate(flops=2 * D * F4 * 4 * quarter, bytes_accessed=4 * D * rows, transcendentals=0),
            compiler_params=pltpu.CompilerParams(vmem_limit_bytes=60 * 1024 * 1024, collective_id=0, has_side_effects=True),
            name='tail',
        )(part, *z['owno'], *z['foro'], *dn_o, *h_own, *h_for, jnp.broadcast_to(gcol[:w2, 3:4], (w2, 128)))
        kv_c = send(kv, PC)
        kv_x = [send(kv[k * half:(k + 1) * half], PX) for k in range(2)]
        kv_xc = [send(kv_x[k], PC) for k in range(2)]
        kv_spec = pl.BlockSpec((tile, gw), by_row)
        kv_outs = []
        for i, (t, tc, n, base) in enumerate(((kv, kv_c, nb, 0), (kv_x[0], kv_xc[0], nt, 0), (kv_x[1], kv_xc[1], nt, nt))):
            extra = i == 2
            at = lambda j, s, i=i, base=base: ((1 - s[0] if i else s[0]) * nb + base + j, 0, 0)
            cspec = [pl.BlockSpec((w4, rows // nt), by_col)] * extra
            kv_outs = call(
                functools.partial(kv_out_kernel, extra=int(extra)), (n,), [kv_spec] * 2 + cspec + [ANY] * len(kv_outs),
                [pl.BlockSpec((tile, 2, hd), at)] * 2 + cspec, [jax.ShapeDtypeStruct((rows, 2, hd), BF)] * 2 + [jax.ShapeDtypeStruct((w4, rows), BF)] * extra,
                flops=100 * rows * hd, aliases={3 + extra: 0, 4 + extra: 1} if i else None)(scal, t, tc, *[out] * extra, *kv_outs)
        k_out, v_out, out = kv_outs
        return out.T, k_out, v_out

    width_spec = P('dm')
    in_specs = (P('dp', 'dm'), P('dp', None), width_spec, P('dm', 'tp', None), P('dm', 'tp', None), P('dm', 'tp', None), P('tp', None, 'dm'), width_spec, width_spec, P('dm', 'tp'), P('dm', 'tp'), P('tp', 'dm'), width_spec)
    out_specs = (P('dp', 'dm'), P('dp', 'tp', None), P('dp', 'tp', None))
    return jax.shard_map(layer, mesh=mesh, in_specs=in_specs, out_specs=out_specs, check_vma=False)
```

```python
import functools

import jax
import jax.numpy as jnp
from jax import lax
from jax.experimental import pallas as pl
from jax.experimental.pallas import tpu as pltpu
from jax.sharding import PartitionSpec as P


NORM_EPS = 1e-6
SOFT_CAP = 50.0
ROPE_BASE = 10000.0
WINDOW_LEN = 4096
LOG2E = 1.4426950408889634
BF = jnp.bfloat16
F32 = jnp.float32
VM = 63 * 1024 * 1024
CH = 128
BIG = 2.0 ** 40
SHRINK = 2.0 ** -88
MT = 256
KT = 512
ANY = pl.BlockSpec(memory_space=pl.ANY)


vcat = functools.partial(jnp.concatenate, axis=0)
hcat = functools.partial(jnp.concatenate, axis=1)
by_col = lambda i, *_: (0, i)
by_row = lambda i, *_: (i, 0)
fixed = lambda *_: 0


def dot(a, b):
    return jnp.dot(a, b, preferred_element_type=F32)


def dot_nt(a, b):
    return lax.dot_general(a, b, (((1,), (1,)), ((), ())), preferred_element_type=F32)


def cols(height, wide, at):
    return pl.BlockSpec((height, wide), lambda i, *s: (0, at(i, *s)))


def bf(*shape):
    return jax.ShapeDtypeStruct(shape, BF)


def f32(*shape):
    return jax.ShapeDtypeStruct(shape, F32)


def vmem(*shape, dtype=BF):
    return pltpu.VMEM(shape, dtype)


def whole(*shape):
    return pl.BlockSpec(shape, lambda *_: (0,) * len(shape))


def inv_rms(blocks, width):
    sq = sum(jnp.sum(jnp.square(b.astype(F32)), axis=0, keepdims=True) for b in blocks)
    return lax.rsqrt(sq / width + NORM_EPS)


def part_of(ref, j, size):
    return ref.at[j * size:(j + 1) * size, :]


def call(kernel, grid, in_specs, out_specs, out_shape, scratch=(), prefetch=1, flops=0, nbytes=0, aliases=None):
    return pl.pallas_call(
        kernel,
        out_shape=out_shape,
        grid_spec=pltpu.PrefetchScalarGridSpec(num_scalar_prefetch=prefetch, grid=grid, in_specs=in_specs, out_specs=out_specs, scratch_shapes=list(scratch)),
        cost_estimate=pl.CostEstimate(flops=flops, bytes_accessed=nbytes, transcendentals=0),
        compiler_params=pltpu.CompilerParams(vmem_limit_bytes=VM),
        input_output_aliases=aliases or {},
    )


def norm_kernel(s_ref, own, own_c, rx, rxc, ry, ryc, g_ref, *rest, width, per_half):
    a_ref = rest[-1]
    w4 = own.shape[0]
    mine = (pl.program_id(0) // per_half) == s_ref[1]
    blocks = [own[...], own_c[...], jnp.where(mine, rx[...], ry[...]), jnp.where(mine, rxc[...], ryc[...])]
    r = inv_rms(blocks, width)
    for j, b in enumerate(blocks):
        part_of(a_ref, j, w4)[...] = (b.astype(F32) * r * part_of(g_ref, j, w4)[:, 0:1]).astype(BF)


def rope_kernel(s_ref, pos_ref, freq_ref, cos_ref, sin_ref):
    ang = freq_ref[...] * pos_ref[...].astype(F32)
    cos_ref[...] = jnp.cos(ang)
    sin_ref[...] = jnp.sin(ang)


def qkv_kernel(s_ref, a_ref, w0, w1, w2, w3, cos_ref, sin_ref, qv_ref, kv_ref, w_t, w_all, *, hd):
    w4 = w0.shape[0]

    @pl.when(pl.program_id(0) == 0)
    def _():
        for j, w in enumerate((w0, w1, w2, w3)):
            part_of(w_all, j, w4)[...] = w[...]
        for r in range(0, w_all.shape[0], MT):
            w_t[:, r:r + MT] = w_all[r:r + MT, :].T

    qkv = dot(w_t[...], a_ref[...]).astype(BF).astype(F32)
    ct, st = cos_ref[...], sin_ref[...]
    hh = hd // 2

    def rot(base):
        u1, u2 = qkv[base:base + hh], qkv[base + hh:base + hd]
        return u1 * ct - u2 * st, u2 * ct + u1 * st

    for g in range(2):
        lo, hi = rot(g * hd)
        qv_ref[g * hd:g * hd + hh, :] = lo.astype(BF)
        qv_ref[g * hd + hh:(g + 1) * hd, :] = hi.astype(BF)
    v = qkv[3 * hd:]
    qv_ref[2 * hd:, :] = v.astype(BF)
    klo, khi = rot(2 * hd)
    kv_ref[:, :hh] = klo.T.astype(BF)
    kv_ref[:, hh:hd] = khi.T.astype(BF)
    kv_ref[:, hd:] = v.T.astype(BF)


def attn_kernel(lo_ref, full_ref, q_ref, k_ref, v_ref, pq_ref, pk_ref, o_ref, acc_ref, qq_ref, l_ref, vs_ref, f_ref, *, bq, bk, q_block0, scale):
    qb = q_block0 + pl.program_id(0)
    hd = k_ref.shape[1]
    groups = q_ref.shape[0] // hd
    lo, full = lo_ref[qb], full_ref[qb]
    diag = (qb * bq) // bk
    last = ((qb + 1) * bq + bk - 1) // bk

    @pl.when(pl.program_id(0) == 0)
    def _():
        top = jnp.max(jnp.abs(v_ref[...].astype(F32)), axis=0, keepdims=True)
        top = jnp.max(top, axis=1, keepdims=True)
        f_ref[...] = jnp.broadcast_to(jnp.where(top > BIG, SHRINK, 1.0), f_ref.shape)
        vs_ref[...] = (v_ref[...].astype(F32) * f_ref[0:1, 0:1]).astype(BF)

    for g in range(groups):
        qq_ref[:, g * bq:(g + 1) * bq] = q_ref[g * hd:(g + 1) * hd, :]
    l_ref[...] = jnp.zeros_like(l_ref)
    acc_ref[...] = jnp.zeros_like(acc_ref)

    def step(j, masked):
        rows = pl.ds(pl.multiple_of(j * bk, bk), bk)
        kb = k_ref[rows, :]
        vb = vs_ref[:, rows]
        for n in range(0, groups * bq, MT):
            cols = slice(n, n + MT)
            s = dot(kb, qq_ref[:, cols])
            p = jnp.exp2(jnp.tanh(s * (scale / SOFT_CAP)) * (SOFT_CAP * LOG2E))
            if masked:
                dif = pq_ref[:, n % bq:n % bq + MT] - pk_ref[rows, :]
                p = jnp.where((dif >= 0) & (dif < WINDOW_LEN), p, 0.0)
            l_ref[:, cols] += jnp.sum(p, axis=0, keepdims=True)
            acc_ref[:, cols] += dot(vb, p.astype(BF))

    mid = jnp.maximum(jnp.minimum(full, diag), lo)

    def masked_step(j, _):
        step(j, True)
        return 0

    def full_step(j, _):
        step(j, False)
        return 0

    lax.fori_loop(lo, mid, masked_step, 0)
    lax.fori_loop(mid, diag, full_step, 0)
    lax.fori_loop(jnp.maximum(diag, mid), last, masked_step, 0)
    for g in range(groups):
        cols = slice(g * bq, (g + 1) * bq)
        o_ref[g * hd:(g + 1) * hd, :] = (acc_ref[:, cols] / l_ref[:, cols] / f_ref[0:1, 0:1]).astype(BF)


def norm_to_m(m_ref, blocks, r, g_ref, col, mt_ref):
    w4 = blocks[0].shape[0]
    for j, b in enumerate(blocks):
        part_of(mt_ref, j, w4)[...] = (b * r * part_of(g_ref, j, w4)[:, col:col + 1]).astype(BF)
    for i in range(0, mt_ref.shape[0], MT):
        m_ref[:, i:i + MT] = mt_ref[i:i + MT, :].T


def proj_kernel(s_ref, o_own, o_c, o_y, o_yc, b0, b0c, b1, b1c, b2, b2c, b3, b3c, x0, x1, x2, x3, g_ref, *rest, width):
    h_ref, m_ref, o_all, mt_ref, w_ref, w_sem = rest[-6:]
    cps = [pltpu.make_async_copy(b, w_ref.at[i], w_sem.at[i]) for i, b in enumerate((b0, b2, b0c, b2c, b1, b3, b1c, b3c))]
    for cp in cps:
        cp.start()
    c = s_ref[2]
    gw = o_own.shape[0]
    first = c == 0
    pairs = ((o_own, o_c), (o_y, o_yc))
    for i, (a, b) in enumerate([t for q in pairs for t in (q, q[::-1])]):
        part_of(o_all, i, gw)[...] = jnp.where(first, a[...], b[...])
    w4 = x0.shape[0]
    heads = b0.shape[0]
    o = o_all[...]
    att = []
    for j in range(4):
        two = (2 * j, 2 * j + 1)
        for i in two:
            cps[i].wait()
        w = hcat([w_ref[i, h] for i in two for h in range(heads)])
        att.append(dot(w, o).astype(BF).astype(F32))
    r = inv_rms(att, width)
    hs = []
    for j, (t, xr) in enumerate(zip(att, (x0, x1, x2, x3))):
        h = (xr[...].astype(F32) + t * r * part_of(g_ref, j, w4)[:, 1:2]).astype(BF)
        part_of(h_ref, j, w4)[...] = h
        hs.append(h.astype(F32))
    norm_to_m(m_ref, hs, inv_rms(hs, width), g_ref, 2, mt_ref)


def renorm_kernel(s_ref, h_ref, g_ref, *rest, width):
    m_ref, mt_ref = rest[-2:]
    w4 = h_ref.shape[0] // 4
    hs = [part_of(h_ref, j, w4)[...].astype(F32) for j in (2, 3, 0, 1)]
    norm_to_m(m_ref, hs, inv_rms(hs, width), g_ref, 2, mt_ref)


def gate_up_kernel(s_ref, *refs, groups, sets, steps):
    ms, ws, z_ref = refs[:groups], refs[groups:-1], refs[-1]
    n = z_ref.shape[1]
    per = len(ws) // sets
    ws = [w[...] for w in ws]
    if sets > 1:
        early = pl.program_id(1) < steps
        ws = [jnp.where(early, a, b) for a, b in zip(ws[:per], ws[per:])]
    w = hcat([vcat(ws[:per // 2]), vcat(ws[per // 2:])])
    for r in range(0, z_ref.shape[0], MT):
        m = [t[r:r + MT, :] for t in ms]
        m = jnp.where(pl.program_id(0) == 0, m[0], m[1]) if groups > 1 else m[0]
        t = dot(m, w)
        g, u = t[:, :n].astype(BF).astype(F32), t[:, n:].astype(BF).astype(F32)
        z_ref[r:r + MT, :] = (jax.nn.gelu(g, approximate=True) * u).astype(BF)


def down_y_kernel(s_ref, zw, zf, d0, d1, d2, d3, acc_ref, d_ref):
    w4 = d0.shape[0]
    n = zw.shape[0]

    @pl.when(pl.program_id(0) == 0)
    def _():
        for j, dd in enumerate((d0, d1, d2, d3)):
            part_of(d_ref, j, w4)[...] = dd[...]

    z = vcat([zw[...], zf[...]])
    for j in range(4):
        t = dot_nt(d_ref[j * w4:(j + 1) * w4, :], z)
        for q in range(n // CH):
            acc_ref[q, j * w4:(j + 1) * w4, :CH] = t[:, q * CH:(q + 1) * CH]
            acc_ref[q, j * w4:(j + 1) * w4, CH:] = t[:, n + q * CH:n + (q + 1) * CH]


def tail_kernel(part, zwa, zfa, zb, d0, d1, d2, d3, dt, hw0, hw1, hf0, hf1, g_ref, out,
                d_ref, z_ref, g_buf, p_ref, lo_ref, hi_ref, rec_ref, h_ref, sqs_ref, sqr_ref, sqo_ref,
                d_sem, z_sem, p_sem, h_sem, loc_sem, rs_s, rs_r, sq_s, sq_r, dt_s, dt_r, out_s, out_r, *, width, chunks):
    w4 = d0.shape[0]
    w2 = 2 * w4
    f8 = zwa.shape[1]
    y = lax.axis_index('tp')
    dm = lax.axis_index('dm')
    x, c = dm // 2, lax.rem(dm, 2)
    px = {'dp': 0, 'tp': y, 'dm': (1 - x) * 2 + c}
    pc = {'dp': 0, 'tp': y, 'dm': x * 2 + 1 - c}
    py = {'dp': 0, 'tp': 1 - y, 'dm': dm}
    pyc = {'dp': 0, 'tp': 1 - y, 'dm': x * 2 + 1 - c}

    def local(src, dst, sem):
        return pltpu.make_async_copy(src, dst, sem)

    def remote(src, dst, s_sem, r_sem, dev):
        return pltpu.make_async_remote_copy(src_ref=src, dst_ref=dst, send_sem=s_sem, recv_sem=r_sem, device_id=dev, device_id_type=pl.DeviceIdType.MESH)

    d_cp = [local(dd, d_ref.at[j * w4:(j + 1) * w4, :dd.shape[1]], d_sem.at[j]) for j, dd in enumerate((d0, d1, d2, d3))]
    g_cp = local(part_of(g_ref, 0, w2), g_buf, d_sem.at[4])
    late = slice(d0.shape[1], d_ref.shape[1])
    dt_y = remote(dt.at[:, late], d_ref.at[:w4, late], dt_s.at[0], dt_r.at[0], py)
    dt_c = remote(d_ref.at[:w4, late], d_ref.at[w4:w2, late], dt_s.at[1], dt_r.at[1], pc)

    def z_cp(p):
        srcs = ((zwa, 0), (zb, 0), (zfa, 0), (zb, zwa.shape[0]))
        return [local(src.at[pl.ds(at + p * CH, CH), :], z_ref.at[p, i // 2 * CH:(i // 2 + 1) * CH, i % 2 * f8:(i % 2 + 1) * f8], z_sem.at[p, i]) for i, (src, at) in enumerate(srcs)]

    def p_cp(p):
        return local(part.at[p], p_ref.at[lax.rem(p, 3)], p_sem.at[lax.rem(p, 3)])

    per = hw0.shape[1] // CH
    h_cp = []
    for q in range(chunks):
        k, l = q // per, (q % per) * CH
        h_cp.append(local((hw0, hw1)[k].at[0:w2, l:l + CH], h_ref.at[q, :, 0:CH], h_sem.at[q, 0]))
        h_cp.append(local((hf0, hf1)[k].at[w2:2 * w2, l:l + CH], h_ref.at[q, :, CH:2 * CH], h_sem.at[q, 1]))

    def start(cps):
        for cp in cps:
            cp.start()

    start(z_cp(0) + [d_cp[2], p_cp(0), d_cp[3]])

    bar = pltpu.get_barrier_semaphore()
    for dev in (px, pc, py, pyc):
        pl.semaphore_signal(bar, inc=1, device_id=dev, device_id_type=pl.DeviceIdType.MESH)
    pl.semaphore_wait(bar, 4)
    dt_y.start()

    def rs(p, i):
        rws = slice(i * w4, (i + 1) * w4)
        return remote(hi_ref.at[p, rws], rec_ref.at[p, rws], rs_s.at[p, i], rs_r.at[p, i], px)

    def sq(p):
        return remote(sqs_ref.at[p], sqr_ref.at[p], sq_s.at[p], sq_r.at[p], px)

    def outs(p):
        k, l = p // per, lax.rem(p, per)
        res = []
        for i, pr in enumerate((x, 1 - x)):
            col = pl.multiple_of(((pr * 2 + k) * 4 + 2 * y + c) * (per * CH) + l * CH, CH)
            mine = rec_ref.at[p, 0:w4, i * CH:(i + 1) * CH]
            give = rec_ref.at[p, w4:w2, i * CH:(i + 1) * CH]
            dst = out.at[:, pl.ds(col, CH)]
            res.append((local(mine, dst, loc_sem.at[p, i]), remote(mine, dst, out_s.at[p, i, 0], out_r.at[p, i, 0], py),
                        remote(give, dst, out_s.at[p, i, 1], out_r.at[p, i, 1], pyc), remote(give, dst, out_s.at[p, i, 2], out_r.at[p, i, 2], pc)))
        return res

    def block(p, j):
        return dot_nt(part_of(d_ref, j, w4)[...], z_ref[p]) + p_ref[lax.rem(p, 3), j * w4:(j + 1) * w4, :]

    def upper(p, first=False):
        p_cp(p).wait()
        for cp in z_cp(p):
            cp.wait()
        if first:
            p_cp(1).start()
        else:
            @pl.when(p + 1 < chunks)
            def _():
                p_cp(p + 1).start()
        for i in range(2):
            if first:
                d_cp[2 + i].wait()
            t = block(p, 2 + i).astype(BF)
            hi_ref[p, i * w4:(i + 1) * w4, :CH] = t[:, CH:]
            hi_ref[p, i * w4:(i + 1) * w4, CH:] = t[:, :CH]
            if first or i == 0:
                rs(p, i).start()

    def lower(p, first=False):
        for j in range(2):
            if first:
                d_cp[j].wait()
            lo_ref[p, j * w4:(j + 1) * w4, :] = block(p, j)

    def add(p):
        for i in range(2):
            rs(p, i).wait_recv()
        t = (lo_ref[p] + rec_ref[p].astype(F32)).astype(BF)
        rec_ref[p] = t
        t = t.astype(F32)
        v = jnp.broadcast_to(jnp.sum(t * t, axis=0, keepdims=True), sqo_ref.shape)
        sqo_ref[...] = v
        sqs_ref[p, :, :CH] = v[:, CH:]
        sqs_ref[p, :, CH:] = v[:, :CH]
        sq(p).start()

    def finish(p):
        sq(p).wait_recv()
        r = lax.rsqrt((sqo_ref[...] + sqr_ref[p]) / width + NORM_EPS)[0:1]
        g = g_buf[:, 3:4]
        rec_ref[p] = (h_ref[p].astype(F32) + rec_ref[p].astype(F32) * r * g).astype(BF)
        for group in outs(p):
            for cp in group[1:] + group[:1]:
                cp.start()

    upper(0, True)
    start(d_cp[:2] + z_cp(1))
    upper(1)
    start([g_cp] + h_cp)
    for q in range(2, chunks):
        start(z_cp(q))
    dt_y.wait_recv()
    dt_c.start()
    dt_c.wait_recv()
    lower(0, True)
    lower(1)
    for cp in [g_cp] + h_cp:
        cp.wait()

    def body(p, _):
        add(p)
        rs(p + 1, 1).start()
        upper(p + 2)
        finish(p)
        lower(p + 2)
        return 0

    lax.fori_loop(0, chunks - 2, body, 0)
    add(chunks - 2)
    rs(chunks - 1, 1).start()
    finish(chunks - 2)
    add(chunks - 1)
    finish(chunks - 1)

    def drain(p, _):
        for i in range(2):
            rs(p, i).wait_send()
        sq(p).wait_send()
        for group in outs(p):
            group[0].wait()
            for cp in group[1:]:
                cp.wait()
        return 0

    lax.fori_loop(0, chunks, drain, 0)
    dt_y.wait_send()
    dt_c.wait_send()


def kv_out_kernel(s_ref, kv0, kv1, *rest, extra):
    if extra:
        rest[-1][...] = rest[0][...]
    k_ref, v_ref = rest[-2 - extra:][:2]
    hd = k_ref.shape[2]
    first = s_ref[2] == 0
    a, b = kv0[...], kv1[...]
    two = jnp.where(first, a, b), jnp.where(first, b, a)
    for ref, at in ((k_ref, 0), (v_ref, hd)):
        ref[...] = hcat([t[:, at:at + hd] for t in two]).reshape(ref.shape)


def solution(mesh):
    tp_size, dm_size = mesh.shape['tp'], mesh.shape['dm']

    def flip(bits):
        return [(i, i ^ bits) for i in range(mesh.size)]

    C, X, Y = 1, 2, dm_size
    PX, PY, PC, PXC, PYC = flip(X), flip(Y), flip(C), flip(X | C), flip(Y | C)

    def send(a, perm):
        return lax.ppermute(a, ('tp', 'dm'), perm)

    def layer(tokens, positions, n1, wq, wk, wv, wo, n2, n3, wg, wu, wd, n4):
        y = lax.axis_index('tp')
        d = lax.axis_index('dm')
        x, c = d // 2, d % 2
        xo, yo, co = 1 - x, 1 - y, 1 - c
        rows, w4 = tokens.shape
        D = w4 * dm_size
        S = positions.shape[1]
        hd = wq.shape[2]
        scale = (D / (wq.shape[1] * tp_size)) ** -0.5
        gw = 2 * hd
        half = S // 2
        quarter = half // 4
        F4 = wg.shape[1] // 2
        scal = jnp.stack([x, y, c]).astype(jnp.int32)

        def take(a, start, size, axis=0):
            return lax.dynamic_slice_in_dim(a, start, size, axis)

        def take_cols(a, start, size):
            return take(a, start, size, 1)

        sets = range(2)
        dma = pltpu.SemaphoreType.DMA
        xt = tokens.T

        gains = jnp.stack([n1, n2, n3, n4])
        gall = hcat([gains, send(gains, PC), send(gains, PX), send(gains, PXC)])
        gcol = (1.0 + gall.astype(F32)).T

        oh = half // 2
        rx = [send(take_cols(xt, xo * S + k * half + y * oh, oh), PX) for k in sets]
        own_p = take_cols(xt, x * S, S)
        own_c = send(own_p, PC)
        ry = [send(rx[k], PY) for k in sets]
        rxc = [send(rx[k], PC) for k in sets]
        ryc = [send(ry[k], PC) for k in sets]

        def group_cols(g):
            return hcat([take_cols(w, n * g, n).reshape(w4, n * hd) for w, n in ((wq, 2), (wk, 1), (wv, 1))])

        wq_own, wq_oth = group_cols(c), group_cols(co)
        wqs = [wq_own, send(wq_oth, PC), send(wq_own, PX), send(wq_oth, PXC)]

        wot = jnp.transpose(wo, (0, 2, 1))
        B0 = wot
        B1 = send(B0, PX)
        B2 = send(B0, PY)
        B3 = send(B1, PY)
        Bs = []
        for b in (B0, B1, B2, B3):
            Bs += [b, send(b, PC)]

        def gather(own, oth, far=None):
            r1 = send(oth, PX)
            s0 = send(own if far is None else far, PY)
            s1 = send(r1, PY)
            ty = [own, send(own, PC), r1, send(r1, PC)]
            to = [s0, send(s0, PC), s1, send(s1, PC)]
            return ty, to

        F8 = F4 // 2

        def gu_half(xx, at):
            return hcat([take_cols(w, xx * F4 + at, F8) for w in (wg, wu)])

        gu = {ab: gather(gu_half(x, at), gu_half(xo, at)) for ab, at in (('a', 0), ('b', F8))}
        wdt = wd.T
        dw_own, dw_oth = (take_cols(wdt, xx * F4, F4) for xx in (x, xo))
        dw_early = dw_own[:, :F4 - KT]
        dn_y, dn_o = gather(dw_own, dw_oth, dw_early)

        pos = take(positions, x, 1)[0]
        inv_freq = ROPE_BASE ** (-2.0 * jnp.arange(hd // 2, dtype=F32) / hd)
        pos_row, pos_col = pos.reshape(1, S), pos.reshape(S, 1)

        tile = 512
        nt = half // tile
        per_half = nt // 2
        nb = S // tile
        cos_t, sin_t = call(
            rope_kernel, (nb,), [pl.BlockSpec((1, tile), by_col), whole(hd // 2, 1)], [pl.BlockSpec((hd // 2, tile), by_col)] * 2,
            [f32(hd // 2, S)] * 2, flops=hd * S * nb)(scal, pos_row, inv_freq.reshape(hd // 2, 1))
        a_all = []
        for k in sets:
            a_all = [call(
                functools.partial(norm_kernel, width=D, per_half=per_half), (nt,),
                [cols(w4, tile, lambda i, s, k=k: s[0] * nb + k * nt + i), cols(w4, tile, lambda i, s, k=k: k * nt + i)] + [cols(w4, tile, lambda i, s: i % per_half)] * 4 + [whole(D, 4)] + [ANY] * k,
                cols(D, tile, lambda i, s, k=k: k * nt + i), bf(D, S),
                flops=D * S, aliases={8: 0} if k else None)(scal, xt, own_c, rx[k], rxc[k], ry[k], ryc[k], gcol, *a_all)]
        qv, kv = call(
            functools.partial(qkv_kernel, hd=hd), (nb,),
            [pl.BlockSpec((D, tile), by_col)] + [whole(w4, 2 * gw)] * 4 + [pl.BlockSpec((hd // 2, tile), by_col)] * 2,
            [pl.BlockSpec((gw + hd, tile), by_col), pl.BlockSpec((tile, gw), by_row)],
            [bf(gw + hd, S), bf(S, gw)],
            [vmem(2 * gw, D), vmem(D, 2 * gw)],
            flops=D * gw * S)(scal, *a_all, *wqs, cos_t, sin_t)

        bq = bk = tile
        bq2 = 2 * bq
        first_q, last_q = pos[0::bq][:, None], pos[bq - 1::bq][:, None]
        first_k, last_k = pos[0::bk][None, :], pos[bk - 1::bk][None, :]
        lo_t = jnp.sum((first_q - last_k >= WINDOW_LEN).astype(jnp.int32), axis=1)
        full_t = jnp.sum((last_q - first_k >= WINDOW_LEN).astype(jnp.int32), axis=1)
        h_own, m_own = [], []
        heads = wo.shape[0]
        qn = half // quarter
        mine = lambda i, s: 2 * s[1] + s[2]
        for k in sets:
            q0 = k * half // bq
            kl = (k + 1) * half
            o = call(
                functools.partial(attn_kernel, bq=bq, bk=bk, q_block0=q0, scale=scale), (half // bq,),
                [
                    cols(gw, bq, lambda i, *_, q0=q0: q0 + i), cols(kl, hd, fixed), pl.BlockSpec((hd, kl), lambda i, *_: (gw // hd, 0)),
                    cols(1, bq, lambda i, *_, q0=q0: q0 + i), cols(kl, 1, fixed),
                ],
                pl.BlockSpec((gw, bq), by_col),
                bf(gw, half),
                [vmem(hd, bq2, dtype=F32), vmem(hd, bq2), vmem(1, bq2, dtype=F32), vmem(hd, kl), vmem(8, CH, dtype=F32)],
                prefetch=2, flops=gw * half * kl)(lo_t, full_t, qv, kv, qv, pos_row, pos_col)
            mc = 2 * y + co
            my, myc = 2 * yo + c, 2 * yo + co
            o_c = send(take_cols(o, mc * quarter, quarter), PC)
            o_y = send(take_cols(o, my * quarter, quarter), PY)
            o_yc = send(take_cols(o, myc * quarter, quarter), PYC)
            h, m = call(
                functools.partial(proj_kernel, width=D), (1,),
                [cols(gw, quarter, mine)] + [whole(gw, quarter)] * 3 + [ANY] * 8 + [
                    cols(w4, quarter, lambda i, s, k=k: (2 * s[0] + k) * qn + mine(i, s)), cols(w4, quarter, lambda i, s, k=k: k * qn + mine(i, s)),
                    *[cols(w4, quarter, lambda i, s: s[2])] * 2,
                    whole(D, 4)] + [ANY] * k,
                [whole(D, quarter), pl.BlockSpec((quarter, D), lambda i, s, k=k: (k, 0))],
                [bf(D, quarter), bf(oh, D)],
                [vmem(4 * gw, quarter), vmem(D, quarter), vmem(len(Bs), heads, w4, hd), dma((len(Bs),))],
                flops=D * gw * half, aliases={18: 1} if k else None)(scal, o, o_c, o_y, o_yc, *Bs, xt, own_c, rx[k], rxc[k], gcol, *m_own)
            h_own.append(h)
            m_own = [m]
        h_for = [send(h_own[k], PX) for k in sets]
        m_for = []
        for k in sets:
            m_for = [call(
                functools.partial(renorm_kernel, width=D), (1,), [whole(D, quarter), whole(D, 4)] + [ANY] * k,
                pl.BlockSpec((quarter, D), lambda i, s, k=k: (k, 0)), bf(oh, D), [vmem(D, quarter)],
                flops=D * half, aliases={3: 0} if k else None)(scal, h_for[k], gcol, *m_for)]

        ft = 384
        nf = F8 // ft

        def gated(ms, wsets):
            groups, sets = len(ms), len(wsets)
            early = lambda i: jnp.minimum(i, nf - 1)
            late = lambda i: jnp.maximum(i - nf, 0)
            specs = [cols(w4, ft, lambda j, i, s, at=at, up=up: up * nf + at(i)) for at in (early, late)[:sets] for up in range(2) for _ in wsets[0]]
            return call(
                functools.partial(gate_up_kernel, groups=groups, sets=sets, steps=nf), (groups, sets * nf),
                [whole(oh, D)] * groups + specs, pl.BlockSpec((oh, ft), lambda j, i, s: (j, i)),
                bf(oh * groups, sets * F8), flops=D * F4 * half * groups * sets)(scal, *ms, *[t for w in wsets for t in w + w])

        gua, gub = gu['a'], gu['b']
        near = [t[0] for t in (gua, gub)]
        zy_own = gated(m_own, near)
        zy_for = gated(m_for, near)
        za_own = gated(m_own, [gua[1]])
        za_for = gated(m_for, [gua[1]])
        zb = gated(m_own + m_for, [gub[1]])
        w2 = 2 * w4
        chunks = oh // CH
        yt = 2 * CH
        part = call(
            down_y_kernel, (oh // yt,), [pl.BlockSpec((yt, F4), by_row)] * 2 + [whole(w4, F4)] * 4,
            pl.BlockSpec((2, D, yt), lambda i, s: (i, 0, 0)), f32(chunks, D, yt),
            [vmem(D, F4)], flops=D * F4 * half)(scal, zy_own, zy_for, *dn_y)
        out = pl.pallas_call(
            functools.partial(tail_kernel, width=D, chunks=chunks),
            out_shape=bf(w4, rows),
            in_specs=[ANY] * 14,
            out_specs=ANY,
            scratch_shapes=[
                vmem(D, F4), vmem(chunks, yt, F4), vmem(w2, 4, dtype=F32), vmem(3, D, yt, dtype=F32), vmem(chunks, w2, yt, dtype=F32),
                *[vmem(chunks, w2, yt)] * 3, *[vmem(chunks, 8, yt, dtype=F32)] * 2, vmem(8, yt, dtype=F32),
                dma((5,)), dma((chunks, 4)), dma((3,)), *[dma((chunks, 2))] * 4, *[dma((chunks,))] * 2, *[dma((2,))] * 2, *[dma((chunks, 2, 3))] * 2],
            cost_estimate=pl.CostEstimate(flops=D * F4 * S, bytes_accessed=D * rows, transcendentals=0),
            compiler_params=pltpu.CompilerParams(vmem_limit_bytes=VM, collective_id=0, has_side_effects=True),
            name='tail',
        )(part, za_own, za_for, zb, *dn_o, dw_own, *h_own, *h_for, gcol)
        kv_c = send(kv, PC)
        kv_sets = jnp.split(kv, [S - oh])
        kv_x = [send(t, PX) for t in kv_sets]
        kv_xc = [send(kv_x[k], PC) for k in sets]
        kv_spec = pl.BlockSpec((tile, gw), by_row)
        kv_outs = []
        for i, (t, tc, n, base) in enumerate(((kv, kv_c, nb, 0), (kv_x[0], kv_xc[0], nb - per_half, 0), (kv_x[1], kv_xc[1], per_half, nb - per_half))):
            extra = i == 2
            at = lambda j, s, i=i, base=base: ((1 - s[0] if i else s[0]) * nb + base + j, 0, 0)
            cspec = [cols(w4, rows // n, lambda i, s: i)] * extra
            kv_outs = call(
                functools.partial(kv_out_kernel, extra=int(extra)), (n,), [kv_spec] * 2 + cspec + [ANY] * len(kv_outs),
                [pl.BlockSpec((tile, 2, hd), at)] * 2 + cspec, [bf(rows, 2, hd)] * 2 + [bf(w4, rows)] * extra,
                flops=rows * gw, aliases={3 + extra: 0, 4 + extra: 1} if i else None)(scal, t, tc, *[out] * extra, *kv_outs)
        k_out, v_out, out = kv_outs
        return out.T, k_out, v_out

    width_spec = P('dm')
    in_specs = (P('dp', 'dm'), P('dp', None), width_spec, P('dm', 'tp', None), P('dm', 'tp', None), P('dm', 'tp', None), P('tp', None, 'dm'), width_spec, width_spec, P('dm', 'tp'), P('dm', 'tp'), P('tp', 'dm'), width_spec)
    out_specs = (P('dp', 'dm'), P('dp', 'tp', None), P('dp', 'tp', None))
    return jax.shard_map(layer, mesh=mesh, in_specs=in_specs, out_specs=out_specs, check_vma=False)
```

```python
import functools

import jax
import jax.numpy as jnp
from jax import lax
from jax.experimental import pallas as pl
from jax.experimental.pallas import tpu as pltpu
from jax.sharding import PartitionSpec as P


NORM_EPS = 1e-6
SOFT_CAP = 50.0
ROPE_BASE = 10000.0
WINDOW_LEN = 4096
LOG2E = 1.4426950408889634
BF = jnp.bfloat16
F32 = jnp.float32
VM = 63 * 1024 * 1024
CH = 128
BIG = 2.0 ** 40
SHRINK = 2.0 ** -88
MT = 256
KT = 256
ANY = pl.BlockSpec(memory_space=pl.ANY)


vcat = functools.partial(jnp.concatenate, axis=0)
hcat = functools.partial(jnp.concatenate, axis=1)
by_col = lambda i, *_: (0, i)
by_row = lambda i, *_: (i, 0)
fixed = lambda *_: 0


def dot(a, b):
    return jnp.dot(a, b, preferred_element_type=F32)


def dot_nt(a, b):
    return lax.dot_general(a, b, (((1,), (1,)), ((), ())), preferred_element_type=F32)


def cols(height, wide, at):
    return pl.BlockSpec((height, wide), lambda i, *s: (0, at(i, *s)))


def bf(*shape):
    return jax.ShapeDtypeStruct(shape, BF)


def f32(*shape):
    return jax.ShapeDtypeStruct(shape, F32)


def vmem(*shape, dtype=BF):
    return pltpu.VMEM(shape, dtype)


def whole(*shape):
    return pl.BlockSpec(shape, lambda *_: (0,) * len(shape))


def inv_rms(blocks, width):
    sq = sum(jnp.sum(jnp.square(b.astype(F32)), axis=0, keepdims=True) for b in blocks)
    return lax.rsqrt(sq / width + NORM_EPS)


def part_of(ref, j, size):
    return ref.at[j * size:(j + 1) * size, :]


def call(kernel, grid, in_specs, out_specs, out_shape, scratch=(), prefetch=1, flops=0, nbytes=0, aliases=None):
    return pl.pallas_call(
        kernel,
        out_shape=out_shape,
        grid_spec=pltpu.PrefetchScalarGridSpec(num_scalar_prefetch=prefetch, grid=grid, in_specs=in_specs, out_specs=out_specs, scratch_shapes=list(scratch)),
        cost_estimate=pl.CostEstimate(flops=flops, bytes_accessed=nbytes, transcendentals=0),
        compiler_params=pltpu.CompilerParams(vmem_limit_bytes=VM),
        input_output_aliases=aliases or {},
    )


def norm_kernel(s_ref, own, own_c, rx, rxc, ry, ryc, g_ref, *rest, width, per_half):
    a_ref = rest[-1]
    w4 = own.shape[0]
    mine = (pl.program_id(0) // per_half) == s_ref[1]
    blocks = [own[...], own_c[...], jnp.where(mine, rx[...], ry[...]), jnp.where(mine, rxc[...], ryc[...])]
    r = inv_rms(blocks, width)
    for j, b in enumerate(blocks):
        part_of(a_ref, j, w4)[...] = (b.astype(F32) * r * part_of(g_ref, j, w4)[:, 0:1]).astype(BF)


def rope_kernel(s_ref, pos_ref, freq_ref, cos_ref, sin_ref):
    ang = freq_ref[...] * pos_ref[...].astype(F32)
    cos_ref[...] = jnp.cos(ang)
    sin_ref[...] = jnp.sin(ang)


def qkv_kernel(s_ref, a_ref, w0, w1, w2, w3, cos_ref, sin_ref, qv_ref, kv_ref, w_t, w_all, *, hd):
    w4 = w0.shape[0]

    @pl.when(pl.program_id(0) == 0)
    def _():
        for j, w in enumerate((w0, w1, w2, w3)):
            part_of(w_all, j, w4)[...] = w[...]
        for r in range(0, w_all.shape[0], MT):
            w_t[:, r:r + MT] = w_all[r:r + MT, :].T

    qkv = dot(w_t[...], a_ref[...]).astype(BF).astype(F32)
    ct, st = cos_ref[...], sin_ref[...]
    hh = hd // 2

    def rot(base):
        u1, u2 = qkv[base:base + hh], qkv[base + hh:base + hd]
        return u1 * ct - u2 * st, u2 * ct + u1 * st

    for g in range(2):
        lo, hi = rot(g * hd)
        qv_ref[g * hd:g * hd + hh, :] = lo.astype(BF)
        qv_ref[g * hd + hh:(g + 1) * hd, :] = hi.astype(BF)
    v = qkv[3 * hd:]
    qv_ref[2 * hd:, :] = v.astype(BF)
    klo, khi = rot(2 * hd)
    kv_ref[:, :hh] = klo.T.astype(BF)
    kv_ref[:, hh:hd] = khi.T.astype(BF)
    kv_ref[:, hd:] = v.T.astype(BF)


def attn_kernel(lo_ref, full_ref, q_ref, k_ref, v_ref, pq_ref, pk_ref, o_ref, acc_ref, qq_ref, l_ref, vs_ref, f_ref, *, bq, bk, q_block0, scale):
    qb = q_block0 + pl.program_id(0)
    hd = k_ref.shape[1]
    groups = q_ref.shape[0] // hd
    lo, full = lo_ref[qb], full_ref[qb]
    diag = (qb * bq) // bk
    last = ((qb + 1) * bq + bk - 1) // bk

    @pl.when(pl.program_id(0) == 0)
    def _():
        top = jnp.max(jnp.abs(v_ref[...].astype(F32)), axis=0, keepdims=True)
        top = jnp.max(top, axis=1, keepdims=True)
        f_ref[...] = jnp.broadcast_to(jnp.where(top > BIG, SHRINK, 1.0), f_ref.shape)
        vs_ref[...] = (v_ref[...].astype(F32) * f_ref[0:1, 0:1]).astype(BF)

    for g in range(groups):
        qq_ref[:, g * bq:(g + 1) * bq] = q_ref[g * hd:(g + 1) * hd, :]
    l_ref[...] = jnp.zeros_like(l_ref)
    acc_ref[...] = jnp.zeros_like(acc_ref)

    def step(j, masked):
        rows = pl.ds(pl.multiple_of(j * bk, bk), bk)
        kb = k_ref[rows, :]
        vb = vs_ref[:, rows]
        for n in range(0, groups * bq, MT):
            cols = slice(n, n + MT)
            s = dot(kb, qq_ref[:, cols])
            p = jnp.exp2(jnp.tanh(s * (scale / SOFT_CAP)) * (SOFT_CAP * LOG2E))
            if masked:
                dif = pq_ref[:, n % bq:n % bq + MT] - pk_ref[rows, :]
                p = jnp.where((dif >= 0) & (dif < WINDOW_LEN), p, 0.0)
            l_ref[:, cols] += jnp.sum(p, axis=0, keepdims=True)
            acc_ref[:, cols] += dot(vb, p.astype(BF))

    mid = jnp.maximum(jnp.minimum(full, diag), lo)

    def masked_step(j, _):
        step(j, True)
        return 0

    def full_step(j, _):
        step(j, False)
        return 0

    lax.fori_loop(lo, mid, masked_step, 0)
    lax.fori_loop(mid, diag, full_step, 0)
    lax.fori_loop(jnp.maximum(diag, mid), last, masked_step, 0)
    for g in range(groups):
        cols = slice(g * bq, (g + 1) * bq)
        o_ref[g * hd:(g + 1) * hd, :] = (acc_ref[:, cols] / l_ref[:, cols] / f_ref[0:1, 0:1]).astype(BF)


def norm_to_m(m_ref, blocks, r, g_ref, col, mt_ref):
    w4 = blocks[0].shape[0]
    for j, b in enumerate(blocks):
        part_of(mt_ref, j, w4)[...] = (b * r * part_of(g_ref, j, w4)[:, col:col + 1]).astype(BF)
    for i in range(0, mt_ref.shape[0], MT):
        m_ref[:, i:i + MT] = mt_ref[i:i + MT, :].T


def proj_kernel(s_ref, o_own, o_c, o_y, o_yc, b0, b0c, b1, b1c, b2, b2c, b3, b3c, x0, x1, x2, x3, g_ref, *rest, width):
    h_ref, m_ref, o_all, mt_ref, w_ref, w_sem = rest[-6:]
    cps = [pltpu.make_async_copy(b, w_ref.at[i], w_sem.at[i]) for i, b in enumerate((b0, b2, b0c, b2c, b1, b3, b1c, b3c))]
    for cp in cps:
        cp.start()
    c = s_ref[2]
    gw = o_own.shape[0]
    first = c == 0
    pairs = ((o_own, o_c), (o_y, o_yc))
    for i, (a, b) in enumerate([t for q in pairs for t in (q, q[::-1])]):
        part_of(o_all, i, gw)[...] = jnp.where(first, a[...], b[...])
    w4 = x0.shape[0]
    heads = b0.shape[0]
    o = o_all[...]
    att = []
    for j in range(4):
        two = (2 * j, 2 * j + 1)
        for i in two:
            cps[i].wait()
        w = hcat([w_ref[i, h] for i in two for h in range(heads)])
        att.append(dot(w, o).astype(BF).astype(F32))
    r = inv_rms(att, width)
    hs = []
    for j, (t, xr) in enumerate(zip(att, (x0, x1, x2, x3))):
        h = (xr[...].astype(F32) + t * r * part_of(g_ref, j, w4)[:, 1:2]).astype(BF)
        part_of(h_ref, j, w4)[...] = h
        hs.append(h.astype(F32))
    norm_to_m(m_ref, hs, inv_rms(hs, width), g_ref, 2, mt_ref)


def renorm_kernel(s_ref, h_ref, g_ref, *rest, width):
    m_ref, mt_ref = rest[-2:]
    w4 = h_ref.shape[0] // 4
    hs = [part_of(h_ref, j, w4)[...].astype(F32) for j in (2, 3, 0, 1)]
    norm_to_m(m_ref, hs, inv_rms(hs, width), g_ref, 2, mt_ref)


def gate_up_kernel(s_ref, *refs, groups, sets, steps):
    ms, ws, z_ref = refs[:groups], refs[groups:-1], refs[-1]
    n = z_ref.shape[1]
    per = len(ws) // sets
    ws = [w[...] for w in ws]
    if sets > 1:
        early = pl.program_id(1) < steps
        ws = [jnp.where(early, a, b) for a, b in zip(ws[:per], ws[per:])]
    w = hcat([vcat(ws[:per // 2]), vcat(ws[per // 2:])])
    for r in range(0, z_ref.shape[0], MT):
        m = [t[r:r + MT, :] for t in ms]
        m = jnp.where(pl.program_id(0) == 0, m[0], m[1]) if groups > 1 else m[0]
        t = dot(m, w)
        g, u = t[:, :n].astype(BF).astype(F32), t[:, n:].astype(BF).astype(F32)
        z_ref[r:r + MT, :] = (jax.nn.gelu(g, approximate=True) * u).astype(BF)


def down_y_kernel(s_ref, zw, zf, d0, d1, d2, d3, acc_ref):
    w4 = d0.shape[0]
    n = zw.shape[0]
    z = vcat([zw[...], zf[...]])
    for j, dd in enumerate((d0, d1, d2, d3)):
        t = dot_nt(dd[...], z)
        for q in range(n // CH):
            acc_ref[q, j * w4:(j + 1) * w4, :CH] = t[:, q * CH:(q + 1) * CH]
            acc_ref[q, j * w4:(j + 1) * w4, CH:] = t[:, n + q * CH:n + (q + 1) * CH]


def tail_kernel(part, zwa, zfa, zb, d0, d1, d2, d3, dt, hw0, hw1, hf0, hf1, g_ref, out,
                d_ref, z_ref, g_buf, p_ref, lo_ref, hi_ref, rec_ref, h_ref, sqs_ref, sqr_ref, sqo_ref,
                d_sem, z_sem, p_sem, h_sem, loc_sem, rs_s, rs_r, sq_s, sq_r, dt_s, dt_r, out_s, out_r, *, width, chunks):
    w4 = d0.shape[0]
    w2 = 2 * w4
    f8 = zwa.shape[1]
    y = lax.axis_index('tp')
    dm = lax.axis_index('dm')
    x, c = dm // 2, lax.rem(dm, 2)
    px = {'dp': 0, 'tp': y, 'dm': (1 - x) * 2 + c}
    pc = {'dp': 0, 'tp': y, 'dm': x * 2 + 1 - c}
    py = {'dp': 0, 'tp': 1 - y, 'dm': dm}
    pyc = {'dp': 0, 'tp': 1 - y, 'dm': x * 2 + 1 - c}

    def local(src, dst, sem):
        return pltpu.make_async_copy(src, dst, sem)

    def remote(src, dst, s_sem, r_sem, dev):
        return pltpu.make_async_remote_copy(src_ref=src, dst_ref=dst, send_sem=s_sem, recv_sem=r_sem, device_id=dev, device_id_type=pl.DeviceIdType.MESH)

    d_cp = [local(dd, d_ref.at[j * w4:(j + 1) * w4, :dd.shape[1]], d_sem.at[j]) for j, dd in enumerate((d0, d1, d2, d3))]
    g_cp = local(part_of(g_ref, 0, w2), g_buf, d_sem.at[4])
    late = slice(d0.shape[1], d_ref.shape[1])
    dt_y = remote(dt.at[:, late], d_ref.at[:w4, late], dt_s.at[0], dt_r.at[0], py)
    dt_c = remote(d_ref.at[:w4, late], d_ref.at[w4:w2, late], dt_s.at[1], dt_r.at[1], pc)

    def z_cp(p):
        srcs = ((zwa, 0), (zb, 0), (zfa, 0), (zb, zwa.shape[0]))
        return [local(src.at[pl.ds(at + p * CH, CH), :], z_ref.at[p, i // 2 * CH:(i // 2 + 1) * CH, i % 2 * f8:(i % 2 + 1) * f8], z_sem.at[p, i]) for i, (src, at) in enumerate(srcs)]

    def p_cp(p):
        return local(part.at[p], p_ref.at[lax.rem(p, 3)], p_sem.at[lax.rem(p, 3)])

    per = hw0.shape[1] // CH
    h_cp = []
    for q in range(chunks):
        k, l = q // per, (q % per) * CH
        h_cp.append(local((hw0, hw1)[k].at[0:w2, l:l + CH], h_ref.at[q, :, 0:CH], h_sem.at[q, 0]))
        h_cp.append(local((hf0, hf1)[k].at[w2:2 * w2, l:l + CH], h_ref.at[q, :, CH:2 * CH], h_sem.at[q, 1]))

    def start(cps):
        for cp in cps:
            cp.start()

    start(z_cp(0) + [d_cp[2], p_cp(0), d_cp[3]])

    bar = pltpu.get_barrier_semaphore()
    for dev in (px, pc, py, pyc):
        pl.semaphore_signal(bar, inc=1, device_id=dev, device_id_type=pl.DeviceIdType.MESH)
    pl.semaphore_wait(bar, 4)
    dt_y.start()

    def lanes(q):
        return pl.ds(pl.multiple_of(CH * (x + q - 2 * x * q), CH), CH)

    def away(q):
        return pl.ds(pl.multiple_of(CH - CH * (x + q - 2 * x * q), CH), CH)

    def rs(p, q):
        return remote(hi_ref.at[p, :, away(q)], rec_ref.at[p, :, away(q)], rs_s.at[p, q], rs_r.at[p, q], px)

    def sq(p, q):
        return remote(sqs_ref.at[p, q], sqr_ref.at[p, q], sq_s.at[p, q], sq_r.at[p, q], px)

    def outs(p, q):
        col = pl.multiple_of(((q * 2 + p // per) * 4 + 2 * y + c) * (per * CH) + lax.rem(p, per) * CH, CH)
        mine = rec_ref.at[p, :w4, lanes(q)]
        give = rec_ref.at[p, w4:, lanes(q)]
        dst = out.at[:, pl.ds(col, CH)]
        far = [remote(src, dst, out_s.at[p, q, i], out_r.at[p, q, i], dev) for i, (src, dev) in enumerate(((mine, py), (give, pyc), (give, pc)))]
        return far + [local(mine, dst, loc_sem.at[p, q])]

    def block(p, j):
        return dot_nt(part_of(d_ref, j, w4)[...], z_ref[p]) + p_ref[lax.rem(p, 3), j * w4:(j + 1) * w4, :]

    def upper(p, first=False):
        p_cp(p).wait()
        for cp in z_cp(p):
            cp.wait()
        if first:
            p_cp(1).start()
        else:
            @pl.when(p + 1 < chunks)
            def _():
                p_cp(p + 1).start()
        for i in range(2):
            if first:
                d_cp[2 + i].wait()
            t = block(p, 2 + i).astype(BF)
            hi_ref[p, i * w4:(i + 1) * w4, :CH] = t[:, CH:]
            hi_ref[p, i * w4:(i + 1) * w4, CH:] = t[:, :CH]

    def lower(p, first=False):
        for j in range(2):
            if first:
                d_cp[j].wait()
            lo_ref[p, j * w4:(j + 1) * w4, :] = block(p, j)

    def add(p, q):
        rs(p, q).wait_recv()
        at = lanes(q)
        t = (lo_ref[p, :, at] + rec_ref[p, :, at].astype(F32)).astype(BF)
        rec_ref[p, :, at] = t
        t = t.astype(F32)
        v = jnp.broadcast_to(jnp.sum(t * t, axis=0, keepdims=True), (8, CH))
        sqo_ref[q] = v
        sqs_ref[p, q] = v
        sq(p, q).start()

    def finish(p, q):
        sq(p, q).wait_recv()
        at = lanes(q)
        r = lax.rsqrt((sqo_ref[q] + sqr_ref[p, q]) / width + NORM_EPS)[0:1]
        rec_ref[p, :, at] = (h_ref[p, :, at].astype(F32) + rec_ref[p, :, at].astype(F32) * r * g_buf[:, 3:4]).astype(BF)
        start(outs(p, q))

    upper(0, True)
    start([rs(0, 0), rs(0, 1)])
    start(d_cp[:2] + z_cp(1))
    upper(1)
    start([g_cp] + h_cp)
    for q in range(2, chunks):
        start(z_cp(q))
    dt_y.wait_recv()
    dt_c.start()
    dt_c.wait_recv()
    lower(0, True)
    lower(1)
    for cp in [g_cp] + h_cp:
        cp.wait()

    def steps(p, more):
        for q in range(2):
            add(p, q)
            if more:
                rs(p + 1, q).start()
            if q:
                finish(p, 0)
            elif isinstance(p, int):
                finish(p - 1, 1)
            else:
                @pl.when(p > 0)
                def _():
                    finish(p - 1, 1)
            if not isinstance(p, int):
                (lower if q else upper)(p + 2)

    def body(p, _):
        steps(p, True)
        return 0

    lax.fori_loop(0, chunks - 2, body, 0)
    steps(chunks - 2, True)
    steps(chunks - 1, False)
    finish(chunks - 1, 1)

    def drain(p, _):
        for q in range(2):
            rs(p, q).wait_send()
            sq(p, q).wait_send()
            for cp in outs(p, q):
                cp.wait()
        return 0

    lax.fori_loop(0, chunks, drain, 0)
    dt_y.wait_send()
    dt_c.wait_send()


def kv_out_kernel(s_ref, kv0, kv1, *rest, extra):
    if extra:
        rest[-1][...] = rest[0][...]
    k_ref, v_ref = rest[-2 - extra:][:2]
    hd = k_ref.shape[2]
    first = s_ref[2] == 0
    a, b = kv0[...], kv1[...]
    two = jnp.where(first, a, b), jnp.where(first, b, a)
    for ref, at in ((k_ref, 0), (v_ref, hd)):
        ref[...] = hcat([t[:, at:at + hd] for t in two]).reshape(ref.shape)


def solution(mesh):
    tp_size, dm_size = mesh.shape['tp'], mesh.shape['dm']

    def flip(bits):
        return [(i, i ^ bits) for i in range(mesh.size)]

    C, X, Y = 1, 2, dm_size
    PX, PY, PC, PXC, PYC = flip(X), flip(Y), flip(C), flip(X | C), flip(Y | C)

    def send(a, perm):
        return lax.ppermute(a, ('tp', 'dm'), perm)

    def layer(tokens, positions, n1, wq, wk, wv, wo, n2, n3, wg, wu, wd, n4):
        y = lax.axis_index('tp')
        d = lax.axis_index('dm')
        x, c = d // 2, d % 2
        xo, yo, co = 1 - x, 1 - y, 1 - c
        rows, w4 = tokens.shape
        D = w4 * dm_size
        S = positions.shape[1]
        hd = wq.shape[2]
        scale = (D / (wq.shape[1] * tp_size)) ** -0.5
        gw = 2 * hd
        half = S // 2
        quarter = half // 4
        F4 = wg.shape[1] // 2
        scal = jnp.stack([x, y, c]).astype(jnp.int32)

        def take(a, start, size, axis=0):
            return lax.dynamic_slice_in_dim(a, start, size, axis)

        def take_cols(a, start, size):
            return take(a, start, size, 1)

        sets = range(2)
        dma = pltpu.SemaphoreType.DMA
        xt = tokens.T

        gains = jnp.stack([n1, n2, n3, n4])
        gall = hcat([gains, send(gains, PC), send(gains, PX), send(gains, PXC)])
        gcol = (1.0 + gall.astype(F32)).T

        oh = half // 2
        rx = [send(take_cols(xt, xo * S + k * half + y * oh, oh), PX) for k in sets]
        own_p = take_cols(xt, x * S, S)
        own_c = send(own_p, PC)
        ry = [send(rx[k], PY) for k in sets]
        rxc = [send(rx[k], PC) for k in sets]
        ryc = [send(ry[k], PC) for k in sets]

        def group_cols(g):
            return hcat([take_cols(w, n * g, n).reshape(w4, n * hd) for w, n in ((wq, 2), (wk, 1), (wv, 1))])

        wq_own, wq_oth = group_cols(c), group_cols(co)
        wqs = [wq_own, send(wq_oth, PC), send(wq_own, PX), send(wq_oth, PXC)]

        wot = jnp.transpose(wo, (0, 2, 1))
        B0 = wot
        B1 = send(B0, PX)
        B2 = send(B0, PY)
        B3 = send(B1, PY)
        Bs = []
        for b in (B0, B1, B2, B3):
            Bs += [b, send(b, PC)]

        def gather(own, oth, far=None):
            r1 = send(oth, PX)
            s0 = send(own if far is None else far, PY)
            s1 = send(r1, PY)
            ty = [own, send(own, PC), r1, send(r1, PC)]
            to = [s0, send(s0, PC), s1, send(s1, PC)]
            return ty, to

        F8 = F4 // 2

        def gu_half(xx, at):
            return hcat([take_cols(w, xx * F4 + at, F8) for w in (wg, wu)])

        gu = {ab: gather(gu_half(x, at), gu_half(xo, at)) for ab, at in (('a', 0), ('b', F8))}
        wdt = wd.T
        dw_own, dw_oth = (take_cols(wdt, xx * F4, F4) for xx in (x, xo))
        dw_early = dw_own[:, :F4 - KT]
        dn_y, dn_o = gather(dw_own, dw_oth, dw_early)

        pos = take(positions, x, 1)[0]
        inv_freq = ROPE_BASE ** (-2.0 * jnp.arange(hd // 2, dtype=F32) / hd)
        pos_row, pos_col = pos.reshape(1, S), pos.reshape(S, 1)

        tile = 512
        nt = half // tile
        per_half = nt // 2
        nb = S // tile
        cos_t, sin_t = call(
            rope_kernel, (nb,), [pl.BlockSpec((1, tile), by_col), whole(hd // 2, 1)], [pl.BlockSpec((hd // 2, tile), by_col)] * 2,
            [f32(hd // 2, S)] * 2, flops=hd * S * nb)(scal, pos_row, inv_freq.reshape(hd // 2, 1))
        a_all = []
        for k in sets:
            a_all = [call(
                functools.partial(norm_kernel, width=D, per_half=per_half), (nt,),
                [cols(w4, tile, lambda i, s, k=k: s[0] * nb + k * nt + i), cols(w4, tile, lambda i, s, k=k: k * nt + i)] + [cols(w4, tile, lambda i, s: i % per_half)] * 4 + [whole(D, 4)] + [ANY] * k,
                cols(D, tile, lambda i, s, k=k: k * nt + i), bf(D, S),
                flops=D * S, aliases={8: 0} if k else None)(scal, xt, own_c, rx[k], rxc[k], ry[k], ryc[k], gcol, *a_all)]
        qv, kv = call(
            functools.partial(qkv_kernel, hd=hd), (nb,),
            [pl.BlockSpec((D, tile), by_col)] + [whole(w4, 2 * gw)] * 4 + [pl.BlockSpec((hd // 2, tile), by_col)] * 2,
            [pl.BlockSpec((gw + hd, tile), by_col), pl.BlockSpec((tile, gw), by_row)],
            [bf(gw + hd, S), bf(S, gw)],
            [vmem(2 * gw, D), vmem(D, 2 * gw)],
            flops=D * gw * S)(scal, *a_all, *wqs, cos_t, sin_t)

        bq = bk = tile
        bq2 = 2 * bq
        first_q, last_q = pos[0::bq][:, None], pos[bq - 1::bq][:, None]
        first_k, last_k = pos[0::bk][None, :], pos[bk - 1::bk][None, :]
        lo_t = jnp.sum((first_q - last_k >= WINDOW_LEN).astype(jnp.int32), axis=1)
        full_t = jnp.sum((last_q - first_k >= WINDOW_LEN).astype(jnp.int32), axis=1)
        h_own, m_own = [], []
        heads = wo.shape[0]
        qn = half // quarter
        mine = lambda i, s: 2 * s[1] + s[2]
        for k in sets:
            q0 = k * half // bq
            kl = (k + 1) * half
            o = call(
                functools.partial(attn_kernel, bq=bq, bk=bk, q_block0=q0, scale=scale), (half // bq,),
                [
                    cols(gw, bq, lambda i, *_, q0=q0: q0 + i), cols(kl, hd, fixed), pl.BlockSpec((hd, kl), lambda i, *_: (gw // hd, 0)),
                    cols(1, bq, lambda i, *_, q0=q0: q0 + i), cols(kl, 1, fixed),
                ],
                pl.BlockSpec((gw, bq), by_col),
                bf(gw, half),
                [vmem(hd, bq2, dtype=F32), vmem(hd, bq2), vmem(1, bq2, dtype=F32), vmem(hd, kl), vmem(8, CH, dtype=F32)],
                prefetch=2, flops=gw * half * kl)(lo_t, full_t, qv, kv, qv, pos_row, pos_col)
            mc = 2 * y + co
            my, myc = 2 * yo + c, 2 * yo + co
            o_c = send(take_cols(o, mc * quarter, quarter), PC)
            o_y = send(take_cols(o, my * quarter, quarter), PY)
            o_yc = send(take_cols(o, myc * quarter, quarter), PYC)
            h, m = call(
                functools.partial(proj_kernel, width=D), (1,),
                [cols(gw, quarter, mine)] + [whole(gw, quarter)] * 3 + [ANY] * 8 + [
                    cols(w4, quarter, lambda i, s, k=k: (2 * s[0] + k) * qn + mine(i, s)), cols(w4, quarter, lambda i, s, k=k: k * qn + mine(i, s)),
                    *[cols(w4, quarter, lambda i, s: s[2])] * 2,
                    whole(D, 4)] + [ANY] * k,
                [whole(D, quarter), pl.BlockSpec((quarter, D), lambda i, s, k=k: (k, 0))],
                [bf(D, quarter), bf(oh, D)],
                [vmem(4 * gw, quarter), vmem(D, quarter), vmem(len(Bs), heads, w4, hd), dma((len(Bs),))],
                flops=D * gw * half, aliases={18: 1} if k else None)(scal, o, o_c, o_y, o_yc, *Bs, xt, own_c, rx[k], rxc[k], gcol, *m_own)
            h_own.append(h)
            m_own = [m]
        h_for = [send(h_own[k], PX) for k in sets]
        m_for = []
        for k in sets:
            m_for = [call(
                functools.partial(renorm_kernel, width=D), (1,), [whole(D, quarter), whole(D, 4)] + [ANY] * k,
                pl.BlockSpec((quarter, D), lambda i, s, k=k: (k, 0)), bf(oh, D), [vmem(D, quarter)],
                flops=D * half, aliases={3: 0} if k else None)(scal, h_for[k], gcol, *m_for)]

        ft = 384
        nf = F8 // ft

        def gated(ms, wsets):
            groups, sets = len(ms), len(wsets)
            early = lambda i: jnp.minimum(i, nf - 1)
            late = lambda i: jnp.maximum(i - nf, 0)
            specs = [cols(w4, ft, lambda j, i, s, at=at, up=up: up * nf + at(i)) for at in (early, late)[:sets] for up in range(2) for _ in wsets[0]]
            return call(
                functools.partial(gate_up_kernel, groups=groups, sets=sets, steps=nf), (groups, sets * nf),
                [whole(oh, D)] * groups + specs, pl.BlockSpec((oh, ft), lambda j, i, s: (j, i)),
                bf(oh * groups, sets * F8), flops=D * F4 * half * groups * sets)(scal, *ms, *[t for w in wsets for t in w + w])

        gua, gub = gu['a'], gu['b']
        near = [t[0] for t in (gua, gub)]
        zy_own = gated(m_own, near)
        zy_for = gated(m_for, near)
        za_own = gated(m_own, [gua[1]])
        za_for = gated(m_for, [gua[1]])
        zb = gated(m_own + m_for, [gub[1]])
        w2 = 2 * w4
        chunks = oh // CH
        yt = 2 * CH
        part = call(
            down_y_kernel, (oh // yt,), [pl.BlockSpec((yt, F4), by_row)] * 2 + [whole(w4, F4)] * 4,
            pl.BlockSpec((2, D, yt), lambda i, s: (i, 0, 0)), f32(chunks, D, yt),
            flops=D * F4 * half)(scal, zy_own, zy_for, *dn_y)
        out = pl.pallas_call(
            functools.partial(tail_kernel, width=D, chunks=chunks),
            out_shape=bf(w4, rows),
            in_specs=[ANY] * 14,
            out_specs=ANY,
            scratch_shapes=[
                vmem(D, F4), vmem(chunks, yt, F4), vmem(w2, 4, dtype=F32), vmem(3, D, yt, dtype=F32), vmem(chunks, w2, yt, dtype=F32),
                *[vmem(chunks, w2, yt)] * 3, *[vmem(chunks, 2, 8, CH, dtype=F32)] * 2, vmem(2, 8, CH, dtype=F32),
                dma((5,)), dma((chunks, 4)), dma((3,)), *[dma((chunks, 2))] * 6, *[dma((2,))] * 2, *[dma((chunks, 2, 3))] * 2],
            cost_estimate=pl.CostEstimate(flops=D * F4 * S, bytes_accessed=D * rows, transcendentals=0),
            compiler_params=pltpu.CompilerParams(vmem_limit_bytes=VM, collective_id=0, has_side_effects=True),
            name='tail',
        )(part, za_own, za_for, zb, *dn_o, dw_own, *h_own, *h_for, gcol)
        kv_c = send(kv, PC)
        kv_sets = jnp.split(kv, [S - oh])
        kv_x = [send(t, PX) for t in kv_sets]
        kv_xc = [send(kv_x[k], PC) for k in sets]
        kv_outs = []
        most = nb - per_half
        for i, (t, tc, base, last) in enumerate(((kv, kv_c, 0, nb), (kv_x[0], kv_xc[0], 0, most // 2), (kv_x[0], kv_xc[0], most // 2, most), (kv_x[1], kv_xc[1], most, nb))):
            extra = i == 3
            n = last - base
            kv_spec = pl.BlockSpec((tile, gw), lambda j, s, at=0 if extra else base: (at + j, 0))
            at = lambda j, s, i=i, base=base: ((1 - s[0] if i else s[0]) * nb + base + j, 0, 0)
            cspec = [cols(w4, rows // n, lambda i, s: i)] * extra
            kv_outs = call(
                functools.partial(kv_out_kernel, extra=int(extra)), (n,), [kv_spec] * 2 + cspec + [ANY] * len(kv_outs),
                [pl.BlockSpec((tile, 2, hd), at)] * 2 + cspec, [bf(rows, 2, hd)] * 2 + [bf(w4, rows)] * extra,
                flops=rows * gw, aliases={3 + extra: 0, 4 + extra: 1} if i else None)(scal, t, tc, *[out] * extra, *kv_outs)
        k_out, v_out, out = kv_outs
        return out.T, k_out, v_out

    width_spec = P('dm')
    in_specs = (P('dp', 'dm'), P('dp', None), width_spec, P('dm', 'tp', None), P('dm', 'tp', None), P('dm', 'tp', None), P('tp', None, 'dm'), width_spec, width_spec, P('dm', 'tp'), P('dm', 'tp'), P('tp', 'dm'), width_spec)
    out_specs = (P('dp', 'dm'), P('dp', 'tp', None), P('dp', 'tp', None))
    return jax.shard_map(layer, mesh=mesh, in_specs=in_specs, out_specs=out_specs, check_vma=False)
```

```python
import functools

import jax
import jax.numpy as jnp
from jax import lax
from jax.experimental import pallas as pl
from jax.experimental.pallas import tpu as pltpu
from jax.sharding import PartitionSpec as P


NORM_EPS = 1e-6
SOFT_CAP = 50.0
ROPE_BASE = 10000.0
WINDOW_LEN = 4096
LOG2E = 1.4426950408889634
BF = jnp.bfloat16
F32 = jnp.float32
VM = 63 * 1024 * 1024
CH = 128
BIG = 2.0 ** 40
SHRINK = 2.0 ** -88
MT = 256
KT = 256
KA = 768
ANY = pl.BlockSpec(memory_space=pl.ANY)


vcat = functools.partial(jnp.concatenate, axis=0)
hcat = functools.partial(jnp.concatenate, axis=1)
by_col = lambda i, *_: (0, i)
by_row = lambda i, *_: (i, 0)
fixed = lambda *_: 0


def dot(a, b):
    return jnp.dot(a, b, preferred_element_type=F32)


def dot_nt(a, b):
    return lax.dot_general(a, b, (((1,), (1,)), ((), ())), preferred_element_type=F32)


def cols(height, wide, at):
    return pl.BlockSpec((height, wide), lambda i, *s: (0, at(i, *s)))


def bf(*shape):
    return jax.ShapeDtypeStruct(shape, BF)


def f32(*shape):
    return jax.ShapeDtypeStruct(shape, F32)


def vmem(*shape, dtype=BF):
    return pltpu.VMEM(shape, dtype)


def whole(*shape):
    return pl.BlockSpec(shape, lambda *_: (0,) * len(shape))


def inv_rms(blocks, width):
    sq = sum(jnp.sum(jnp.square(b.astype(F32)), axis=0, keepdims=True) for b in blocks)
    return lax.rsqrt(sq / width + NORM_EPS)


def part_of(ref, j, size):
    return ref.at[j * size:(j + 1) * size, :]


def block_of(j, size):
    return pl.ds(pl.multiple_of(j * size, size), size)


def loop(n, body, init=0):
    return lax.fori_loop(0, n, body, init)


def call(kernel, grid, in_specs, out_specs, out_shape, scratch=(), prefetch=1, flops=0, nbytes=0, aliases=None):
    return pl.pallas_call(
        kernel,
        out_shape=out_shape,
        grid_spec=pltpu.PrefetchScalarGridSpec(num_scalar_prefetch=prefetch, grid=grid, in_specs=in_specs, out_specs=out_specs, scratch_shapes=list(scratch)),
        cost_estimate=pl.CostEstimate(flops=flops, bytes_accessed=nbytes, transcendentals=0),
        compiler_params=pltpu.CompilerParams(vmem_limit_bytes=VM),
        input_output_aliases=aliases or {},
    )


def norm_kernel(s_ref, own, own_c, rx, rxc, ry, ryc, g_ref, *rest, width, per_half):
    a_ref = rest[-1]
    w4 = own.shape[0]
    mine = (pl.program_id(0) // per_half) == s_ref[1]
    blocks = [own[...], own_c[...], jnp.where(mine, rx[...], ry[...]), jnp.where(mine, rxc[...], ryc[...])]
    r = inv_rms(blocks, width)
    for j, b in enumerate(blocks):
        part_of(a_ref, j, w4)[...] = (b.astype(F32) * r * part_of(g_ref, j, w4)[:, 0:1]).astype(BF)


def rope_kernel(s_ref, pos_ref, freq_ref, cos_ref, sin_ref):
    ang = freq_ref[...] * pos_ref[...].astype(F32)
    cos_ref[...] = jnp.cos(ang)
    sin_ref[...] = jnp.sin(ang)


def split_kernel(s_ref, wq, wk, wv, own_ref, oth_ref):
    rows, _, hd = wk.shape
    q, k, v = (w[...].reshape(rows, w.shape[1] * hd) for w in (wq, wk, wv))
    two = [hcat([q[:, 2 * g * hd:2 * (g + 1) * hd], k[:, g * hd:(g + 1) * hd], v[:, g * hd:(g + 1) * hd]]) for g in range(2)]
    first = s_ref[2] == 0
    own_ref[...] = jnp.where(first, *two)
    oth_ref[...] = jnp.where(first, *two[::-1])


def qkv_kernel(s_ref, a_ref, w0, w1, w2, w3, cos_ref, sin_ref, qv_ref, kv_ref, w_t, w_all, w_sem, *, hd):
    w4 = w0.shape[0]

    @pl.when(pl.program_id(0) == 0)
    def _():
        cps = [pltpu.make_async_copy(w, part_of(w_all, j, w4), w_sem.at[j]) for j, w in enumerate((w0, w1, w2, w3))]
        for cp in cps:
            cp.start()
        for cp in cps:
            cp.wait()
        to_rows(w_t, w_all)

    hh = hd // 2

    def part(n, _):
        cols = block_of(n, MT)
        qkv = dot(w_t[...], a_ref[:, cols]).astype(BF).astype(F32)
        ct, st = cos_ref[:, cols], sin_ref[:, cols]

        def rot(base):
            u1, u2 = qkv[base:base + hh], qkv[base + hh:base + hd]
            return u1 * ct - u2 * st, u2 * ct + u1 * st

        for g in range(2):
            lo, hi = rot(g * hd)
            qv_ref[g * hd:g * hd + hh, cols] = lo.astype(BF)
            qv_ref[g * hd + hh:(g + 1) * hd, cols] = hi.astype(BF)
        v = qkv[3 * hd:]
        qv_ref[2 * hd:, cols] = v.astype(BF)
        klo, khi = rot(2 * hd)
        kv_ref[cols, :hh] = klo.T.astype(BF)
        kv_ref[cols, hh:hd] = khi.T.astype(BF)
        kv_ref[cols, hd:] = v.T.astype(BF)
        return 0

    loop(a_ref.shape[1] // MT, part)


def attn_kernel(lo_ref, full_ref, q_ref, k_ref, v_ref, pq_ref, pk_ref, o_ref, acc_ref, qq_ref, l_ref, vs_ref, f_ref, *, bq, bk, q_block0, scale):
    qb = q_block0 + pl.program_id(0)
    hd = k_ref.shape[1]
    groups = q_ref.shape[0] // hd
    lo, full = lo_ref[qb], full_ref[qb]
    diag = (qb * bq) // bk
    last = ((qb + 1) * bq + bk - 1) // bk

    @pl.when(pl.program_id(0) == 0)
    def _():
        top = jnp.max(jnp.abs(v_ref[...].astype(F32)), axis=0, keepdims=True)
        top = jnp.max(top, axis=1, keepdims=True)
        f_ref[...] = jnp.broadcast_to(jnp.where(top > BIG, SHRINK, 1.0), f_ref.shape)
        vs_ref[...] = (v_ref[...].astype(F32) * f_ref[0:1, 0:1]).astype(BF)

    for g in range(groups):
        qq_ref[:, g * bq:(g + 1) * bq] = q_ref[g * hd:(g + 1) * hd, :]
    l_ref[...] = jnp.zeros_like(l_ref)
    acc_ref[...] = jnp.zeros_like(acc_ref)

    def step(j, masked):
        rows = block_of(j, bk)

        def part(n, _):
            cols = block_of(n, MT)
            s = dot(k_ref[rows, :], qq_ref[:, cols])
            p = jnp.exp2(jnp.tanh(s * (scale / SOFT_CAP)) * (SOFT_CAP * LOG2E))
            if masked:
                dif = pq_ref[:, block_of(lax.rem(n, bq // MT), MT)] - pk_ref[rows, :]
                p = jnp.where((dif >= 0) & (dif < WINDOW_LEN), p, 0.0)
            l_ref[:, cols] += jnp.sum(p, axis=0, keepdims=True)
            acc_ref[:, cols] += dot(vs_ref[:, rows], p.astype(BF))
            return 0

        lax.fori_loop(0, groups * bq // MT, part, 0, unroll=2)

    mid = jnp.maximum(jnp.minimum(full, diag), lo)
    edge = jnp.maximum(diag, mid)

    def masked_step(i, _):
        j = lo + i
        step(jnp.where(j < mid, j, j - mid + edge), True)
        return 0

    def full_step(j, _):
        step(j, False)
        return 0

    lax.fori_loop(0, mid - lo + last - edge, masked_step, 0)
    lax.fori_loop(mid, diag, full_step, 0)
    for g in range(groups):
        cols = slice(g * bq, (g + 1) * bq)
        o_ref[g * hd:(g + 1) * hd, :] = (acc_ref[:, cols] / l_ref[:, cols] / f_ref[0:1, 0:1]).astype(BF)


def to_rows(m_ref, mt_ref):
    def turn(i, _):
        at = block_of(i, MT)
        m_ref[:, at] = mt_ref[at, :].T
        return 0

    loop(mt_ref.shape[0] // MT, turn)


def sum_sq(t):
    return jnp.sum(t * t, axis=0, keepdims=True)


def proj_kernel(s_ref, o_own, o_c, o_y, o_yc, b0, b0c, b1, b1c, b2, b2c, b3, b3c, x0, x1, x2, x3, g_ref, *rest, width):
    h_ref, m_ref, o_all, mt_ref, w_ref, x_ref, att_ref, w_sem = rest[-8:]
    for i, b in enumerate((b0, b2, b0c, b2c, b1, b3, b1c, b3c)):
        pltpu.make_async_copy(b, w_ref.at[i], w_sem.at[i]).start()
    first = s_ref[2] == 0
    gw = o_own.shape[0]
    pairs = ((o_own, o_c), (o_y, o_yc))
    for i, (a, b) in enumerate([t for q in pairs for t in (q, q[::-1])]):
        part_of(o_all, i, gw)[...] = jnp.where(first, a[...], b[...])
    for j, t in enumerate((x0, x1, x2, x3)):
        x_ref[j] = t[...]
    w4 = x0.shape[0]
    heads = b0.shape[0]
    n = x_ref.shape[0]
    zero = jnp.zeros((1, m_ref.shape[0]), F32)

    def product(j, sq):
        two = (2 * j, 2 * j + 1)
        for i in two:
            pltpu.make_async_copy(b0, w_ref.at[i], w_sem.at[i]).wait()
        t = dot(hcat([w_ref[i, h] for i in two for h in range(heads)]), o_all[...]).astype(BF).astype(F32)
        att_ref[j] = t
        return sq + sum_sq(t)

    r = lax.rsqrt(loop(n, product, zero) / width + NORM_EPS)

    def residual(j, sq):
        at = block_of(j, w4)
        h = (x_ref[j].astype(F32) + att_ref[j] * r * g_ref[at, 1:2]).astype(BF)
        h_ref[at, :] = h
        h = h.astype(F32)
        att_ref[j] = h
        return sq + sum_sq(h)

    r3 = lax.rsqrt(loop(n, residual, zero) / width + NORM_EPS)

    def scaled(j, _):
        at = block_of(j, w4)
        mt_ref[at, :] = (att_ref[j] * r3 * g_ref[at, 2:3]).astype(BF)
        return 0

    loop(n, scaled)
    to_rows(m_ref, mt_ref)


def renorm_kernel(s_ref, h_ref, g_ref, *rest, width):
    m_ref, mt_ref = rest[-2:]
    n = 4
    w4 = h_ref.shape[0] // n

    def theirs(j):
        return h_ref[block_of(lax.rem(j + 2, n), w4), :].astype(F32)

    r = lax.rsqrt(loop(n, lambda j, sq: sq + sum_sq(theirs(j)), jnp.zeros((1, h_ref.shape[1]), F32)) / width + NORM_EPS)

    def scaled(j, _):
        at = block_of(j, w4)
        mt_ref[at, :] = (theirs(j) * r * g_ref[at, 2:3]).astype(BF)
        return 0

    loop(n, scaled)
    to_rows(m_ref, mt_ref)


def gate_up_kernel(s_ref, *refs, groups, sets, steps):
    ms, ws, z_ref = refs[:groups], refs[groups:-1], refs[-1]
    n = z_ref.shape[1]
    per = len(ws) // sets
    ws = [w[...] for w in ws]
    if sets > 1:
        early = pl.program_id(1) < steps
        ws = [jnp.where(early, a, b) for a, b in zip(ws[:per], ws[per:])]
    w = hcat([vcat(ws[:per // 2]), vcat(ws[per // 2:])])
    for r in range(0, z_ref.shape[0], MT):
        m = [t[r:r + MT, :] for t in ms]
        m = jnp.where(pl.program_id(0) == 0, m[0], m[1]) if groups > 1 else m[0]
        t = dot(m, w)
        g, u = t[:, :n].astype(BF).astype(F32), t[:, n:].astype(BF).astype(F32)
        z_ref[r:r + MT, :] = (jax.nn.gelu(g, approximate=True) * u).astype(BF)


def down_y_kernel(s_ref, zw, zf, d0, d1, d2, d3, acc_ref, d_ref):
    w4 = d0.shape[0]
    n = zw.shape[0]

    @pl.when(pl.program_id(0) == 0)
    def _():
        for j, dd in enumerate((d0, d1, d2, d3)):
            part_of(d_ref, j, w4)[...] = dd[...]

    z = vcat([zw[...], zf[...]])

    def rows(j, _):
        at = block_of(j, w4)
        t = dot_nt(d_ref[at, :], z)
        for q in range(n // CH):
            acc_ref[q, at, :CH] = t[:, q * CH:(q + 1) * CH]
            acc_ref[q, at, CH:] = t[:, n + q * CH:n + (q + 1) * CH]
        return 0

    loop(4, rows)


def tail_kernel(part, zwa, zfa, zb, d0, d1, d2, d3, e0, e1, dt, hw0, hw1, hf0, hf1, g_ref, out,
                d_ref, z_ref, g_buf, p_ref, lo_ref, hi_ref, rec_ref, h_ref, sqs_ref, sqr_ref, sqo_ref,
                d_sem, z_sem, p_sem, h_sem, loc_sem, rs_s, rs_r, sq_s, sq_r, dt_s, dt_r, out_s, out_r, *, width, chunks):
    w4 = d0.shape[0]
    w2 = 2 * w4
    f8 = zwa.shape[1]
    y = lax.axis_index('tp')
    dm = lax.axis_index('dm')
    x, c = dm // 2, lax.rem(dm, 2)
    px = {'dp': 0, 'tp': y, 'dm': (1 - x) * 2 + c}
    pc = {'dp': 0, 'tp': y, 'dm': x * 2 + 1 - c}
    py = {'dp': 0, 'tp': 1 - y, 'dm': dm}
    pyc = {'dp': 0, 'tp': 1 - y, 'dm': x * 2 + 1 - c}

    def local(src, dst, sem):
        return pltpu.make_async_copy(src, dst, sem)

    def remote(src, dst, s_sem, r_sem, dev):
        return pltpu.make_async_remote_copy(src_ref=src, dst_ref=dst, send_sem=s_sem, recv_sem=r_sem, device_id=dev, device_id_type=pl.DeviceIdType.MESH)

    d_cp = [local(dd, d_ref.at[j * w4:(j + 1) * w4, :dd.shape[1]], d_sem.at[j]) for j, dd in enumerate((d0, d1, d2, d3))]
    cut = d0.shape[1]
    last = cut + e0.shape[1]
    e_cp = [local(dd, d_ref.at[j * w4:(j + 1) * w4, cut:last], d_sem.at[4 + j]) for j, dd in enumerate((e0, e1))]
    g_cp = local(part_of(g_ref, 0, w2), g_buf, d_sem.at[6])
    late = slice(last, d_ref.shape[1])
    dt_y = remote(dt.at[:, late], d_ref.at[:w4, late], dt_s.at[0], dt_r.at[0], py)
    dt_c = remote(d_ref.at[:w4, late], d_ref.at[w4:w2, late], dt_s.at[1], dt_r.at[1], pc)

    def z_cp(p):
        srcs = ((zwa, 0), (zb, 0), (zfa, 0), (zb, zwa.shape[0]))
        return [local(src.at[pl.ds(at + p * CH, CH), :], z_ref.at[p, i // 2 * CH:(i // 2 + 1) * CH, i % 2 * f8:(i % 2 + 1) * f8], z_sem.at[p, i]) for i, (src, at) in enumerate(srcs)]

    def p_cp(p):
        return local(part.at[p], p_ref.at[lax.rem(p, 3)], p_sem.at[lax.rem(p, 3)])

    per = hw0.shape[1] // CH
    h_cp = []
    for q in range(chunks):
        k, l = q // per, (q % per) * CH
        h_cp.append(local((hw0, hw1)[k].at[0:w2, l:l + CH], h_ref.at[q, :, 0:CH], h_sem.at[q, 0]))
        h_cp.append(local((hf0, hf1)[k].at[w2:2 * w2, l:l + CH], h_ref.at[q, :, CH:2 * CH], h_sem.at[q, 1]))

    def start(cps):
        for cp in cps:
            cp.start()

    start(z_cp(0) + [d_cp[2], p_cp(0), d_cp[3]] + z_cp(1))

    bar = pltpu.get_barrier_semaphore()
    for dev in (px, pc, py, pyc):
        pl.semaphore_signal(bar, inc=1, device_id=dev, device_id_type=pl.DeviceIdType.MESH)
    pl.semaphore_wait(bar, 4)
    dt_y.start()

    def lanes(q):
        return pl.ds(pl.multiple_of(CH * (x + q - 2 * x * q), CH), CH)

    def away(q):
        return pl.ds(pl.multiple_of(CH - CH * (x + q - 2 * x * q), CH), CH)

    def rs(p, q):
        return remote(hi_ref.at[p, :, away(q)], rec_ref.at[p, :, away(q)], rs_s.at[p, q], rs_r.at[p, q], px)

    def sq(p, q):
        return remote(sqs_ref.at[p, q], sqr_ref.at[p, q], sq_s.at[p, q], sq_r.at[p, q], px)

    def outs(p, q):
        col = pl.multiple_of(((q * 2 + p // per) * 4 + 2 * y + c) * (per * CH) + lax.rem(p, per) * CH, CH)
        mine = rec_ref.at[p, :w4, lanes(q)]
        give = rec_ref.at[p, w4:, lanes(q)]
        dst = out.at[:, pl.ds(col, CH)]
        far = [remote(src, dst, out_s.at[p, q, i], out_r.at[p, q, i], dev) for i, (src, dev) in enumerate(((mine, py), (give, pyc), (give, pc)))]
        return far + [local(mine, dst, loc_sem.at[p, q])]

    def block(p, j):
        at = block_of(j, w4)
        return dot_nt(d_ref[at, :], z_ref[p]) + p_ref[lax.rem(p, 3), at, :]

    def upper(p):
        p_cp(p).wait()
        for cp in z_cp(p):
            cp.wait()

        @pl.when(p + 1 < chunks)
        def _():
            p_cp(p + 1).start()

        def half(i, _):
            t = block(p, 2 + i).astype(BF)
            at = block_of(i, w4)
            hi_ref[p, at, :CH] = t[:, CH:]
            hi_ref[p, at, CH:] = t[:, :CH]
            return 0

        loop(2, half)

    def lower(p):
        def half(j, _):
            lo_ref[p, block_of(j, w4), :] = block(p, j)
            return 0

        loop(2, half)

    def add(p, q):
        rs(p, q).wait_recv()
        at = lanes(q)
        t = (lo_ref[p, :, at] + rec_ref[p, :, at].astype(F32)).astype(BF)
        rec_ref[p, :, at] = t
        t = t.astype(F32)
        v = jnp.broadcast_to(jnp.sum(t * t, axis=0, keepdims=True), (8, CH))
        sqo_ref[q] = v
        sqs_ref[p, q] = v
        sq(p, q).start()

    def finish(p, q):
        sq(p, q).wait_recv()
        at = lanes(q)
        r = lax.rsqrt((sqo_ref[q] + sqr_ref[p, q]) / width + NORM_EPS)[0:1]
        rec_ref[p, :, at] = (h_ref[p, :, at].astype(F32) + rec_ref[p, :, at].astype(F32) * r * g_buf[:, 3:4]).astype(BF)
        start(outs(p, q))

    for cp in d_cp[2:]:
        cp.wait()

    def first_upper(p, _):
        upper(p)

        @pl.when(p == 0)
        def _():
            start([rs(0, 0), rs(0, 1)])

        return 0

    loop(2, first_upper)
    start(d_cp[:2] + e_cp + [g_cp] + h_cp)
    for q in range(2, chunks):
        start(z_cp(q))
    dt_y.wait_recv()
    dt_c.start()
    for cp in d_cp[:2] + e_cp:
        cp.wait()
    dt_c.wait_recv()

    def first_lower(p, _):
        lower(p)
        return 0

    loop(2, first_lower)
    for cp in [g_cp] + h_cp:
        cp.wait()

    def body(p, _):
        for q in range(2):
            add(p, q)

            @pl.when(p + 1 < chunks)
            def _():
                rs(p + 1, q).start()

            if q:
                finish(p, 0)
            else:
                @pl.when(p > 0)
                def _():
                    finish(p - 1, 1)

            @pl.when(p + 2 < chunks)
            def _():
                (lower if q else upper)(p + 2)
        return 0

    loop(chunks, body)
    finish(chunks - 1, 1)

    def drain(p, _):
        for q in range(2):
            rs(p, q).wait_send()
            sq(p, q).wait_send()
            for cp in outs(p, q):
                cp.wait()
        return 0

    lax.fori_loop(0, chunks, drain, 0)
    dt_y.wait_send()
    dt_c.wait_send()


def kv_out_kernel(s_ref, kv0, kv1, *rest, extra):
    if extra:
        rest[-1][...] = rest[0][...]
    k_ref, v_ref = rest[-2 - extra:][:2]
    hd = k_ref.shape[2]
    first = s_ref[2] == 0
    a, b = kv0[...], kv1[...]
    two = jnp.where(first, a, b), jnp.where(first, b, a)
    for ref, at in ((k_ref, 0), (v_ref, hd)):
        ref[...] = hcat([t[:, at:at + hd] for t in two]).reshape(ref.shape)


def solution(mesh):
    tp_size, dm_size = mesh.shape['tp'], mesh.shape['dm']

    def flip(bits):
        return [(i, i ^ bits) for i in range(mesh.size)]

    C, X, Y = 1, 2, dm_size
    PX, PY, PC, PXC, PYC = flip(X), flip(Y), flip(C), flip(X | C), flip(Y | C)

    def send(a, perm):
        return lax.ppermute(a, ('tp', 'dm'), perm)

    def layer(tokens, positions, n1, wq, wk, wv, wo, n2, n3, wg, wu, wd, n4):
        y = lax.axis_index('tp')
        d = lax.axis_index('dm')
        x, c = d // 2, d % 2
        xo, yo, co = 1 - x, 1 - y, 1 - c
        rows, w4 = tokens.shape
        D = w4 * dm_size
        S = positions.shape[1]
        hd = wq.shape[2]
        scale = (D / (wq.shape[1] * tp_size)) ** -0.5
        gw = 2 * hd
        half = S // 2
        quarter = half // 4
        F4 = wg.shape[1] // 2
        scal = jnp.stack([x, y, c]).astype(jnp.int32)

        def take(a, start, size, axis=0):
            return lax.dynamic_slice_in_dim(a, start, size, axis)

        def take_cols(a, start, size):
            return take(a, start, size, 1)

        sets = range(2)
        dma = pltpu.SemaphoreType.DMA
        xt = tokens.T

        gains = jnp.stack([n1, n2, n3, n4])
        gall = hcat([gains, send(gains, PC), send(gains, PX), send(gains, PXC)])
        gcol = (1.0 + gall.astype(F32)).T

        oh = half // 2
        rx = [send(take_cols(xt, xo * S + k * half + y * oh, oh), PX) for k in sets]
        own_p = take_cols(xt, x * S, S)
        own_c = send(own_p, PC)
        ry = [send(rx[k], PY) for k in sets]
        rxc = [send(rx[k], PC) for k in sets]
        ryc = [send(ry[k], PC) for k in sets]

        wr = w4 // 9
        heads_of = lambda w: pl.BlockSpec((wr,) + w.shape[1:], lambda i, s: (i, 0, 0))
        wq_own, wq_oth = call(split_kernel, (9,), [heads_of(w) for w in (wq, wk, wv)], [pl.BlockSpec((wr, 2 * gw), by_row)] * 2, [bf(w4, 2 * gw)] * 2, flops=w4 * gw)(scal, wq, wk, wv)
        wqs = [wq_own, send(wq_oth, PC), send(wq_own, PX), send(wq_oth, PXC)]

        wot = jnp.transpose(wo, (0, 2, 1))
        B0 = wot
        B1 = send(B0, PX)
        B2 = send(B0, PY)
        B3 = send(B1, PY)
        Bs = []
        for b in (B0, B1, B2, B3):
            Bs += [b, send(b, PC)]

        def gather(own, oth, far=None):
            r1 = send(oth, PX)
            s0 = send(own if far is None else far, PY)
            s1 = send(r1, PY)
            ty = [own, send(own, PC), r1, send(r1, PC)]
            to = [s0, send(s0, PC), s1, send(s1, PC)]
            return ty, to

        F8 = F4 // 2

        def gu_half(xx, at):
            return hcat([take_cols(w, xx * F4 + at, F8) for w in (wg, wu)])

        gu = {ab: gather(gu_half(x, at), gu_half(xo, at)) for ab, at in (('a', 0), ('b', F8))}
        wdt = wd.T
        dw_own, dw_oth = (take_cols(wdt, xx * F4, F4) for xx in (x, xo))
        dw_a, dw_b = dw_own[:, :KA], dw_own[:, KA:F4 - KT]
        dn_y, dn_o = gather(dw_own, dw_oth, dw_a)
        dwb = send(dw_b, PY)
        dwb_c = send(dwb, PC)

        pos = take(positions, x, 1)[0]
        inv_freq = ROPE_BASE ** (-2.0 * jnp.arange(hd // 2, dtype=F32) / hd)
        pos_row, pos_col = pos.reshape(1, S), pos.reshape(S, 1)

        tile = 512
        nt = half // tile
        per_half = nt // 2
        nb = S // tile
        cos_t, sin_t = call(
            rope_kernel, (nb,), [pl.BlockSpec((1, tile), by_col), whole(hd // 2, 1)], [pl.BlockSpec((hd // 2, tile), by_col)] * 2,
            [f32(hd // 2, S)] * 2, flops=hd * S * nb)(scal, pos_row, inv_freq.reshape(hd // 2, 1))
        a_all = []
        for k in sets:
            a_all = [call(
                functools.partial(norm_kernel, width=D, per_half=per_half), (nt,),
                [cols(w4, tile, lambda i, s, k=k: s[0] * nb + k * nt + i), cols(w4, tile, lambda i, s, k=k: k * nt + i)] + [cols(w4, tile, lambda i, s: i % per_half)] * 4 + [whole(D, 4)] + [ANY] * k,
                cols(D, tile, lambda i, s, k=k: k * nt + i), bf(D, S),
                flops=D * S, aliases={8: 0} if k else None)(scal, xt, own_c, rx[k], rxc[k], ry[k], ryc[k], gcol, *a_all)]
        qv, kv = call(
            functools.partial(qkv_kernel, hd=hd), (nb,),
            [pl.BlockSpec((D, tile), by_col)] + [ANY] * 4 + [pl.BlockSpec((hd // 2, tile), by_col)] * 2,
            [pl.BlockSpec((gw + hd, tile), by_col), pl.BlockSpec((tile, gw), by_row)],
            [bf(gw + hd, S), bf(S, gw)],
            [vmem(2 * gw, D), vmem(D, 2 * gw), dma((4,))],
            flops=D * gw * S)(scal, *a_all, *wqs, cos_t, sin_t)

        bq = bk = tile
        bq2 = 2 * bq
        first_q, last_q = pos[0::bq][:, None], pos[bq - 1::bq][:, None]
        first_k, last_k = pos[0::bk][None, :], pos[bk - 1::bk][None, :]
        lo_t = jnp.sum((first_q - last_k >= WINDOW_LEN).astype(jnp.int32), axis=1)
        full_t = jnp.sum((last_q - first_k >= WINDOW_LEN).astype(jnp.int32), axis=1)
        h_own, m_own = [], []
        heads = wo.shape[0]
        qn = half // quarter
        mine = lambda i, s: 2 * s[1] + s[2]
        for k in sets:
            q0 = k * half // bq
            kl = (k + 1) * half
            o = call(
                functools.partial(attn_kernel, bq=bq, bk=bk, q_block0=q0, scale=scale), (half // bq,),
                [
                    cols(gw, bq, lambda i, *_, q0=q0: q0 + i), cols(kl, hd, fixed), pl.BlockSpec((hd, kl), lambda i, *_: (gw // hd, 0)),
                    cols(1, bq, lambda i, *_, q0=q0: q0 + i), cols(kl, 1, fixed),
                ],
                pl.BlockSpec((gw, bq), by_col),
                bf(gw, half),
                [vmem(hd, bq2, dtype=F32), vmem(hd, bq2), vmem(1, bq2, dtype=F32), vmem(hd, kl), vmem(8, CH, dtype=F32)],
                prefetch=2, flops=gw * half * kl)(lo_t, full_t, qv, kv, qv, pos_row, pos_col)
            mc = 2 * y + co
            my, myc = 2 * yo + c, 2 * yo + co
            o_c = send(take_cols(o, mc * quarter, quarter), PC)
            o_y = send(take_cols(o, my * quarter, quarter), PY)
            o_yc = send(take_cols(o, myc * quarter, quarter), PYC)
            h, m = call(
                functools.partial(proj_kernel, width=D), (1,),
                [cols(gw, quarter, mine)] + [whole(gw, quarter)] * 3 + [ANY] * 8 + [
                    cols(w4, quarter, lambda i, s, k=k: (2 * s[0] + k) * qn + mine(i, s)), cols(w4, quarter, lambda i, s, k=k: k * qn + mine(i, s)),
                    *[cols(w4, quarter, lambda i, s: s[2])] * 2,
                    whole(D, 4)] + [ANY] * k,
                [whole(D, quarter), pl.BlockSpec((quarter, D), lambda i, s, k=k: (k, 0))],
                [bf(D, quarter), bf(oh, D)],
                [vmem(4 * gw, quarter), vmem(D, quarter), vmem(len(Bs), heads, w4, hd), vmem(4, w4, quarter), vmem(4, w4, quarter, dtype=F32), dma((len(Bs),))],
                flops=D * gw * half, aliases={18: 1} if k else None)(scal, o, o_c, o_y, o_yc, *Bs, xt, own_c, rx[k], rxc[k], gcol, *m_own)
            h_own.append(h)
            m_own = [m]
        h_for = [send(h_own[k], PX) for k in sets]
        m_for = []
        for k in sets:
            m_for = [call(
                functools.partial(renorm_kernel, width=D), (1,), [whole(D, quarter), whole(D, 4)] + [ANY] * k,
                pl.BlockSpec((quarter, D), lambda i, s, k=k: (k, 0)), bf(oh, D), [vmem(D, quarter)],
                flops=D * half, aliases={3: 0} if k else None)(scal, h_for[k], gcol, *m_for)]

        def gated(ms, wsets, ft=128):
            nf = F8 // ft
            groups, sets = len(ms), len(wsets)
            early = lambda i: jnp.minimum(i, nf - 1)
            late = lambda i: jnp.maximum(i - nf, 0)
            specs = [cols(w4, ft, lambda j, i, s, at=at, up=up: up * nf + at(i)) for at in (early, late)[:sets] for up in range(2) for _ in wsets[0]]
            return call(
                functools.partial(gate_up_kernel, groups=groups, sets=sets, steps=nf), (groups, sets * nf),
                [whole(oh, D)] * groups + specs, pl.BlockSpec((oh, ft), lambda j, i, s: (j, i)),
                bf(oh * groups, sets * F8), flops=D * F4 * half * groups * sets)(scal, *ms, *[t for w in wsets for t in w + w])

        gua, gub = gu['a'], gu['b']
        near = [t[0] for t in (gua, gub)]
        zy_own = gated(m_own, near)
        zy_for = gated(m_for, near)
        za_own = gated(m_own, [gua[1]])
        za_for = gated(m_for, [gua[1]])
        zb = gated(m_own + m_for, [gub[1]], 3 * CH)
        w2 = 2 * w4
        chunks = oh // CH
        yt = 2 * CH
        part = call(
            down_y_kernel, (oh // yt,), [pl.BlockSpec((yt, F4), by_row)] * 2 + [whole(w4, F4)] * 4,
            pl.BlockSpec((2, D, yt), lambda i, s: (i, 0, 0)), f32(chunks, D, yt),
            [vmem(D, F4)], flops=D * F4 * half)(scal, zy_own, zy_for, *dn_y)
        out = pl.pallas_call(
            functools.partial(tail_kernel, width=D, chunks=chunks),
            out_shape=bf(w4, rows),
            in_specs=[ANY] * 16,
            out_specs=ANY,
            scratch_shapes=[
                vmem(D, F4), vmem(chunks, yt, F4), vmem(w2, 4, dtype=F32), vmem(3, D, yt, dtype=F32), vmem(chunks, w2, yt, dtype=F32),
                *[vmem(chunks, w2, yt)] * 3, *[vmem(chunks, 2, 8, CH, dtype=F32)] * 2, vmem(2, 8, CH, dtype=F32),
                dma((7,)), dma((chunks, 4)), dma((3,)), *[dma((chunks, 2))] * 6, *[dma((2,))] * 2, *[dma((chunks, 2, 3))] * 2],
            cost_estimate=pl.CostEstimate(flops=D * F4 * S, bytes_accessed=D * rows, transcendentals=0),
            compiler_params=pltpu.CompilerParams(vmem_limit_bytes=VM, collective_id=0, has_side_effects=True),
            name='tail',
        )(part, za_own, za_for, zb, *dn_o, dwb, dwb_c, dw_own, *h_own, *h_for, gcol)
        kv_c = send(kv, PC)
        most = nb - per_half
        kv_sets = jnp.split(kv, [most * tile // 2, most * tile])
        kv_x = [send(t, PX) for t in kv_sets]
        kv_xc = [send(t, PC) for t in kv_x]
        kt = tile // 2
        kv_outs = []
        for i, (t, tc, base, last) in enumerate(zip([kv] + kv_x, [kv_c] + kv_xc, (0, 0, most // 2, most), (nb, most // 2, most, nb))):
            extra = i == 3
            n = 2 * (last - base)
            kv_spec = pl.BlockSpec((kt, gw), by_row)
            at = lambda j, s, i=i, base=base: (((1 - s[0] if i else s[0]) * nb + base) * 2 + j, 0, 0)
            cspec = [cols(w4, rows // n, lambda i, s: i)] * extra
            kv_outs = call(
                functools.partial(kv_out_kernel, extra=int(extra)), (n,), [kv_spec] * 2 + cspec + [ANY] * len(kv_outs),
                [pl.BlockSpec((kt, 2, hd), at)] * 2 + cspec, [bf(rows, 2, hd)] * 2 + [bf(w4, rows)] * extra,
                flops=rows * gw, aliases={3 + extra: 0, 4 + extra: 1} if i else None)(scal, t, tc, *[out] * extra, *kv_outs)
        k_out, v_out, out = kv_outs
        return out.T, k_out, v_out

    width_spec = P('dm')
    in_specs = (P('dp', 'dm'), P('dp', None), width_spec, P('dm', 'tp', None), P('dm', 'tp', None), P('dm', 'tp', None), P('tp', None, 'dm'), width_spec, width_spec, P('dm', 'tp'), P('dm', 'tp'), P('tp', 'dm'), width_spec)
    out_specs = (P('dp', 'dm'), P('dp', 'tp', None), P('dp', 'tp', None))
    return jax.shard_map(layer, mesh=mesh, in_specs=in_specs, out_specs=out_specs, check_vma=False)
```

```python
import functools

import jax
import jax.numpy as jnp
from jax import lax
from jax.experimental import pallas as pl
from jax.experimental.pallas import tpu as pltpu
from jax.sharding import PartitionSpec as P


NORM_EPS = 1e-6
SOFT_CAP = 50.0
ROPE_BASE = 10000.0
WINDOW_LEN = 4096
LOG2E = 1.4426950408889634
BF = jnp.bfloat16
F32 = jnp.float32
VM = 63 * 1024 * 1024
CH = 128
BIG = 2.0 ** 40
SHRINK = 2.0 ** -88
MT = 256
KT = 384
KA = 768
ANY = pl.BlockSpec(memory_space=pl.ANY)


vcat = functools.partial(jnp.concatenate, axis=0)
hcat = functools.partial(jnp.concatenate, axis=1)
by_col = lambda i, *_: (0, i)
by_row = lambda i, *_: (i, 0)
fixed = lambda *_: 0


def dot(a, b):
    return jnp.dot(a, b, preferred_element_type=F32)


def dot_nt(a, b):
    return lax.dot_general(a, b, (((1,), (1,)), ((), ())), preferred_element_type=F32)


def cols(height, wide, at):
    return pl.BlockSpec((height, wide), lambda i, *s: (0, at(i, *s)))


def bf(*shape):
    return jax.ShapeDtypeStruct(shape, BF)


def f32(*shape):
    return jax.ShapeDtypeStruct(shape, F32)


def vmem(*shape, dtype=BF):
    return pltpu.VMEM(shape, dtype)


def whole(*shape):
    return pl.BlockSpec(shape, lambda *_: (0,) * len(shape))


def inv_rms(blocks, width):
    sq = sum(jnp.sum(jnp.square(b.astype(F32)), axis=0, keepdims=True) for b in blocks)
    return lax.rsqrt(sq / width + NORM_EPS)


def part_of(ref, j, size):
    return ref.at[j * size:(j + 1) * size, :]


def block_of(j, size):
    return pl.ds(pl.multiple_of(j * size, size), size)


def loop(n, body, init=0):
    return lax.fori_loop(0, n, body, init)


def call(kernel, grid, in_specs, out_specs, out_shape, scratch=(), prefetch=1, flops=0, nbytes=0, aliases=None):
    return pl.pallas_call(
        kernel,
        out_shape=out_shape,
        grid_spec=pltpu.PrefetchScalarGridSpec(num_scalar_prefetch=prefetch, grid=grid, in_specs=in_specs, out_specs=out_specs, scratch_shapes=list(scratch)),
        cost_estimate=pl.CostEstimate(flops=flops, bytes_accessed=nbytes, transcendentals=0),
        compiler_params=pltpu.CompilerParams(vmem_limit_bytes=VM),
        input_output_aliases=aliases or {},
    )


def norm_kernel(s_ref, own, own_c, rx, rxc, ry, ryc, g_ref, *rest, width, per_half):
    a_ref = rest[-1]
    w4 = own.shape[0]
    mine = (pl.program_id(0) // per_half) == s_ref[1]
    blocks = [own[...], own_c[...], jnp.where(mine, rx[...], ry[...]), jnp.where(mine, rxc[...], ryc[...])]
    r = inv_rms(blocks, width)
    for j, b in enumerate(blocks):
        part_of(a_ref, j, w4)[...] = (b.astype(F32) * r * part_of(g_ref, j, w4)[:, 0:1]).astype(BF)


def rope_kernel(s_ref, pos_ref, freq_ref, cos_ref, sin_ref):
    ang = freq_ref[...] * pos_ref[...].astype(F32)
    cos_ref[...] = jnp.cos(ang)
    sin_ref[...] = jnp.sin(ang)


def split_kernel(s_ref, wq, wk, wv, own_ref, oth_ref):
    rows, _, hd = wk.shape
    q, k, v = (w[...].reshape(rows, w.shape[1] * hd) for w in (wq, wk, wv))
    two = [hcat([q[:, 2 * g * hd:2 * (g + 1) * hd], k[:, g * hd:(g + 1) * hd], v[:, g * hd:(g + 1) * hd]]) for g in range(2)]
    first = s_ref[2] == 0
    own_ref[...] = jnp.where(first, *two)
    oth_ref[...] = jnp.where(first, *two[::-1])


def qkv_kernel(s_ref, a_ref, w0, w1, w2, w3, cos_ref, sin_ref, qv_ref, kv_ref, w_t, w_all, w_sem, *, hd):
    w4 = w0.shape[0]

    @pl.when(pl.program_id(0) == 0)
    def _():
        cps = [pltpu.make_async_copy(w, part_of(w_all, j, w4), w_sem.at[j]) for j, w in enumerate((w0, w1, w2, w3))]
        for cp in cps:
            cp.start()
        for cp in cps:
            cp.wait()
        to_rows(w_t, w_all)

    hh = hd // 2

    def part(n, _):
        cols = block_of(n, MT)
        qkv = dot(w_t[...], a_ref[:, cols]).astype(BF).astype(F32)
        ct, st = cos_ref[:, cols], sin_ref[:, cols]

        def rot(base):
            u1, u2 = qkv[base:base + hh], qkv[base + hh:base + hd]
            return u1 * ct - u2 * st, u2 * ct + u1 * st

        for g in range(2):
            lo, hi = rot(g * hd)
            qv_ref[g * hd:g * hd + hh, cols] = lo.astype(BF)
            qv_ref[g * hd + hh:(g + 1) * hd, cols] = hi.astype(BF)
        v = qkv[3 * hd:]
        qv_ref[2 * hd:, cols] = v.astype(BF)
        klo, khi = rot(2 * hd)
        kv_ref[cols, :hh] = klo.T.astype(BF)
        kv_ref[cols, hh:hd] = khi.T.astype(BF)
        kv_ref[cols, hd:] = v.T.astype(BF)
        return 0

    loop(a_ref.shape[1] // MT, part)


def attn_kernel(lo_ref, full_ref, q_ref, k_ref, v_ref, pq_ref, pk_ref, o_ref, acc_ref, qq_ref, l_ref, vs_ref, f_ref, *, bq, bk, q_block0, scale):
    qb = q_block0 + pl.program_id(0)
    hd = k_ref.shape[1]
    groups = q_ref.shape[0] // hd
    lo, full = lo_ref[qb], full_ref[qb]
    diag = (qb * bq) // bk
    last = ((qb + 1) * bq + bk - 1) // bk

    @pl.when(pl.program_id(0) == 0)
    def _():
        top = jnp.max(jnp.abs(v_ref[...].astype(F32)), axis=0, keepdims=True)
        top = jnp.max(top, axis=1, keepdims=True)
        f_ref[...] = jnp.broadcast_to(jnp.where(top > BIG, SHRINK, 1.0), f_ref.shape)
        vs_ref[...] = (v_ref[...].astype(F32) * f_ref[0:1, 0:1]).astype(BF)

    for g in range(groups):
        qq_ref[:, g * bq:(g + 1) * bq] = q_ref[g * hd:(g + 1) * hd, :]
    l_ref[...] = jnp.zeros_like(l_ref)
    acc_ref[...] = jnp.zeros_like(acc_ref)

    def step(j, masked):
        rows = block_of(j, bk)

        def part(n, _):
            cols = block_of(n, MT)
            s = dot(k_ref[rows, :], qq_ref[:, cols])
            p = jnp.exp2(jnp.tanh(s * (scale / SOFT_CAP)) * (SOFT_CAP * LOG2E))
            if masked:
                dif = pq_ref[:, block_of(lax.rem(n, bq // MT), MT)] - pk_ref[rows, :]
                p = jnp.where((dif >= 0) & (dif < WINDOW_LEN), p, 0.0)
            l_ref[:, cols] += jnp.sum(p, axis=0, keepdims=True)
            acc_ref[:, cols] += dot(vs_ref[:, rows], p.astype(BF))
            return 0

        lax.fori_loop(0, groups * bq // MT, part, 0, unroll=2)

    mid = jnp.maximum(jnp.minimum(full, diag), lo)
    edge = jnp.maximum(diag, mid)

    def masked_step(i, _):
        j = lo + i
        step(jnp.where(j < mid, j, j - mid + edge), True)
        return 0

    def full_step(j, _):
        step(j, False)
        return 0

    lax.fori_loop(0, mid - lo + last - edge, masked_step, 0)
    lax.fori_loop(mid, diag, full_step, 0)
    for g in range(groups):
        cols = slice(g * bq, (g + 1) * bq)
        o_ref[g * hd:(g + 1) * hd, :] = (acc_ref[:, cols] / l_ref[:, cols] / f_ref[0:1, 0:1]).astype(BF)


def to_rows(m_ref, mt_ref):
    def turn(i, _):
        at = block_of(i, MT)
        m_ref[:, at] = mt_ref[at, :].T
        return 0

    loop(mt_ref.shape[0] // MT, turn)


def sum_sq(t):
    return jnp.sum(t * t, axis=0, keepdims=True)


def proj_kernel(s_ref, o_own, o_c, o_y, o_yc, b0, b0c, b1, b1c, b2, b2c, b3, b3c, x0, x1, x2, x3, g_ref, *rest, width):
    h_ref, m_ref, o_all, mt_ref, w_ref, x_ref, att_ref, w_sem = rest[-8:]
    for i, b in enumerate((b0, b2, b0c, b2c, b1, b3, b1c, b3c)):
        pltpu.make_async_copy(b, w_ref.at[i], w_sem.at[i]).start()
    first = s_ref[2] == 0
    gw = o_own.shape[0]
    pairs = ((o_own, o_c), (o_y, o_yc))
    for i, (a, b) in enumerate([t for q in pairs for t in (q, q[::-1])]):
        part_of(o_all, i, gw)[...] = jnp.where(first, a[...], b[...])
    for j, t in enumerate((x0, x1, x2, x3)):
        x_ref[j] = t[...]
    w4 = x0.shape[0]
    heads = b0.shape[0]
    n = x_ref.shape[0]
    zero = jnp.zeros((1, m_ref.shape[0]), F32)

    def product(j, sq):
        two = (2 * j, 2 * j + 1)
        for i in two:
            pltpu.make_async_copy(b0, w_ref.at[i], w_sem.at[i]).wait()
        t = dot(hcat([w_ref[i, h] for i in two for h in range(heads)]), o_all[...]).astype(BF).astype(F32)
        att_ref[j] = t
        return sq + sum_sq(t)

    r = lax.rsqrt(loop(n, product, zero) / width + NORM_EPS)

    def residual(j, sq):
        at = block_of(j, w4)
        h = (x_ref[j].astype(F32) + att_ref[j] * r * g_ref[at, 1:2]).astype(BF)
        h_ref[at, :] = h
        h = h.astype(F32)
        att_ref[j] = h
        return sq + sum_sq(h)

    r3 = lax.rsqrt(loop(n, residual, zero) / width + NORM_EPS)

    def scaled(j, _):
        at = block_of(j, w4)
        mt_ref[at, :] = (att_ref[j] * r3 * g_ref[at, 2:3]).astype(BF)
        return 0

    loop(n, scaled)
    to_rows(m_ref, mt_ref)


def renorm_kernel(s_ref, h_ref, g_ref, *rest, width):
    m_ref, mt_ref = rest[-2:]
    n = 4
    w4 = h_ref.shape[0] // n

    def theirs(j):
        return h_ref[block_of(lax.rem(j + 2, n), w4), :].astype(F32)

    r = lax.rsqrt(loop(n, lambda j, sq: sq + sum_sq(theirs(j)), jnp.zeros((1, h_ref.shape[1]), F32)) / width + NORM_EPS)

    def scaled(j, _):
        at = block_of(j, w4)
        mt_ref[at, :] = (theirs(j) * r * g_ref[at, 2:3]).astype(BF)
        return 0

    loop(n, scaled)
    to_rows(m_ref, mt_ref)


def gate_up_kernel(s_ref, *refs, groups, sets, steps):
    ms, ws, z_ref = refs[:groups], refs[groups:-1], refs[-1]
    n = z_ref.shape[1]
    per = len(ws) // sets
    ws = [w[...] for w in ws]
    if sets > 1:
        early = pl.program_id(1) < steps
        ws = [jnp.where(early, a, b) for a, b in zip(ws[:per], ws[per:])]
    w = hcat([vcat(ws[:per // 2]), vcat(ws[per // 2:])])
    for r in range(0, z_ref.shape[0], MT):
        m = [t[r:r + MT, :] for t in ms]
        m = jnp.where(pl.program_id(0) == 0, m[0], m[1]) if groups > 1 else m[0]
        t = dot(m, w)
        g, u = t[:, :n].astype(BF).astype(F32), t[:, n:].astype(BF).astype(F32)
        z_ref[r:r + MT, :] = (jax.nn.gelu(g, approximate=True) * u).astype(BF)


def down_y_kernel(s_ref, zw, zf, d0, d1, d2, d3, acc_ref, d_ref, d_sem):
    w4 = d0.shape[0]
    n = zw.shape[0]
    at_start = pl.program_id(0) == 0

    @pl.when(at_start)
    def _():
        for j, dd in enumerate((d0, d1, d2, d3)):
            pltpu.make_async_copy(dd, part_of(d_ref, j, w4), d_sem.at[j]).start()

    z = vcat([zw[...], zf[...]])

    def rows(j, _):
        at = block_of(j, w4)

        @pl.when(at_start)
        def _():
            pltpu.make_async_copy(d0, d_ref.at[at, :], d_sem.at[j]).wait()

        t = dot_nt(d_ref[at, :], z)
        for q in range(n // CH):
            acc_ref[q, at, :CH] = t[:, q * CH:(q + 1) * CH]
            acc_ref[q, at, CH:] = t[:, n + q * CH:n + (q + 1) * CH]
        return 0

    loop(4, rows)


def tail_kernel(part, zwa, zfa, zb, d0, d1, d2, d3, e0, e1, dt, hw0, hw1, hf0, hf1, g_ref, out,
                d_ref, z_ref, g_buf, p_ref, lo_ref, hi_ref, rec_ref, h_ref, sqs_ref, sqr_ref, sqo_ref,
                d_sem, z_sem, p_sem, h_sem, loc_sem, rs_s, rs_r, sq_s, sq_r, dt_s, dt_r, out_s, out_r, *, width, chunks):
    w4 = d0.shape[0]
    w2 = 2 * w4
    f8 = zwa.shape[1]
    y = lax.axis_index('tp')
    dm = lax.axis_index('dm')
    x, c = dm // 2, lax.rem(dm, 2)
    px = {'dp': 0, 'tp': y, 'dm': (1 - x) * 2 + c}
    pc = {'dp': 0, 'tp': y, 'dm': x * 2 + 1 - c}
    py = {'dp': 0, 'tp': 1 - y, 'dm': dm}
    pyc = {'dp': 0, 'tp': 1 - y, 'dm': x * 2 + 1 - c}

    def local(src, dst, sem):
        return pltpu.make_async_copy(src, dst, sem)

    def remote(src, dst, s_sem, r_sem, dev):
        return pltpu.make_async_remote_copy(src_ref=src, dst_ref=dst, send_sem=s_sem, recv_sem=r_sem, device_id=dev, device_id_type=pl.DeviceIdType.MESH)

    d_cp = [local(dd, d_ref.at[j * w4:(j + 1) * w4, :dd.shape[1]], d_sem.at[j]) for j, dd in enumerate((d0, d1, d2, d3))]
    cut = d0.shape[1]
    last = cut + e0.shape[1]
    e_cp = [local(dd, d_ref.at[j * w4:(j + 1) * w4, cut:last], d_sem.at[4 + j]) for j, dd in enumerate((e0, e1))]
    g_cp = local(part_of(g_ref, 0, w2), g_buf, d_sem.at[6])
    late = slice(last, d_ref.shape[1])
    dt_y = remote(dt.at[:, late], d_ref.at[:w4, late], dt_s.at[0], dt_r.at[0], py)
    dt_c = remote(d_ref.at[:w4, late], d_ref.at[w4:w2, late], dt_s.at[1], dt_r.at[1], pc)

    def z_cp(p):
        srcs = ((zwa, 0), (zb, 0), (zfa, 0), (zb, zwa.shape[0]))
        return [local(src.at[pl.ds(at + p * CH, CH), :], z_ref.at[p, i // 2 * CH:(i // 2 + 1) * CH, i % 2 * f8:(i % 2 + 1) * f8], z_sem.at[p, i]) for i, (src, at) in enumerate(srcs)]

    def p_cp(p):
        return local(part.at[p], p_ref.at[lax.rem(p, 3)], p_sem.at[lax.rem(p, 3)])

    per = hw0.shape[1] // CH
    h_cp = []
    for q in range(chunks):
        k, l = q // per, (q % per) * CH
        h_cp.append(local((hw0, hw1)[k].at[0:w2, l:l + CH], h_ref.at[q, :, 0:CH], h_sem.at[q, 0]))
        h_cp.append(local((hf0, hf1)[k].at[w2:2 * w2, l:l + CH], h_ref.at[q, :, CH:2 * CH], h_sem.at[q, 1]))

    def start(cps):
        for cp in cps:
            cp.start()

    start(z_cp(0) + [d_cp[2], p_cp(0), d_cp[3]] + z_cp(1))

    bar = pltpu.get_barrier_semaphore()
    for dev in (px, pc, py, pyc):
        pl.semaphore_signal(bar, inc=1, device_id=dev, device_id_type=pl.DeviceIdType.MESH)
    pl.semaphore_wait(bar, 4)
    dt_y.start()

    def lanes(q):
        return pl.ds(pl.multiple_of(CH * (x + q - 2 * x * q), CH), CH)

    def away(q):
        return pl.ds(pl.multiple_of(CH - CH * (x + q - 2 * x * q), CH), CH)

    def rs(p, q):
        return remote(hi_ref.at[p, :, away(q)], rec_ref.at[p, :, away(q)], rs_s.at[p, q], rs_r.at[p, q], px)

    def sq(p, q):
        return remote(sqs_ref.at[p, q], sqr_ref.at[p, q], sq_s.at[p, q], sq_r.at[p, q], px)

    def outs(p, q):
        col = pl.multiple_of(((q * 2 + p // per) * 4 + 2 * y + c) * (per * CH) + lax.rem(p, per) * CH, CH)
        mine = rec_ref.at[p, :w4, lanes(q)]
        give = rec_ref.at[p, w4:, lanes(q)]
        dst = out.at[:, pl.ds(col, CH)]
        far = [remote(src, dst, out_s.at[p, q, i], out_r.at[p, q, i], dev) for i, (src, dev) in enumerate(((mine, py), (give, pyc), (give, pc)))]
        return far + [local(mine, dst, loc_sem.at[p, q])]

    def block(p, j):
        at = block_of(j, w4)
        return dot_nt(d_ref[at, :], z_ref[p]) + p_ref[lax.rem(p, 3), at, :]

    def upper(p):
        p_cp(p).wait()
        for cp in z_cp(p):
            cp.wait()

        @pl.when(p + 1 < chunks)
        def _():
            p_cp(p + 1).start()

        def half(i, _):
            t = block(p, 2 + i).astype(BF)
            at = block_of(i, w4)
            hi_ref[p, at, :CH] = t[:, CH:]
            hi_ref[p, at, CH:] = t[:, :CH]
            return 0

        loop(2, half)

    def lower(p):
        def half(j, _):
            lo_ref[p, block_of(j, w4), :] = block(p, j)
            return 0

        loop(2, half)

    def add(p, q):
        rs(p, q).wait_recv()
        at = lanes(q)
        t = (lo_ref[p, :, at] + rec_ref[p, :, at].astype(F32)).astype(BF)
        rec_ref[p, :, at] = t
        t = t.astype(F32)
        v = jnp.broadcast_to(jnp.sum(t * t, axis=0, keepdims=True), (8, CH))
        sqo_ref[q] = v
        sqs_ref[p, q] = v
        sq(p, q).start()

    def finish(p, q):
        sq(p, q).wait_recv()
        at = lanes(q)
        r = lax.rsqrt((sqo_ref[q] + sqr_ref[p, q]) / width + NORM_EPS)[0:1]
        rec_ref[p, :, at] = (h_ref[p, :, at].astype(F32) + rec_ref[p, :, at].astype(F32) * r * g_buf[:, 3:4]).astype(BF)
        start(outs(p, q))

    for cp in d_cp[2:]:
        cp.wait()

    def first_upper(p, _):
        upper(p)

        @pl.when(p == 0)
        def _():
            start([rs(0, 0), rs(0, 1)])

        return 0

    loop(2, first_upper)
    start(d_cp[:2] + e_cp + [g_cp] + h_cp)
    for q in range(2, chunks):
        start(z_cp(q))
    dt_y.wait_recv()
    dt_c.start()
    for cp in d_cp[:2] + e_cp:
        cp.wait()
    dt_c.wait_recv()

    def first_lower(p, _):
        lower(p)
        return 0

    loop(2, first_lower)
    for cp in [g_cp] + h_cp:
        cp.wait()

    def body(p, _):
        for q in range(2):
            add(p, q)

            @pl.when(p + 1 < chunks)
            def _():
                rs(p + 1, q).start()

            if q:
                finish(p, 0)
            else:
                @pl.when(p > 0)
                def _():
                    finish(p - 1, 1)

            @pl.when(p + 2 < chunks)
            def _():
                (lower if q else upper)(p + 2)
        return 0

    loop(chunks, body)
    finish(chunks - 1, 1)

    def drain(p, _):
        for q in range(2):
            rs(p, q).wait_send()
            sq(p, q).wait_send()
            for cp in outs(p, q):
                cp.wait()
        return 0

    lax.fori_loop(0, chunks, drain, 0)
    dt_y.wait_send()
    dt_c.wait_send()


def kv_out_kernel(s_ref, kv0, kv1, *rest, extra):
    if extra:
        rest[-1][...] = rest[0][...]
    k_ref, v_ref = rest[-2 - extra:][:2]
    hd = k_ref.shape[2]
    first = s_ref[2] == 0
    a, b = kv0[...], kv1[...]
    two = jnp.where(first, a, b), jnp.where(first, b, a)
    for ref, at in ((k_ref, 0), (v_ref, hd)):
        ref[...] = hcat([t[:, at:at + hd] for t in two]).reshape(ref.shape)


def solution(mesh):
    tp_size, dm_size = mesh.shape['tp'], mesh.shape['dm']

    def flip(bits):
        return [(i, i ^ bits) for i in range(mesh.size)]

    C, X, Y = 1, 2, dm_size
    PX, PY, PC, PXC, PYC = flip(X), flip(Y), flip(C), flip(X | C), flip(Y | C)

    def send(a, perm):
        return lax.ppermute(a, ('tp', 'dm'), perm)

    def layer(tokens, positions, n1, wq, wk, wv, wo, n2, n3, wg, wu, wd, n4):
        y = lax.axis_index('tp')
        d = lax.axis_index('dm')
        x, c = d // 2, d % 2
        xo, yo, co = 1 - x, 1 - y, 1 - c
        rows, w4 = tokens.shape
        D = w4 * dm_size
        S = positions.shape[1]
        hd = wq.shape[2]
        scale = (D / (wq.shape[1] * tp_size)) ** -0.5
        gw = 2 * hd
        half = S // 2
        quarter = half // 4
        F4 = wg.shape[1] // 2
        scal = jnp.stack([x, y, c]).astype(jnp.int32)

        def take(a, start, size, axis=0):
            return lax.dynamic_slice_in_dim(a, start, size, axis)

        def take_cols(a, start, size):
            return take(a, start, size, 1)

        sets = range(2)
        dma = pltpu.SemaphoreType.DMA
        xt = tokens.T

        gains = jnp.stack([n1, n2, n3, n4])
        gall = hcat([gains, send(gains, PC), send(gains, PX), send(gains, PXC)])
        gcol = (1.0 + gall.astype(F32)).T

        oh = half // 2
        rx = [send(take_cols(xt, xo * S + k * half + y * oh, oh), PX) for k in sets]
        own_p = take_cols(xt, x * S, S)
        own_c = send(own_p, PC)
        ry = [send(rx[k], PY) for k in sets]
        rxc = [send(rx[k], PC) for k in sets]
        ryc = [send(ry[k], PC) for k in sets]

        wr = w4 // 9
        heads_of = lambda w: pl.BlockSpec((wr,) + w.shape[1:], lambda i, s: (i, 0, 0))
        wq_own, wq_oth = call(split_kernel, (9,), [heads_of(w) for w in (wq, wk, wv)], [pl.BlockSpec((wr, 2 * gw), by_row)] * 2, [bf(w4, 2 * gw)] * 2, flops=w4 * gw)(scal, wq, wk, wv)
        wqs = [wq_own, send(wq_oth, PC), send(wq_own, PX), send(wq_oth, PXC)]

        wot = jnp.transpose(wo, (0, 2, 1))
        B0 = wot
        B1 = send(B0, PX)
        B2 = send(B0, PY)
        B3 = send(B1, PY)
        Bs = []
        for b in (B0, B1, B2, B3):
            Bs += [b, send(b, PC)]

        def gather(own, oth, far=None):
            r1 = send(oth, PX)
            s0 = send(own if far is None else far, PY)
            s1 = send(r1, PY)
            ty = [own, send(own, PC), r1, send(r1, PC)]
            to = [s0, send(s0, PC), s1, send(s1, PC)]
            return ty, to

        F8 = F4 // 2

        def gu_half(xx, at):
            return hcat([take_cols(w, xx * F4 + at, F8) for w in (wg, wu)])

        gu = {ab: gather(gu_half(x, at), gu_half(xo, at)) for ab, at in (('a', 0), ('b', F8))}
        wdt = wd.T
        dw_own, dw_oth = (take_cols(wdt, xx * F4, F4) for xx in (x, xo))
        dw_a, dw_b = dw_own[:, :KA], dw_own[:, KA:F4 - KT]
        dn_y, dn_o = gather(dw_own, dw_oth, dw_a)
        dwb = send(dw_b, PY)
        dwb_c = send(dwb, PC)

        pos = take(positions, x, 1)[0]
        inv_freq = ROPE_BASE ** (-2.0 * jnp.arange(hd // 2, dtype=F32) / hd)
        pos_row, pos_col = pos.reshape(1, S), pos.reshape(S, 1)

        tile = 512
        nt = half // tile
        per_half = nt // 2
        nb = S // tile
        cos_t, sin_t = call(
            rope_kernel, (S // MT,), [pl.BlockSpec((1, MT), by_col), whole(hd // 2, 1)], [pl.BlockSpec((hd // 2, MT), by_col)] * 2,
            [f32(hd // 2, S)] * 2, flops=hd * S * nb)(scal, pos_row, inv_freq.reshape(hd // 2, 1))
        a_all = []
        for k in sets:
            a_all = [call(
                functools.partial(norm_kernel, width=D, per_half=per_half), (nt,),
                [cols(w4, tile, lambda i, s, k=k: s[0] * nb + k * nt + i), cols(w4, tile, lambda i, s, k=k: k * nt + i)] + [cols(w4, tile, lambda i, s: i % per_half)] * 4 + [whole(D, 4)] + [ANY] * k,
                cols(D, tile, lambda i, s, k=k: k * nt + i), bf(D, S),
                flops=D * S, aliases={8: 0} if k else None)(scal, xt, own_c, rx[k], rxc[k], ry[k], ryc[k], gcol, *a_all)]
        qv, kv = call(
            functools.partial(qkv_kernel, hd=hd), (nb,),
            [pl.BlockSpec((D, tile), by_col)] + [ANY] * 4 + [pl.BlockSpec((hd // 2, tile), by_col)] * 2,
            [pl.BlockSpec((gw + hd, tile), by_col), pl.BlockSpec((tile, gw), by_row)],
            [bf(gw + hd, S), bf(S, gw)],
            [vmem(2 * gw, D), vmem(D, 2 * gw), dma((4,))],
            flops=D * gw * S)(scal, *a_all, *wqs, cos_t, sin_t)

        bq = bk = tile
        bq2 = 2 * bq
        first_q, last_q = pos[0::bq][:, None], pos[bq - 1::bq][:, None]
        first_k, last_k = pos[0::bk][None, :], pos[bk - 1::bk][None, :]
        lo_t = jnp.sum((first_q - last_k >= WINDOW_LEN).astype(jnp.int32), axis=1)
        full_t = jnp.sum((last_q - first_k >= WINDOW_LEN).astype(jnp.int32), axis=1)
        h_own, m_own = [], []
        heads = wo.shape[0]
        qn = half // quarter
        mine = lambda i, s: 2 * s[1] + s[2]
        for k in sets:
            q0 = k * half // bq
            kl = (k + 1) * half
            o = call(
                functools.partial(attn_kernel, bq=bq, bk=bk, q_block0=q0, scale=scale), (half // bq,),
                [
                    cols(gw, bq, lambda i, *_, q0=q0: q0 + i), cols(kl, hd, fixed), pl.BlockSpec((hd, kl), lambda i, *_: (gw // hd, 0)),
                    cols(1, bq, lambda i, *_, q0=q0: q0 + i), cols(kl, 1, fixed),
                ],
                pl.BlockSpec((gw, bq), by_col),
                bf(gw, half),
                [vmem(hd, bq2, dtype=F32), vmem(hd, bq2), vmem(1, bq2, dtype=F32), vmem(hd, kl), vmem(8, CH, dtype=F32)],
                prefetch=2, flops=gw * half * kl)(lo_t, full_t, qv, kv, qv, pos_row, pos_col)
            mc = 2 * y + co
            my, myc = 2 * yo + c, 2 * yo + co
            o_c = send(take_cols(o, mc * quarter, quarter), PC)
            o_y = send(take_cols(o, my * quarter, quarter), PY)
            o_yc = send(take_cols(o, myc * quarter, quarter), PYC)
            h, m = call(
                functools.partial(proj_kernel, width=D), (1,),
                [cols(gw, quarter, mine)] + [whole(gw, quarter)] * 3 + [ANY] * 8 + [
                    cols(w4, quarter, lambda i, s, k=k: (2 * s[0] + k) * qn + mine(i, s)), cols(w4, quarter, lambda i, s, k=k: k * qn + mine(i, s)),
                    *[cols(w4, quarter, lambda i, s: s[2])] * 2,
                    whole(D, 4)] + [ANY] * k,
                [whole(D, quarter), pl.BlockSpec((quarter, D), lambda i, s, k=k: (k, 0))],
                [bf(D, quarter), bf(oh, D)],
                [vmem(4 * gw, quarter), vmem(D, quarter), vmem(len(Bs), heads, w4, hd), vmem(4, w4, quarter), vmem(4, w4, quarter, dtype=F32), dma((len(Bs),))],
                flops=D * gw * half, aliases={18: 1} if k else None)(scal, o, o_c, o_y, o_yc, *Bs, xt, own_c, rx[k], rxc[k], gcol, *m_own)
            h_own.append(h)
            m_own = [m]
        h_for = [send(h_own[k], PX) for k in sets]
        m_for = []
        for k in sets:
            m_for = [call(
                functools.partial(renorm_kernel, width=D), (1,), [whole(D, quarter), whole(D, 4)] + [ANY] * k,
                pl.BlockSpec((quarter, D), lambda i, s, k=k: (k, 0)), bf(oh, D), [vmem(D, quarter)],
                flops=D * half, aliases={3: 0} if k else None)(scal, h_for[k], gcol, *m_for)]

        def gated(ms, wsets, ft=128):
            nf = F8 // ft
            groups, sets = len(ms), len(wsets)
            early = lambda i: jnp.minimum(i, nf - 1)
            late = lambda i: jnp.maximum(i - nf, 0)
            specs = [cols(w4, ft, lambda j, i, s, at=at, up=up: up * nf + at(i)) for at in (early, late)[:sets] for up in range(2) for _ in wsets[0]]
            return call(
                functools.partial(gate_up_kernel, groups=groups, sets=sets, steps=nf), (groups, sets * nf),
                [whole(oh, D)] * groups + specs, pl.BlockSpec((oh, ft), lambda j, i, s: (j, i)),
                bf(oh * groups, sets * F8), flops=D * F4 * half * groups * sets)(scal, *ms, *[t for w in wsets for t in w + w])

        gua, gub = gu['a'], gu['b']
        near = [t[0] for t in (gua, gub)]
        zy_own = gated(m_own, near)
        zy_for = gated(m_for, near)
        za_own = gated(m_own, [gua[1]])
        za_for = gated(m_for, [gua[1]])
        zb = gated(m_own + m_for, [gub[1]], 3 * CH)
        w2 = 2 * w4
        chunks = oh // CH
        yt = 2 * CH
        part = call(
            down_y_kernel, (oh // yt,), [pl.BlockSpec((yt, F4), by_row)] * 2 + [ANY] * 4,
            pl.BlockSpec((2, D, yt), lambda i, s: (i, 0, 0)), f32(chunks, D, yt),
            [vmem(D, F4), dma((4,))], flops=D * F4 * half)(scal, zy_own, zy_for, *dn_y)
        out = pl.pallas_call(
            functools.partial(tail_kernel, width=D, chunks=chunks),
            out_shape=bf(w4, rows),
            in_specs=[ANY] * 16,
            out_specs=ANY,
            scratch_shapes=[
                vmem(D, F4), vmem(chunks, yt, F4), vmem(w2, 4, dtype=F32), vmem(3, D, yt, dtype=F32), vmem(chunks, w2, yt, dtype=F32),
                *[vmem(chunks, w2, yt)] * 3, *[vmem(chunks, 2, 8, CH, dtype=F32)] * 2, vmem(2, 8, CH, dtype=F32),
                dma((7,)), dma((chunks, 4)), dma((3,)), *[dma((chunks, 2))] * 6, *[dma((2,))] * 2, *[dma((chunks, 2, 3))] * 2],
            cost_estimate=pl.CostEstimate(flops=D * F4 * S, bytes_accessed=D * rows, transcendentals=0),
            compiler_params=pltpu.CompilerParams(vmem_limit_bytes=VM, collective_id=0, has_side_effects=True),
            name='tail',
        )(part, za_own, za_for, zb, *dn_o, dwb, dwb_c, dw_own, *h_own, *h_for, gcol)
        kv_c = send(kv, PC)
        most = nb - per_half
        kv_sets = jnp.split(kv, [most * tile // 2, most * tile])
        kv_x = [send(t, PX) for t in kv_sets]
        kv_xc = [send(t, PC) for t in kv_x]
        kv_outs = []
        for i, (t, tc, base, last) in enumerate(zip([kv] + kv_x, [kv_c] + kv_xc, (0, 0, most // 2, most), (nb, most // 2, most, nb))):
            extra = i == 3
            cut = 2 if i == 0 else 1
            kt = tile // cut
            n = cut * (last - base)
            kv_spec = pl.BlockSpec((kt, gw), by_row)
            at = lambda j, s, i=i, base=base, cut=cut: (((1 - s[0] if i else s[0]) * nb + base) * cut + j, 0, 0)
            cspec = [cols(w4, rows // n, lambda i, s: i)] * extra
            kv_outs = call(
                functools.partial(kv_out_kernel, extra=int(extra)), (n,), [kv_spec] * 2 + cspec + [ANY] * len(kv_outs),
                [pl.BlockSpec((kt, 2, hd), at)] * 2 + cspec, [bf(rows, 2, hd)] * 2 + [bf(w4, rows)] * extra,
                flops=rows * gw, aliases={3 + extra: 0, 4 + extra: 1} if i else None)(scal, t, tc, *[out] * extra, *kv_outs)
        k_out, v_out, out = kv_outs
        return out.T, k_out, v_out

    width_spec = P('dm')
    in_specs = (P('dp', 'dm'), P('dp', None), width_spec, P('dm', 'tp', None), P('dm', 'tp', None), P('dm', 'tp', None), P('tp', None, 'dm'), width_spec, width_spec, P('dm', 'tp'), P('dm', 'tp'), P('tp', 'dm'), width_spec)
    out_specs = (P('dp', 'dm'), P('dp', 'tp', None), P('dp', 'tp', None))
    return jax.shard_map(layer, mesh=mesh, in_specs=in_specs, out_specs=out_specs, check_vma=False)
```

```python
import functools

import jax
import jax.numpy as jnp
from jax import lax
from jax.experimental import pallas as pl
from jax.experimental.pallas import tpu as pltpu
from jax.sharding import PartitionSpec as P


NORM_EPS = 1e-6
SOFT_CAP = 50.0
ROPE_BASE = 10000.0
WINDOW_LEN = 4096
LOG2E = 1.4426950408889634
BF = jnp.bfloat16
F32 = jnp.float32
VM = 63 * 1024 * 1024
CH = 128
BIG = 2.0 ** 40
SHRINK = 2.0 ** -88
MT = 256
KT = 512
KA = 768
ANY = pl.BlockSpec(memory_space=pl.ANY)


vcat = functools.partial(jnp.concatenate, axis=0)
hcat = functools.partial(jnp.concatenate, axis=1)
by_col = lambda i, *_: (0, i)
by_row = lambda i, *_: (i, 0)
fixed = lambda *_: 0


def dot(a, b):
    return jnp.dot(a, b, preferred_element_type=F32)


def dot_nt(a, b):
    return lax.dot_general(a, b, (((1,), (1,)), ((), ())), preferred_element_type=F32)


def cols(height, wide, at):
    return pl.BlockSpec((height, wide), lambda i, *s: (0, at(i, *s)))


def bf(*shape):
    return jax.ShapeDtypeStruct(shape, BF)


def f32(*shape):
    return jax.ShapeDtypeStruct(shape, F32)


def vmem(*shape, dtype=BF):
    return pltpu.VMEM(shape, dtype)


def whole(*shape):
    return pl.BlockSpec(shape, lambda *_: (0,) * len(shape))


def inv_rms(blocks, width):
    sq = sum(jnp.sum(jnp.square(b.astype(F32)), axis=0, keepdims=True) for b in blocks)
    return lax.rsqrt(sq / width + NORM_EPS)


def part_of(ref, j, size):
    return ref.at[j * size:(j + 1) * size, :]


def block_of(j, size):
    return pl.ds(pl.multiple_of(j * size, size), size)


def loop(n, body, init=0):
    return lax.fori_loop(0, n, body, init)


def call(kernel, grid, in_specs, out_specs, out_shape, scratch=(), prefetch=1, flops=0, nbytes=0, aliases=None):
    return pl.pallas_call(
        kernel,
        out_shape=out_shape,
        grid_spec=pltpu.PrefetchScalarGridSpec(num_scalar_prefetch=prefetch, grid=grid, in_specs=in_specs, out_specs=out_specs, scratch_shapes=list(scratch)),
        cost_estimate=pl.CostEstimate(flops=flops, bytes_accessed=nbytes, transcendentals=0),
        compiler_params=pltpu.CompilerParams(vmem_limit_bytes=VM),
        input_output_aliases=aliases or {},
    )


def norm_kernel(s_ref, own, own_c, rx, rxc, ry, ryc, g_ref, *rest, width, per_half):
    a_ref = rest[-1]
    w4 = own.shape[0]
    mine = (pl.program_id(0) // per_half) == s_ref[1]
    blocks = [own[...], own_c[...], jnp.where(mine, rx[...], ry[...]), jnp.where(mine, rxc[...], ryc[...])]
    r = inv_rms(blocks, width)
    for j, b in enumerate(blocks):
        part_of(a_ref, j, w4)[...] = (b.astype(F32) * r * part_of(g_ref, j, w4)[:, 0:1]).astype(BF)


def rope_kernel(s_ref, pos_ref, freq_ref, cos_ref, sin_ref):
    ang = freq_ref[...] * pos_ref[...].astype(F32)
    cos_ref[...] = jnp.cos(ang)
    sin_ref[...] = jnp.sin(ang)


def split_kernel(s_ref, wq, wk, wv, own_ref, oth_ref):
    rows, _, hd = wk.shape
    q, k, v = (w[...].reshape(rows, w.shape[1] * hd) for w in (wq, wk, wv))
    two = [hcat([q[:, 2 * g * hd:2 * (g + 1) * hd], k[:, g * hd:(g + 1) * hd], v[:, g * hd:(g + 1) * hd]]) for g in range(2)]
    first = s_ref[2] == 0
    own_ref[...] = jnp.where(first, *two)
    oth_ref[...] = jnp.where(first, *two[::-1])


def qkv_kernel(s_ref, a_ref, w0, w1, w2, w3, cos_ref, sin_ref, qv_ref, kv_ref, w_t, w_all, w_sem, *, hd):
    w4 = w0.shape[0]

    @pl.when(pl.program_id(0) == 0)
    def _():
        cps = [pltpu.make_async_copy(w, part_of(w_all, j, w4), w_sem.at[j]) for j, w in enumerate((w0, w1, w2, w3))]
        for cp in cps:
            cp.start()
        for cp in cps:
            cp.wait()
        to_rows(w_t, w_all)

    hh = hd // 2

    def part(n, _):
        cols = block_of(n, MT)
        qkv = dot(w_t[...], a_ref[:, cols]).astype(BF).astype(F32)
        ct, st = cos_ref[:, cols], sin_ref[:, cols]

        def rot(base):
            u1, u2 = qkv[base:base + hh], qkv[base + hh:base + hd]
            return u1 * ct - u2 * st, u2 * ct + u1 * st

        for g in range(2):
            lo, hi = rot(g * hd)
            qv_ref[g * hd:g * hd + hh, cols] = lo.astype(BF)
            qv_ref[g * hd + hh:(g + 1) * hd, cols] = hi.astype(BF)
        v = qkv[3 * hd:]
        qv_ref[2 * hd:, cols] = v.astype(BF)
        klo, khi = rot(2 * hd)
        kv_ref[cols, :hh] = klo.T.astype(BF)
        kv_ref[cols, hh:hd] = khi.T.astype(BF)
        kv_ref[cols, hd:] = v.T.astype(BF)
        return 0

    loop(a_ref.shape[1] // MT, part)


def attn_kernel(lo_ref, full_ref, q_ref, k_ref, v_ref, pq_ref, pk_ref, o_ref, acc_ref, qq_ref, l_ref, vs_ref, f_ref, *, bq, bk, q_block0, scale):
    qb = q_block0 + pl.program_id(0)
    hd = k_ref.shape[1]
    groups = q_ref.shape[0] // hd
    lo, full = lo_ref[qb], full_ref[qb]
    diag = (qb * bq) // bk
    last = ((qb + 1) * bq + bk - 1) // bk

    @pl.when(pl.program_id(0) == 0)
    def _():
        top = jnp.max(jnp.abs(v_ref[...].astype(F32)), axis=0, keepdims=True)
        top = jnp.max(top, axis=1, keepdims=True)
        f_ref[...] = jnp.broadcast_to(jnp.where(top > BIG, SHRINK, 1.0), f_ref.shape)
        vs_ref[...] = (v_ref[...].astype(F32) * f_ref[0:1, 0:1]).astype(BF)

    for g in range(groups):
        qq_ref[:, g * bq:(g + 1) * bq] = q_ref[g * hd:(g + 1) * hd, :]
    l_ref[...] = jnp.zeros_like(l_ref)
    acc_ref[...] = jnp.zeros_like(acc_ref)

    def step(j, masked):
        rows = block_of(j, bk)

        def part(n, _):
            cols = block_of(n, MT)
            s = dot(k_ref[rows, :], qq_ref[:, cols])
            p = jnp.exp2(jnp.tanh(s * (scale / SOFT_CAP)) * (SOFT_CAP * LOG2E))
            if masked:
                dif = pq_ref[:, block_of(lax.rem(n, bq // MT), MT)] - pk_ref[rows, :]
                p = jnp.where((dif >= 0) & (dif < WINDOW_LEN), p, 0.0)
            l_ref[:, cols] += jnp.sum(p, axis=0, keepdims=True)
            acc_ref[:, cols] += dot(vs_ref[:, rows], p.astype(BF))
            return 0

        lax.fori_loop(0, groups * bq // MT, part, 0, unroll=2 if masked else 4)

    mid = jnp.maximum(jnp.minimum(full, diag), lo)
    edge = jnp.maximum(diag, mid)

    def masked_step(i, _):
        j = lo + i
        step(jnp.where(j < mid, j, j - mid + edge), True)
        return 0

    def full_step(j, _):
        step(j, False)
        return 0

    lax.fori_loop(0, mid - lo + last - edge, masked_step, 0)
    lax.fori_loop(mid, diag, full_step, 0)
    for g in range(groups):
        cols = slice(g * bq, (g + 1) * bq)
        o_ref[g * hd:(g + 1) * hd, :] = (acc_ref[:, cols] / l_ref[:, cols] / f_ref[0:1, 0:1]).astype(BF)


def to_rows(m_ref, mt_ref):
    def turn(i, _):
        at = block_of(i, MT)
        m_ref[:, at] = mt_ref[at, :].T
        return 0

    loop(mt_ref.shape[0] // MT, turn)


def sum_sq(t):
    return jnp.sum(t * t, axis=0, keepdims=True)


def proj_kernel(s_ref, o_own, o_c, o_y, o_yc, b0, b0c, b1, b1c, b2, b2c, b3, b3c, x0, x1, x2, x3, g_ref, *rest, width):
    h_ref, m_ref, o_all, mt_ref, w_ref, x_ref, att_ref, w_sem = rest[-8:]
    for i, b in enumerate((b0, b2, b0c, b2c, b1, b3, b1c, b3c)):
        pltpu.make_async_copy(b, w_ref.at[i], w_sem.at[i]).start()
    first = s_ref[2] == 0
    gw = o_own.shape[0]
    pairs = ((o_own, o_c), (o_y, o_yc))
    for i, (a, b) in enumerate([t for q in pairs for t in (q, q[::-1])]):
        part_of(o_all, i, gw)[...] = jnp.where(first, a[...], b[...])
    for j, t in enumerate((x0, x1, x2, x3)):
        x_ref[j] = t[...]
    w4 = x0.shape[0]
    heads = b0.shape[0]
    n = x_ref.shape[0]
    zero = jnp.zeros((1, m_ref.shape[0]), F32)

    def product(j, sq):
        two = (2 * j, 2 * j + 1)
        for i in two:
            pltpu.make_async_copy(b0, w_ref.at[i], w_sem.at[i]).wait()
        t = dot(hcat([w_ref[i, h] for i in two for h in range(heads)]), o_all[...]).astype(BF).astype(F32)
        att_ref[j] = t
        return sq + sum_sq(t)

    r = lax.rsqrt(loop(n, product, zero) / width + NORM_EPS)

    def residual(j, sq):
        at = block_of(j, w4)
        h = (x_ref[j].astype(F32) + att_ref[j] * r * g_ref[at, 1:2]).astype(BF)
        h_ref[at, :] = h
        h = h.astype(F32)
        att_ref[j] = h
        return sq + sum_sq(h)

    r3 = lax.rsqrt(loop(n, residual, zero) / width + NORM_EPS)

    def scaled(j, _):
        at = block_of(j, w4)
        mt_ref[at, :] = (att_ref[j] * r3 * g_ref[at, 2:3]).astype(BF)
        return 0

    loop(n, scaled)
    to_rows(m_ref, mt_ref)


def renorm_kernel(s_ref, h_ref, g_ref, *rest, width):
    m_ref, mt_ref = rest[-2:]
    n = 4
    w4 = h_ref.shape[0] // n

    def theirs(j):
        return h_ref[block_of(lax.rem(j + 2, n), w4), :].astype(F32)

    r = lax.rsqrt(loop(n, lambda j, sq: sq + sum_sq(theirs(j)), jnp.zeros((1, h_ref.shape[1]), F32)) / width + NORM_EPS)

    def scaled(j, _):
        at = block_of(j, w4)
        mt_ref[at, :] = (theirs(j) * r * g_ref[at, 2:3]).astype(BF)
        return 0

    loop(n, scaled)
    to_rows(m_ref, mt_ref)


def gate_up_kernel(s_ref, *refs, groups, sets, steps):
    ms, ws, z_ref = refs[:groups], refs[groups:-1], refs[-1]
    n = z_ref.shape[1]
    per = len(ws) // sets
    ws = [w[...] for w in ws]
    if sets > 1:
        early = pl.program_id(1) < steps
        ws = [jnp.where(early, a, b) for a, b in zip(ws[:per], ws[per:])]
    w = hcat([vcat(ws[:per // 2]), vcat(ws[per // 2:])])
    for r in range(0, z_ref.shape[0], MT):
        m = [t[r:r + MT, :] for t in ms]
        m = jnp.where(pl.program_id(0) == 0, m[0], m[1]) if groups > 1 else m[0]
        t = dot(m, w)
        g, u = t[:, :n].astype(BF).astype(F32), t[:, n:].astype(BF).astype(F32)
        z_ref[r:r + MT, :] = (jax.nn.gelu(g, approximate=True) * u).astype(BF)


def down_y_kernel(s_ref, zw, zf, d0, d1, d2, d3, acc_ref, d_ref, d_sem):
    w4 = d0.shape[0]
    n = zw.shape[0]
    at_start = pl.program_id(0) == 0

    @pl.when(at_start)
    def _():
        for j, dd in enumerate((d0, d1, d2, d3)):
            pltpu.make_async_copy(dd, part_of(d_ref, j, w4), d_sem.at[j]).start()

    z = vcat([zw[...], zf[...]])

    def rows(j, _):
        at = block_of(j, w4)

        @pl.when(at_start)
        def _():
            pltpu.make_async_copy(d0, d_ref.at[at, :], d_sem.at[j]).wait()

        t = dot_nt(d_ref[at, :], z)
        for q in range(n // CH):
            acc_ref[q, at, :CH] = t[:, q * CH:(q + 1) * CH]
            acc_ref[q, at, CH:] = t[:, n + q * CH:n + (q + 1) * CH]
        return 0

    loop(4, rows)


def tail_kernel(part, zwa, zfa, zb, d0, d1, d2, d3, e0, e1, dt, hw0, hw1, hf0, hf1, g_ref, out,
                d_ref, z_ref, g_buf, p_ref, lo_ref, hi_ref, rec_ref, h_ref, sqs_ref, sqr_ref, sqo_ref,
                d_sem, z_sem, p_sem, h_sem, loc_sem, rs_s, rs_r, sq_s, sq_r, dt_s, dt_r, out_s, out_r, *, width, chunks):
    w4 = d0.shape[0]
    w2 = 2 * w4
    f8 = zwa.shape[1]
    y = lax.axis_index('tp')
    dm = lax.axis_index('dm')
    x, c = dm // 2, lax.rem(dm, 2)
    px = {'dp': 0, 'tp': y, 'dm': (1 - x) * 2 + c}
    pc = {'dp': 0, 'tp': y, 'dm': x * 2 + 1 - c}
    py = {'dp': 0, 'tp': 1 - y, 'dm': dm}
    pyc = {'dp': 0, 'tp': 1 - y, 'dm': x * 2 + 1 - c}

    def local(src, dst, sem):
        return pltpu.make_async_copy(src, dst, sem)

    def remote(src, dst, s_sem, r_sem, dev):
        return pltpu.make_async_remote_copy(src_ref=src, dst_ref=dst, send_sem=s_sem, recv_sem=r_sem, device_id=dev, device_id_type=pl.DeviceIdType.MESH)

    d_cp = [local(dd, d_ref.at[j * w4:(j + 1) * w4, :dd.shape[1]], d_sem.at[j]) for j, dd in enumerate((d0, d1, d2, d3))]
    cut = d0.shape[1]
    last = cut + e0.shape[1]
    e_cp = [local(dd, d_ref.at[j * w4:(j + 1) * w4, cut:last], d_sem.at[4 + j]) for j, dd in enumerate((e0, e1))]
    g_cp = local(part_of(g_ref, 0, w2), g_buf, d_sem.at[6])
    late = slice(last, d_ref.shape[1])
    dt_y = remote(dt.at[:, late], d_ref.at[:w4, late], dt_s.at[0], dt_r.at[0], py)
    dt_c = remote(d_ref.at[:w4, late], d_ref.at[w4:w2, late], dt_s.at[1], dt_r.at[1], pc)

    def z_cp(p):
        srcs = ((zwa, 0), (zb, 0), (zfa, 0), (zb, zwa.shape[0]))
        return [local(src.at[pl.ds(at + p * CH, CH), :], z_ref.at[p, i // 2 * CH:(i // 2 + 1) * CH, i % 2 * f8:(i % 2 + 1) * f8], z_sem.at[p, i]) for i, (src, at) in enumerate(srcs)]

    def p_cp(p):
        return local(part.at[p], p_ref.at[lax.rem(p, 3)], p_sem.at[lax.rem(p, 3)])

    per = hw0.shape[1] // CH
    h_cp = []
    for q in range(chunks):
        k, l = q // per, (q % per) * CH
        h_cp.append(local((hw0, hw1)[k].at[0:w2, l:l + CH], h_ref.at[q, :, 0:CH], h_sem.at[q, 0]))
        h_cp.append(local((hf0, hf1)[k].at[w2:2 * w2, l:l + CH], h_ref.at[q, :, CH:2 * CH], h_sem.at[q, 1]))

    def start(cps):
        for cp in cps:
            cp.start()

    start(z_cp(0) + [d_cp[2], p_cp(0), d_cp[3]] + z_cp(1))

    bar = pltpu.get_barrier_semaphore()
    for dev in (px, pc, py, pyc):
        pl.semaphore_signal(bar, inc=1, device_id=dev, device_id_type=pl.DeviceIdType.MESH)
    pl.semaphore_wait(bar, 4)
    dt_y.start()

    def lanes(q):
        return pl.ds(pl.multiple_of(CH * (x + q - 2 * x * q), CH), CH)

    def away(q):
        return pl.ds(pl.multiple_of(CH - CH * (x + q - 2 * x * q), CH), CH)

    def rs(p, q):
        return remote(hi_ref.at[p, :, away(q)], rec_ref.at[p, :, away(q)], rs_s.at[p, q], rs_r.at[p, q], px)

    def sq(p, q):
        return remote(sqs_ref.at[p, q], sqr_ref.at[p, q], sq_s.at[p, q], sq_r.at[p, q], px)

    def outs(p, q):
        col = pl.multiple_of(((q * 2 + p // per) * 4 + 2 * y + c) * (per * CH) + lax.rem(p, per) * CH, CH)
        mine = rec_ref.at[p, :w4, lanes(q)]
        give = rec_ref.at[p, w4:, lanes(q)]
        dst = out.at[:, pl.ds(col, CH)]
        far = [remote(src, dst, out_s.at[p, q, i], out_r.at[p, q, i], dev) for i, (src, dev) in enumerate(((mine, py), (give, pyc), (give, pc)))]
        return far + [local(mine, dst, loc_sem.at[p, q])]

    def block(p, j):
        at = block_of(j, w4)
        return dot_nt(d_ref[at, :], z_ref[p]) + p_ref[lax.rem(p, 3), at, :]

    def upper(p):
        p_cp(p).wait()
        for cp in z_cp(p):
            cp.wait()

        @pl.when(p + 1 < chunks)
        def _():
            p_cp(p + 1).start()

        def half(i, _):
            t = block(p, 2 + i).astype(BF)
            at = block_of(i, w4)
            hi_ref[p, at, :CH] = t[:, CH:]
            hi_ref[p, at, CH:] = t[:, :CH]
            return 0

        loop(2, half)

    def lower(p):
        def half(j, _):
            lo_ref[p, block_of(j, w4), :] = block(p, j)
            return 0

        loop(2, half)

    def add(p, q):
        rs(p, q).wait_recv()
        at = lanes(q)
        t = (lo_ref[p, :, at] + rec_ref[p, :, at].astype(F32)).astype(BF)
        rec_ref[p, :, at] = t
        t = t.astype(F32)
        v = jnp.broadcast_to(jnp.sum(t * t, axis=0, keepdims=True), (8, CH))
        sqo_ref[q] = v
        sqs_ref[p, q] = v
        sq(p, q).start()

    def finish(p, q):
        sq(p, q).wait_recv()
        at = lanes(q)
        r = lax.rsqrt((sqo_ref[q] + sqr_ref[p, q]) / width + NORM_EPS)[0:1]
        rec_ref[p, :, at] = (h_ref[p, :, at].astype(F32) + rec_ref[p, :, at].astype(F32) * r * g_buf[:, 3:4]).astype(BF)
        start(outs(p, q))

    for cp in d_cp[2:]:
        cp.wait()

    def first_upper(p, _):
        upper(p)

        @pl.when(p == 0)
        def _():
            start([rs(0, 0), rs(0, 1)])

        return 0

    loop(2, first_upper)
    start(d_cp[:2] + e_cp + [g_cp] + h_cp)
    for q in range(2, chunks):
        start(z_cp(q))
    for cp in d_cp[:2] + e_cp:
        cp.wait()

    def early(i, _):
        p, at = i // 2, block_of(lax.rem(i, 2), w4)
        lo_ref[p, at, :] = dot_nt(d_ref[at, :last], z_ref[p, :, :last]) + p_ref[p, at, :]
        return 0

    loop(4, early)
    dt_y.wait_recv()
    dt_c.start()
    dt_c.wait_recv()

    def rest(i, _):
        p, at = i // 2, block_of(lax.rem(i, 2), w4)
        lo_ref[p, at, :] += dot_nt(d_ref[at, late], z_ref[p, :, late])
        return 0

    loop(4, rest)
    for cp in [g_cp] + h_cp:
        cp.wait()

    def body(p, _):
        for q in range(2):
            add(p, q)

            @pl.when(p + 1 < chunks)
            def _():
                rs(p + 1, q).start()

            if q:
                finish(p, 0)
            else:
                @pl.when(p > 0)
                def _():
                    finish(p - 1, 1)

            @pl.when(p + 2 < chunks)
            def _():
                (lower if q else upper)(p + 2)
        return 0

    loop(chunks, body)
    finish(chunks - 1, 1)

    def drain(p, _):
        for q in range(2):
            rs(p, q).wait_send()
            sq(p, q).wait_send()
            for cp in outs(p, q):
                cp.wait()
        return 0

    lax.fori_loop(0, chunks, drain, 0)
    dt_y.wait_send()
    dt_c.wait_send()


def kv_out_kernel(s_ref, kv0, kv1, *rest, extra):
    if extra:
        rest[-1][...] = rest[0][...]
    k_ref, v_ref = rest[-2 - extra:][:2]
    hd = k_ref.shape[2]
    first = s_ref[2] == 0
    a, b = kv0[...], kv1[...]
    two = jnp.where(first, a, b), jnp.where(first, b, a)
    for ref, at in ((k_ref, 0), (v_ref, hd)):
        ref[...] = hcat([t[:, at:at + hd] for t in two]).reshape(ref.shape)


def solution(mesh):
    tp_size, dm_size = mesh.shape['tp'], mesh.shape['dm']

    def flip(bits):
        return [(i, i ^ bits) for i in range(mesh.size)]

    C, X, Y = 1, 2, dm_size
    PX, PY, PC, PXC, PYC = flip(X), flip(Y), flip(C), flip(X | C), flip(Y | C)

    def send(a, perm):
        return lax.ppermute(a, ('tp', 'dm'), perm)

    def layer(tokens, positions, n1, wq, wk, wv, wo, n2, n3, wg, wu, wd, n4):
        y = lax.axis_index('tp')
        d = lax.axis_index('dm')
        x, c = d // 2, d % 2
        xo, yo, co = 1 - x, 1 - y, 1 - c
        rows, w4 = tokens.shape
        D = w4 * dm_size
        S = positions.shape[1]
        hd = wq.shape[2]
        scale = (D / (wq.shape[1] * tp_size)) ** -0.5
        gw = 2 * hd
        half = S // 2
        quarter = half // 4
        F4 = wg.shape[1] // 2
        scal = jnp.stack([x, y, c]).astype(jnp.int32)

        def take(a, start, size, axis=0):
            return lax.dynamic_slice_in_dim(a, start, size, axis)

        def take_cols(a, start, size):
            return take(a, start, size, 1)

        sets = range(2)
        dma = pltpu.SemaphoreType.DMA
        xt = tokens.T

        gains = jnp.stack([n1, n2, n3, n4])
        gall = hcat([gains, send(gains, PC), send(gains, PX), send(gains, PXC)])
        gcol = (1.0 + gall.astype(F32)).T

        oh = half // 2
        rx = [send(take_cols(xt, xo * S + k * half + y * oh, oh), PX) for k in sets]
        own_p = take_cols(xt, x * S, S)
        own_c = send(own_p, PC)
        ry = [send(rx[k], PY) for k in sets]
        rxc = [send(rx[k], PC) for k in sets]
        ryc = [send(ry[k], PC) for k in sets]

        wr = w4 // 9
        heads_of = lambda w: pl.BlockSpec((wr,) + w.shape[1:], lambda i, s: (i, 0, 0))
        wq_own, wq_oth = call(split_kernel, (9,), [heads_of(w) for w in (wq, wk, wv)], [pl.BlockSpec((wr, 2 * gw), by_row)] * 2, [bf(w4, 2 * gw)] * 2, flops=w4 * gw)(scal, wq, wk, wv)
        wqs = [wq_own, send(wq_oth, PC), send(wq_own, PX), send(wq_oth, PXC)]

        wot = jnp.transpose(wo, (0, 2, 1))
        B0 = wot
        B1 = send(B0, PX)
        B2 = send(B0, PY)
        B3 = send(B1, PY)
        Bs = []
        for b in (B0, B1, B2, B3):
            Bs += [b, send(b, PC)]

        def gather(own, oth, far=None):
            r1 = send(oth, PX)
            s0 = send(own if far is None else far, PY)
            s1 = send(r1, PY)
            ty = [own, send(own, PC), r1, send(r1, PC)]
            to = [s0, send(s0, PC), s1, send(s1, PC)]
            return ty, to

        F8 = F4 // 2

        def gu_half(xx, at):
            return hcat([take_cols(w, xx * F4 + at, F8) for w in (wg, wu)])

        gu = {ab: gather(gu_half(x, at), gu_half(xo, at)) for ab, at in (('a', 0), ('b', F8))}
        wdt = wd.T
        dw_own, dw_oth = (take_cols(wdt, xx * F4, F4) for xx in (x, xo))
        dw_a, dw_b = dw_own[:, :KA], dw_own[:, KA:F4 - KT]
        dn_y, dn_o = gather(dw_own, dw_oth, dw_a)
        dwb = send(dw_b, PY)
        dwb_c = send(dwb, PC)

        pos = take(positions, x, 1)[0]
        inv_freq = ROPE_BASE ** (-2.0 * jnp.arange(hd // 2, dtype=F32) / hd)
        pos_row, pos_col = pos.reshape(1, S), pos.reshape(S, 1)

        tile = 512
        nt = half // tile
        per_half = nt // 2
        nb = S // tile
        cos_t, sin_t = call(
            rope_kernel, (S // MT,), [pl.BlockSpec((1, MT), by_col), whole(hd // 2, 1)], [pl.BlockSpec((hd // 2, MT), by_col)] * 2,
            [f32(hd // 2, S)] * 2, flops=hd * S * nb)(scal, pos_row, inv_freq.reshape(hd // 2, 1))
        a_all = []
        for k in sets:
            a_all = [call(
                functools.partial(norm_kernel, width=D, per_half=half // 2 // MT), (half // MT,),
                [cols(w4, MT, lambda i, s, k=k: (s[0] * nb + k * nt) * per_half + i), cols(w4, MT, lambda i, s, k=k: k * nt * per_half + i)] + [cols(w4, MT, lambda i, s: i % nt)] * 4 + [whole(D, 4)] + [ANY] * k,
                cols(D, MT, lambda i, s, k=k: k * nt * per_half + i), bf(D, S),
                flops=D * S, aliases={8: 0} if k else None)(scal, xt, own_c, rx[k], rxc[k], ry[k], ryc[k], gcol, *a_all)]
        qv, kv = call(
            functools.partial(qkv_kernel, hd=hd), (nb,),
            [pl.BlockSpec((D, tile), by_col)] + [ANY] * 4 + [pl.BlockSpec((hd // 2, tile), by_col)] * 2,
            [pl.BlockSpec((gw + hd, tile), by_col), pl.BlockSpec((tile, gw), by_row)],
            [bf(gw + hd, S), bf(S, gw)],
            [vmem(2 * gw, D), vmem(D, 2 * gw), dma((4,))],
            flops=D * gw * S)(scal, *a_all, *wqs, cos_t, sin_t)

        bq = bk = tile
        bq2 = 2 * bq
        first_q, last_q = pos[0::bq][:, None], pos[bq - 1::bq][:, None]
        first_k, last_k = pos[0::bk][None, :], pos[bk - 1::bk][None, :]
        lo_t = jnp.sum((first_q - last_k >= WINDOW_LEN).astype(jnp.int32), axis=1)
        full_t = jnp.sum((last_q - first_k >= WINDOW_LEN).astype(jnp.int32), axis=1)
        h_own, m_own = [], []
        heads = wo.shape[0]
        qn = half // quarter
        mine = lambda i, s: 2 * s[1] + s[2]
        for k in sets:
            q0 = k * half // bq
            kl = (k + 1) * half
            o = call(
                functools.partial(attn_kernel, bq=bq, bk=bk, q_block0=q0, scale=scale), (half // bq,),
                [
                    cols(gw, bq, lambda i, *_, q0=q0: q0 + i), cols(kl, hd, fixed), pl.BlockSpec((hd, kl), lambda i, *_: (gw // hd, 0)),
                    cols(1, bq, lambda i, *_, q0=q0: q0 + i), cols(kl, 1, fixed),
                ],
                pl.BlockSpec((gw, bq), by_col),
                bf(gw, half),
                [vmem(hd, bq2, dtype=F32), vmem(hd, bq2), vmem(1, bq2, dtype=F32), vmem(hd, kl), vmem(8, CH, dtype=F32)],
                prefetch=2, flops=gw * half * kl)(lo_t, full_t, qv, kv, qv, pos_row, pos_col)
            mc = 2 * y + co
            my, myc = 2 * yo + c, 2 * yo + co
            o_c = send(take_cols(o, mc * quarter, quarter), PC)
            o_y = send(take_cols(o, my * quarter, quarter), PY)
            o_yc = send(take_cols(o, myc * quarter, quarter), PYC)
            h, m = call(
                functools.partial(proj_kernel, width=D), (1,),
                [cols(gw, quarter, mine)] + [whole(gw, quarter)] * 3 + [ANY] * 8 + [
                    cols(w4, quarter, lambda i, s, k=k: (2 * s[0] + k) * qn + mine(i, s)), cols(w4, quarter, lambda i, s, k=k: k * qn + mine(i, s)),
                    *[cols(w4, quarter, lambda i, s: s[2])] * 2,
                    whole(D, 4)] + [ANY] * k,
                [whole(D, quarter), pl.BlockSpec((quarter, D), lambda i, s, k=k: (k, 0))],
                [bf(D, quarter), bf(oh, D)],
                [vmem(4 * gw, quarter), vmem(D, quarter), vmem(len(Bs), heads, w4, hd), vmem(4, w4, quarter), vmem(4, w4, quarter, dtype=F32), dma((len(Bs),))],
                flops=D * gw * half, aliases={18: 1} if k else None)(scal, o, o_c, o_y, o_yc, *Bs, xt, own_c, rx[k], rxc[k], gcol, *m_own)
            h_own.append(h)
            m_own = [m]
        h_for = [send(h_own[k], PX) for k in sets]
        m_for = []
        for k in sets:
            m_for = [call(
                functools.partial(renorm_kernel, width=D), (1,), [whole(D, quarter), whole(D, 4)] + [ANY] * k,
                pl.BlockSpec((quarter, D), lambda i, s, k=k: (k, 0)), bf(oh, D), [vmem(D, quarter)],
                flops=D * half, aliases={3: 0} if k else None)(scal, h_for[k], gcol, *m_for)]

        def gated(ms, wsets, ft=128):
            nf = F8 // ft
            groups, sets = len(ms), len(wsets)
            early = lambda i: jnp.minimum(i, nf - 1)
            late = lambda i: jnp.maximum(i - nf, 0)
            specs = [cols(w4, ft, lambda j, i, s, at=at, up=up: up * nf + at(i)) for at in (early, late)[:sets] for up in range(2) for _ in wsets[0]]
            return call(
                functools.partial(gate_up_kernel, groups=groups, sets=sets, steps=nf), (groups, sets * nf),
                [whole(oh, D)] * groups + specs, pl.BlockSpec((oh, ft), lambda j, i, s: (j, i)),
                bf(oh * groups, sets * F8), flops=D * F4 * half * groups * sets)(scal, *ms, *[t for w in wsets for t in w + w])

        gua, gub = gu['a'], gu['b']
        near = [t[0] for t in (gua, gub)]
        zy_own = gated(m_own, near)
        zy_for = gated(m_for, near)
        za_own = gated(m_own, [gua[1]])
        za_for = gated(m_for, [gua[1]])
        zb = gated(m_own + m_for, [gub[1]], 3 * CH)
        w2 = 2 * w4
        chunks = oh // CH
        yt = 2 * CH
        part = call(
            down_y_kernel, (oh // yt,), [pl.BlockSpec((yt, F4), by_row)] * 2 + [ANY] * 4,
            pl.BlockSpec((2, D, yt), lambda i, s: (i, 0, 0)), f32(chunks, D, yt),
            [vmem(D, F4), dma((4,))], flops=D * F4 * half)(scal, zy_own, zy_for, *dn_y)
        out = pl.pallas_call(
            functools.partial(tail_kernel, width=D, chunks=chunks),
            out_shape=bf(w4, rows),
            in_specs=[ANY] * 16,
            out_specs=ANY,
            scratch_shapes=[
                vmem(D, F4), vmem(chunks, yt, F4), vmem(w2, 4, dtype=F32), vmem(3, D, yt, dtype=F32), vmem(chunks, w2, yt, dtype=F32),
                *[vmem(chunks, w2, yt)] * 3, *[vmem(chunks, 2, 8, CH, dtype=F32)] * 2, vmem(2, 8, CH, dtype=F32),
                dma((7,)), dma((chunks, 4)), dma((3,)), *[dma((chunks, 2))] * 6, *[dma((2,))] * 2, *[dma((chunks, 2, 3))] * 2],
            cost_estimate=pl.CostEstimate(flops=D * F4 * S, bytes_accessed=D * rows, transcendentals=0),
            compiler_params=pltpu.CompilerParams(vmem_limit_bytes=VM, collective_id=0, has_side_effects=True),
            name='tail',
        )(part, za_own, za_for, zb, *dn_o, dwb, dwb_c, dw_own, *h_own, *h_for, gcol)
        kv_c = send(kv, PC)
        most = nb - per_half
        kv_sets = jnp.split(kv, [most * tile // 2, most * tile])
        kv_x = [send(t, PX) for t in kv_sets]
        kv_xc = [send(t, PC) for t in kv_x]
        kv_outs = []
        for i, (t, tc, base, last) in enumerate(zip([kv] + kv_x, [kv_c] + kv_xc, (0, 0, most // 2, most), (nb, most // 2, most, nb))):
            extra = i == 3
            cut = 2 if i == 0 else 1
            kt = tile // cut
            n = cut * (last - base)
            kv_spec = pl.BlockSpec((kt, gw), by_row)
            at = lambda j, s, i=i, base=base, cut=cut: (((1 - s[0] if i else s[0]) * nb + base) * cut + j, 0, 0)
            cspec = [cols(w4, rows // n, lambda i, s: i)] * extra
            kv_outs = call(
                functools.partial(kv_out_kernel, extra=int(extra)), (n,), [kv_spec] * 2 + cspec + [ANY] * len(kv_outs),
                [pl.BlockSpec((kt, 2, hd), at)] * 2 + cspec, [bf(rows, 2, hd)] * 2 + [bf(w4, rows)] * extra,
                flops=rows * gw, aliases={3 + extra: 0, 4 + extra: 1} if i else None)(scal, t, tc, *[out] * extra, *kv_outs)
        k_out, v_out, out = kv_outs
        return out.T, k_out, v_out

    width_spec = P('dm')
    in_specs = (P('dp', 'dm'), P('dp', None), width_spec, P('dm', 'tp', None), P('dm', 'tp', None), P('dm', 'tp', None), P('tp', None, 'dm'), width_spec, width_spec, P('dm', 'tp'), P('dm', 'tp'), P('tp', 'dm'), width_spec)
    out_specs = (P('dp', 'dm'), P('dp', 'tp', None), P('dp', 'tp', None))
    return jax.shard_map(layer, mesh=mesh, in_specs=in_specs, out_specs=out_specs, check_vma=False)
```

```python
import functools

import jax
import jax.numpy as jnp
from jax import lax
from jax.experimental import pallas as pl
from jax.experimental.pallas import tpu as pltpu
from jax.sharding import PartitionSpec as P


NORM_EPS = 1e-6
SOFT_CAP = 50.0
ROPE_BASE = 10000.0
WINDOW_LEN = 4096
LOG2E = 1.4426950408889634
BF = jnp.bfloat16
F32 = jnp.float32
VM = 67043328
CH = 128
BIG = 2.0 ** 40
SHRINK = 2.0 ** -88
MT = 256
KT = 512
KA = 768
ANY = pl.BlockSpec(memory_space=pl.ANY)


vcat = functools.partial(jnp.concatenate, axis=0)
hcat = functools.partial(jnp.concatenate, axis=1)
by_col = lambda i, *_: (0, i)
by_row = lambda i, *_: (i, 0)
fixed = lambda *_: 0


def dot(a, b):
    return jnp.dot(a, b, preferred_element_type=F32)


def dot_nt(a, b):
    return lax.dot_general(a, b, (((1,), (1,)), ((), ())), preferred_element_type=F32)


def cols(height, wide, at):
    return pl.BlockSpec((height, wide), lambda i, *s: (0, at(i, *s)))


def bf(*shape):
    return jax.ShapeDtypeStruct(shape, BF)


def f32(*shape):
    return jax.ShapeDtypeStruct(shape, F32)


def vmem(*shape, dtype=BF):
    return pltpu.VMEM(shape, dtype)


def whole(*shape):
    return pl.BlockSpec(shape, lambda *_: (0,) * len(shape))


def inv_rms(blocks, width):
    sq = sum(jnp.sum(jnp.square(b.astype(F32)), axis=0, keepdims=True) for b in blocks)
    return lax.rsqrt(sq / width + NORM_EPS)


def part_of(ref, j, size):
    return ref.at[j * size:(j + 1) * size, :]


def block_of(j, size):
    return pl.ds(pl.multiple_of(j * size, size), size)


def loop(n, body, init=0):
    return lax.fori_loop(0, n, body, init)


def call(kernel, grid, in_specs, out_specs, out_shape, scratch=(), prefetch=1, flops=0, nbytes=0, aliases=None):
    return pl.pallas_call(
        kernel,
        out_shape=out_shape,
        grid_spec=pltpu.PrefetchScalarGridSpec(num_scalar_prefetch=prefetch, grid=grid, in_specs=in_specs, out_specs=out_specs, scratch_shapes=list(scratch)),
        cost_estimate=pl.CostEstimate(flops=flops, bytes_accessed=nbytes, transcendentals=0),
        compiler_params=pltpu.CompilerParams(vmem_limit_bytes=VM),
        input_output_aliases=aliases or {},
    )


def norm_kernel(s_ref, own, own_c, rx, rxc, ry, ryc, g_ref, *rest, width, per_half):
    a_ref = rest[-1]
    w4 = own.shape[0]
    mine = (pl.program_id(0) // per_half) == s_ref[1]
    blocks = [own[...], own_c[...], jnp.where(mine, rx[...], ry[...]), jnp.where(mine, rxc[...], ryc[...])]
    r = inv_rms(blocks, width)
    for j, b in enumerate(blocks):
        part_of(a_ref, j, w4)[...] = (b.astype(F32) * r * part_of(g_ref, j, w4)[:, 0:1]).astype(BF)


def rope_kernel(s_ref, pos_ref, freq_ref, cos_ref, sin_ref):
    ang = freq_ref[...] * pos_ref[...].astype(F32)
    cos_ref[...] = jnp.cos(ang)
    sin_ref[...] = jnp.sin(ang)


def split_kernel(s_ref, wq, wk, wv, own_ref, oth_ref):
    rows, _, hd = wk.shape
    q, k, v = (w[...].reshape(rows, w.shape[1] * hd) for w in (wq, wk, wv))
    two = [hcat([q[:, 2 * g * hd:2 * (g + 1) * hd], k[:, g * hd:(g + 1) * hd], v[:, g * hd:(g + 1) * hd]]) for g in range(2)]
    first = s_ref[2] == 0
    own_ref[...] = jnp.where(first, *two)
    oth_ref[...] = jnp.where(first, *two[::-1])


def qkv_kernel(s_ref, a_ref, w0, w1, w2, w3, cos_ref, sin_ref, qv_ref, kv_ref, w_t, w_all, w_sem, *, hd):
    w4 = w0.shape[0]

    @pl.when(pl.program_id(0) == 0)
    def _():
        cps = [pltpu.make_async_copy(w, part_of(w_all, j, w4), w_sem.at[j]) for j, w in enumerate((w0, w1, w2, w3))]
        for cp in cps:
            cp.start()
        for cp in cps:
            cp.wait()
        to_rows(w_t, w_all)

    hh = hd // 2

    def part(n, _):
        cols = block_of(n, MT)
        qkv = dot(w_t[...], a_ref[:, cols]).astype(BF).astype(F32)
        ct, st = cos_ref[:, cols], sin_ref[:, cols]

        def rot(base):
            u1, u2 = qkv[base:base + hh], qkv[base + hh:base + hd]
            return u1 * ct - u2 * st, u2 * ct + u1 * st

        for g in range(2):
            lo, hi = rot(g * hd)
            qv_ref[g * hd:g * hd + hh, cols] = lo.astype(BF)
            qv_ref[g * hd + hh:(g + 1) * hd, cols] = hi.astype(BF)
        v = qkv[3 * hd:]
        qv_ref[2 * hd:, cols] = v.astype(BF)
        klo, khi = rot(2 * hd)
        kv_ref[cols, :hh] = klo.T.astype(BF)
        kv_ref[cols, hh:hd] = khi.T.astype(BF)
        kv_ref[cols, hd:] = v.T.astype(BF)
        return 0

    loop(a_ref.shape[1] // MT, part)


def attn_kernel(lo_ref, full_ref, q_ref, k_ref, v_ref, pq_ref, pk_ref, o_ref, acc_ref, qq_ref, l_ref, vs_ref, f_ref, *, bq, bk, q_block0, scale):
    qb = q_block0 + pl.program_id(0)
    hd = k_ref.shape[1]
    groups = q_ref.shape[0] // hd
    lo, full = lo_ref[qb], full_ref[qb]
    diag = (qb * bq) // bk
    last = ((qb + 1) * bq + bk - 1) // bk

    @pl.when(pl.program_id(0) == 0)
    def _():
        top = jnp.max(jnp.abs(v_ref[...].astype(F32)), axis=0, keepdims=True)
        top = jnp.max(top, axis=1, keepdims=True)
        f_ref[...] = jnp.broadcast_to(jnp.where(top > BIG, SHRINK, 1.0), f_ref.shape)
        vs_ref[...] = (v_ref[...].astype(F32) * f_ref[0:1, 0:1]).astype(BF)

    for g in range(groups):
        qq_ref[:, g * bq:(g + 1) * bq] = q_ref[g * hd:(g + 1) * hd, :]
    l_ref[...] = jnp.zeros_like(l_ref)
    acc_ref[...] = jnp.zeros_like(acc_ref)

    def step(j, masked):
        rows = block_of(j, bk)

        def part(n, _):
            cols = block_of(n, MT)
            s = dot(k_ref[rows, :], qq_ref[:, cols])
            p = jnp.exp2(jnp.tanh(s * (scale / SOFT_CAP)) * (SOFT_CAP * LOG2E))
            if masked:
                dif = pq_ref[:, block_of(lax.rem(n, bq // MT), MT)] - pk_ref[rows, :]
                p = jnp.where((dif >= 0) & (dif < WINDOW_LEN), p, 0.0)
            l_ref[:, cols] += jnp.sum(p, axis=0, keepdims=True)
            acc_ref[:, cols] += dot(vs_ref[:, rows], p.astype(BF))
            return 0

        lax.fori_loop(0, groups * bq // MT, part, 0, unroll=2 if masked else 4)

    mid = jnp.maximum(jnp.minimum(full, diag), lo)
    edge = jnp.maximum(diag, mid)

    def masked_step(i, _):
        j = lo + i
        step(jnp.where(j < mid, j, j - mid + edge), True)
        return 0

    def full_step(j, _):
        step(j, False)
        return 0

    lax.fori_loop(0, mid - lo + last - edge, masked_step, 0)
    lax.fori_loop(mid, diag, full_step, 0)
    for g in range(groups):
        cols = slice(g * bq, (g + 1) * bq)
        o_ref[g * hd:(g + 1) * hd, :] = (acc_ref[:, cols] / l_ref[:, cols] / f_ref[0:1, 0:1]).astype(BF)


def to_rows(m_ref, mt_ref):
    def turn(i, _):
        at = block_of(i, MT)
        m_ref[:, at] = mt_ref[at, :].T
        return 0

    loop(mt_ref.shape[0] // MT, turn)


def sum_sq(t):
    return jnp.sum(t * t, axis=0, keepdims=True)


def proj_kernel(s_ref, o_own, o_c, o_y, o_yc, b0, b0c, b1, b1c, b2, b2c, b3, b3c, x0, x1, x2, x3, g_ref, *rest, width):
    h_ref, m_ref, o_all, mt_ref, w_ref, x_ref, att_ref, w_sem = rest[-8:]
    for i, b in enumerate((b0, b2, b0c, b2c, b1, b3, b1c, b3c)):
        pltpu.make_async_copy(b, w_ref.at[i], w_sem.at[i]).start()
    first = s_ref[2] == 0
    gw = o_own.shape[0]
    pairs = ((o_own, o_c), (o_y, o_yc))
    for i, (a, b) in enumerate([t for q in pairs for t in (q, q[::-1])]):
        part_of(o_all, i, gw)[...] = jnp.where(first, a[...], b[...])
    for j, t in enumerate((x0, x1, x2, x3)):
        x_ref[j] = t[...]
    w4 = x0.shape[0]
    heads = b0.shape[0]
    n = x_ref.shape[0]
    zero = jnp.zeros((1, m_ref.shape[0]), F32)

    def product(j, sq):
        two = (2 * j, 2 * j + 1)
        for i in two:
            pltpu.make_async_copy(b0, w_ref.at[i], w_sem.at[i]).wait()
        t = dot(hcat([w_ref[i, h] for i in two for h in range(heads)]), o_all[...]).astype(BF).astype(F32)
        att_ref[j] = t
        return sq + sum_sq(t)

    r = lax.rsqrt(loop(n, product, zero) / width + NORM_EPS)

    def residual(j, sq):
        at = block_of(j, w4)
        h = (x_ref[j].astype(F32) + att_ref[j] * r * g_ref[at, 1:2]).astype(BF)
        h_ref[at, :] = h
        h = h.astype(F32)
        att_ref[j] = h
        return sq + sum_sq(h)

    r3 = lax.rsqrt(loop(n, residual, zero) / width + NORM_EPS)

    def scaled(j, _):
        at = block_of(j, w4)
        mt_ref[at, :] = (att_ref[j] * r3 * g_ref[at, 2:3]).astype(BF)
        return 0

    loop(n, scaled)
    to_rows(m_ref, mt_ref)


def renorm_kernel(s_ref, h_ref, g_ref, *rest, width):
    m_ref, mt_ref = rest[-2:]
    n = 4
    w4 = h_ref.shape[0] // n

    def theirs(j):
        return h_ref[block_of(lax.rem(j + 2, n), w4), :].astype(F32)

    r = lax.rsqrt(loop(n, lambda j, sq: sq + sum_sq(theirs(j)), jnp.zeros((1, h_ref.shape[1]), F32)) / width + NORM_EPS)

    def scaled(j, _):
        at = block_of(j, w4)
        mt_ref[at, :] = (theirs(j) * r * g_ref[at, 2:3]).astype(BF)
        return 0

    loop(n, scaled)
    to_rows(m_ref, mt_ref)


def gate_up_kernel(s_ref, *refs, groups, sets, steps):
    ms, ws, z_ref = refs[:groups], refs[groups:-1], refs[-1]
    n = z_ref.shape[1]
    per = len(ws) // sets
    ws = [w[...] for w in ws]
    if sets > 1:
        early = pl.program_id(1) < steps
        ws = [jnp.where(early, a, b) for a, b in zip(ws[:per], ws[per:])]
    w = hcat([vcat(ws[:per // 2]), vcat(ws[per // 2:])])
    for r in range(0, z_ref.shape[0], MT):
        m = [t[r:r + MT, :] for t in ms]
        m = jnp.where(pl.program_id(0) == 0, m[0], m[1]) if groups > 1 else m[0]
        t = dot(m, w)
        g, u = t[:, :n].astype(BF).astype(F32), t[:, n:].astype(BF).astype(F32)
        z_ref[r:r + MT, :] = (jax.nn.gelu(g, approximate=True) * u).astype(BF)


def down_y_kernel(s_ref, zw, zf, d0, d1, d2, d3, acc_ref, d_ref, d_sem):
    w4 = d0.shape[0]
    n = zw.shape[0]
    at_start = pl.program_id(0) == 0

    @pl.when(at_start)
    def _():
        for j, dd in enumerate((d0, d1, d2, d3)):
            pltpu.make_async_copy(dd, part_of(d_ref, j, w4), d_sem.at[j]).start()

    z = vcat([zw[...], zf[...]])

    def rows(j, _):
        at = block_of(j, w4)

        @pl.when(at_start)
        def _():
            pltpu.make_async_copy(d0, d_ref.at[at, :], d_sem.at[j]).wait()

        t = dot_nt(d_ref[at, :], z)
        for q in range(n // CH):
            acc_ref[q, at, :CH] = t[:, q * CH:(q + 1) * CH]
            acc_ref[q, at, CH:] = t[:, n + q * CH:n + (q + 1) * CH]
        return 0

    loop(4, rows)


def tail_kernel(part, zwa, zfa, zb, d0, d1, d2, d3, e0, e1, dt, hw0, hw1, hf0, hf1, g_ref, out,
                d_ref, z_ref, g_buf, p_ref, lo_ref, hi_ref, rec_ref, h_ref, sqs_ref, sqr_ref, sqo_ref,
                d_sem, z_sem, p_sem, h_sem, loc_sem, rs_s, rs_r, sq_s, sq_r, dt_s, dt_r, out_s, out_r, *, width, chunks):
    w4 = d0.shape[0]
    w2 = 2 * w4
    f8 = zwa.shape[1]
    y = lax.axis_index('tp')
    dm = lax.axis_index('dm')
    x, c = dm // 2, lax.rem(dm, 2)
    px = {'dp': 0, 'tp': y, 'dm': (1 - x) * 2 + c}
    pc = {'dp': 0, 'tp': y, 'dm': x * 2 + 1 - c}
    py = {'dp': 0, 'tp': 1 - y, 'dm': dm}
    pyc = {'dp': 0, 'tp': 1 - y, 'dm': x * 2 + 1 - c}

    def local(src, dst, sem):
        return pltpu.make_async_copy(src, dst, sem)

    def remote(src, dst, s_sem, r_sem, dev):
        return pltpu.make_async_remote_copy(src_ref=src, dst_ref=dst, send_sem=s_sem, recv_sem=r_sem, device_id=dev, device_id_type=pl.DeviceIdType.MESH)

    d_cp = [local(dd, d_ref.at[j * w4:(j + 1) * w4, :dd.shape[1]], d_sem.at[j]) for j, dd in enumerate((d0, d1, d2, d3))]
    cut = d0.shape[1]
    last = cut + e0.shape[1]
    e_cp = [local(dd, d_ref.at[j * w4:(j + 1) * w4, cut:last], d_sem.at[4 + j]) for j, dd in enumerate((e0, e1))]
    g_cp = local(part_of(g_ref, 0, w2), g_buf, d_sem.at[6])
    late = slice(last, d_ref.shape[1])
    dt_y = remote(dt.at[:, late], d_ref.at[:w4, late], dt_s.at[0], dt_r.at[0], py)
    dt_c = remote(d_ref.at[:w4, late], d_ref.at[w4:w2, late], dt_s.at[1], dt_r.at[1], pc)

    def z_cp(p):
        srcs = ((zwa, 0), (zb, 0), (zfa, 0), (zb, zwa.shape[0]))
        return [local(src.at[pl.ds(at + p * CH, CH), :], z_ref.at[p, i // 2 * CH:(i // 2 + 1) * CH, i % 2 * f8:(i % 2 + 1) * f8], z_sem.at[p, i]) for i, (src, at) in enumerate(srcs)]

    def p_cp(p):
        return local(part.at[p], p_ref.at[lax.rem(p, 3)], p_sem.at[lax.rem(p, 3)])

    per = hw0.shape[1] // CH
    h_cp = []
    for q in range(chunks):
        k, l = q // per, (q % per) * CH
        h_cp.append(local((hw0, hw1)[k].at[0:w2, l:l + CH], h_ref.at[q, :, 0:CH], h_sem.at[q, 0]))
        h_cp.append(local((hf0, hf1)[k].at[w2:2 * w2, l:l + CH], h_ref.at[q, :, CH:2 * CH], h_sem.at[q, 1]))

    def start(cps):
        for cp in cps:
            cp.start()

    start(z_cp(0) + [d_cp[2], p_cp(0), d_cp[3]])

    bar = pltpu.get_barrier_semaphore()
    for dev in (px, pc, py, pyc):
        pl.semaphore_signal(bar, inc=1, device_id=dev, device_id_type=pl.DeviceIdType.MESH)
    pl.semaphore_wait(bar, 4)
    dt_y.start()
    start(z_cp(1))

    def lanes(q):
        return pl.ds(pl.multiple_of(CH * (x + q - 2 * x * q), CH), CH)

    def away(q):
        return pl.ds(pl.multiple_of(CH - CH * (x + q - 2 * x * q), CH), CH)

    def rs(p, q):
        return remote(hi_ref.at[p, :, away(q)], rec_ref.at[p, :, away(q)], rs_s.at[p, q], rs_r.at[p, q], px)

    def sq(p, q):
        return remote(sqs_ref.at[p, q], sqr_ref.at[p, q], sq_s.at[p, q], sq_r.at[p, q], px)

    def outs(p, q):
        col = pl.multiple_of(((q * 2 + p // per) * 4 + 2 * y + c) * (per * CH) + lax.rem(p, per) * CH, CH)
        mine = rec_ref.at[p, :w4, lanes(q)]
        give = rec_ref.at[p, w4:, lanes(q)]
        dst = out.at[:, pl.ds(col, CH)]
        far = [remote(src, dst, out_s.at[p, q, i], out_r.at[p, q, i], dev) for i, (src, dev) in enumerate(((mine, py), (give, pyc), (give, pc)))]
        return far + [local(mine, dst, loc_sem.at[p, q])]

    def block(p, j):
        at = block_of(j, w4)
        return dot_nt(d_ref[at, :], z_ref[p]) + p_ref[lax.rem(p, 3), at, :]

    def upper(p):
        p_cp(p).wait()
        for cp in z_cp(p):
            cp.wait()

        @pl.when(p + 1 < chunks)
        def _():
            p_cp(p + 1).start()

        def half(i, _):
            t = block(p, 2 + i).astype(BF)
            at = block_of(i, w4)
            hi_ref[p, at, :CH] = t[:, CH:]
            hi_ref[p, at, CH:] = t[:, :CH]
            return 0

        loop(2, half)

    def lower(p):
        def half(j, _):
            lo_ref[p, block_of(j, w4), :] = block(p, j)
            return 0

        loop(2, half)

    def add(p, q):
        rs(p, q).wait_recv()
        at = lanes(q)
        t = (lo_ref[p, :, at] + rec_ref[p, :, at].astype(F32)).astype(BF)
        rec_ref[p, :, at] = t
        t = t.astype(F32)
        v = jnp.broadcast_to(jnp.sum(t * t, axis=0, keepdims=True), (8, CH))
        sqo_ref[q] = v
        sqs_ref[p, q] = v
        sq(p, q).start()

    def finish(p, q):
        sq(p, q).wait_recv()
        at = lanes(q)
        r = lax.rsqrt((sqo_ref[q] + sqr_ref[p, q]) / width + NORM_EPS)[0:1]
        rec_ref[p, :, at] = (h_ref[p, :, at].astype(F32) + rec_ref[p, :, at].astype(F32) * r * g_buf[:, 3:4]).astype(BF)
        start(outs(p, q))

    for cp in d_cp[2:]:
        cp.wait()

    def first_upper(p, _):
        upper(p)

        @pl.when(p == 0)
        def _():
            start([rs(0, 0), rs(0, 1)])

        return 0

    loop(2, first_upper)
    start(d_cp[:2] + e_cp + [g_cp] + h_cp)
    for q in range(2, chunks):
        start(z_cp(q))
    for cp in d_cp[:2] + e_cp:
        cp.wait()

    def early(i, _):
        p, at = i // 2, block_of(lax.rem(i, 2), w4)
        lo_ref[p, at, :] = dot_nt(d_ref[at, :last], z_ref[p, :, :last]) + p_ref[p, at, :]
        return 0

    loop(4, early)
    dt_y.wait_recv()
    dt_c.start()
    dt_c.wait_recv()

    def rest(i, _):
        p, at = i // 2, block_of(lax.rem(i, 2), w4)
        lo_ref[p, at, :] += dot_nt(d_ref[at, late], z_ref[p, :, late])
        return 0

    loop(4, rest)
    for cp in [g_cp] + h_cp:
        cp.wait()

    def body(p, _):
        for q in range(2):
            add(p, q)

            @pl.when(p + 1 < chunks)
            def _():
                rs(p + 1, q).start()

            if q:
                finish(p, 0)
            else:
                @pl.when(p > 0)
                def _():
                    finish(p - 1, 1)

            @pl.when(p + 2 < chunks)
            def _():
                (lower if q else upper)(p + 2)
        return 0

    loop(chunks, body)
    finish(chunks - 1, 1)

    def drain(p, _):
        for q in range(2):
            rs(p, q).wait_send()
            sq(p, q).wait_send()
            for cp in outs(p, q):
                cp.wait()
        return 0

    lax.fori_loop(0, chunks, drain, 0)
    dt_y.wait_send()
    dt_c.wait_send()


def kv_out_kernel(s_ref, kv0, kv1, *rest, extra):
    if extra:
        rest[-1][...] = rest[0][...]
    k_ref, v_ref = rest[-2 - extra:][:2]
    hd = k_ref.shape[2]
    first = s_ref[2] == 0
    a, b = kv0[...], kv1[...]
    two = jnp.where(first, a, b), jnp.where(first, b, a)
    for ref, at in ((k_ref, 0), (v_ref, hd)):
        ref[...] = hcat([t[:, at:at + hd] for t in two]).reshape(ref.shape)


def solution(mesh):
    tp_size, dm_size = mesh.shape['tp'], mesh.shape['dm']

    def flip(bits):
        return [(i, i ^ bits) for i in range(mesh.size)]

    C, X, Y = 1, 2, dm_size
    PX, PY, PC, PXC, PYC = flip(X), flip(Y), flip(C), flip(X | C), flip(Y | C)

    def send(a, perm):
        return lax.ppermute(a, ('tp', 'dm'), perm)

    def layer(tokens, positions, n1, wq, wk, wv, wo, n2, n3, wg, wu, wd, n4):
        y = lax.axis_index('tp')
        d = lax.axis_index('dm')
        x, c = d // 2, d % 2
        xo, yo, co = 1 - x, 1 - y, 1 - c
        rows, w4 = tokens.shape
        D = w4 * dm_size
        S = positions.shape[1]
        hd = wq.shape[2]
        scale = (D / (wq.shape[1] * tp_size)) ** -0.5
        gw = 2 * hd
        half = S // 2
        quarter = half // 4
        F4 = wg.shape[1] // 2
        scal = jnp.stack([x, y, c]).astype(jnp.int32)

        def take(a, start, size, axis=0):
            return lax.dynamic_slice_in_dim(a, start, size, axis)

        def take_cols(a, start, size):
            return take(a, start, size, 1)

        sets = range(2)
        dma = pltpu.SemaphoreType.DMA
        xt = tokens.T

        gains = jnp.stack([n1, n2, n3, n4])
        gall = hcat([gains, send(gains, PC), send(gains, PX), send(gains, PXC)])
        gcol = (1.0 + gall.astype(F32)).T

        oh = half // 2
        rx = [send(take_cols(xt, xo * S + k * half + y * oh, oh), PX) for k in sets]
        own_p = take_cols(xt, x * S, S)
        own_c = send(own_p, PC)
        ry = [send(rx[k], PY) for k in sets]
        rxc = [send(rx[k], PC) for k in sets]
        ryc = [send(ry[k], PC) for k in sets]

        wr = w4 // 9
        heads_of = lambda w: pl.BlockSpec((wr,) + w.shape[1:], lambda i, s: (i, 0, 0))
        wq_own, wq_oth = call(split_kernel, (9,), [heads_of(w) for w in (wq, wk, wv)], [pl.BlockSpec((wr, 2 * gw), by_row)] * 2, [bf(w4, 2 * gw)] * 2, flops=w4 * gw)(scal, wq, wk, wv)
        wqs = [wq_own, send(wq_oth, PC), send(wq_own, PX), send(wq_oth, PXC)]

        wot = jnp.transpose(wo, (0, 2, 1))
        B0 = wot
        B1 = send(B0, PX)
        B2 = send(B0, PY)
        B3 = send(B1, PY)
        Bs = []
        for b in (B0, B1, B2, B3):
            Bs += [b, send(b, PC)]

        def gather(own, oth, far=None):
            r1 = send(oth, PX)
            s0 = send(own if far is None else far, PY)
            s1 = send(r1, PY)
            ty = [own, send(own, PC), r1, send(r1, PC)]
            to = [s0, send(s0, PC), s1, send(s1, PC)]
            return ty, to

        F8 = F4 // 2

        def gu_half(xx, at):
            return hcat([take_cols(w, xx * F4 + at, F8) for w in (wg, wu)])

        gu = {ab: gather(gu_half(x, at), gu_half(xo, at)) for ab, at in (('a', 0), ('b', F8))}
        wdt = wd.T
        dw_own, dw_oth = (take_cols(wdt, xx * F4, F4) for xx in (x, xo))
        dw_a, dw_b = dw_own[:, :KA], dw_own[:, KA:F4 - KT]
        dn_y, dn_o = gather(dw_own, dw_oth, dw_a)
        dwb = send(dw_b, PY)
        dwb_c = send(dwb, PC)

        pos = take(positions, x, 1)[0]
        inv_freq = ROPE_BASE ** (-2.0 * jnp.arange(hd // 2, dtype=F32) / hd)
        pos_row, pos_col = pos.reshape(1, S), pos.reshape(S, 1)

        tile = 512
        nt = half // tile
        per_half = nt // 2
        nb = S // tile
        cos_t, sin_t = call(
            rope_kernel, (S // MT,), [pl.BlockSpec((1, MT), by_col), whole(hd // 2, 1)], [pl.BlockSpec((hd // 2, MT), by_col)] * 2,
            [f32(hd // 2, S)] * 2, flops=hd * S * nb)(scal, pos_row, inv_freq.reshape(hd // 2, 1))
        a_all = []
        for k in sets:
            a_all = [call(
                functools.partial(norm_kernel, width=D, per_half=half // 2 // MT), (half // MT,),
                [cols(w4, MT, lambda i, s, k=k: (s[0] * nb + k * nt) * per_half + i), cols(w4, MT, lambda i, s, k=k: k * nt * per_half + i)] + [cols(w4, MT, lambda i, s: i % nt)] * 4 + [whole(D, 4)] + [ANY] * k,
                cols(D, MT, lambda i, s, k=k: k * nt * per_half + i), bf(D, S),
                flops=D * S, aliases={8: 0} if k else None)(scal, xt, own_c, rx[k], rxc[k], ry[k], ryc[k], gcol, *a_all)]
        qv, kv = call(
            functools.partial(qkv_kernel, hd=hd), (nb,),
            [pl.BlockSpec((D, tile), by_col)] + [ANY] * 4 + [pl.BlockSpec((hd // 2, tile), by_col)] * 2,
            [pl.BlockSpec((gw + hd, tile), by_col), pl.BlockSpec((tile, gw), by_row)],
            [bf(gw + hd, S), bf(S, gw)],
            [vmem(2 * gw, D), vmem(D, 2 * gw), dma((4,))],
            flops=D * gw * S)(scal, *a_all, *wqs, cos_t, sin_t)

        bq = bk = tile
        bq2 = 2 * bq
        first_q, last_q = pos[0::bq][:, None], pos[bq - 1::bq][:, None]
        first_k, last_k = pos[0::bk][None, :], pos[bk - 1::bk][None, :]
        lo_t = jnp.sum((first_q - last_k >= WINDOW_LEN).astype(jnp.int32), axis=1)
        full_t = jnp.sum((last_q - first_k >= WINDOW_LEN).astype(jnp.int32), axis=1)
        h_own, m_own = [], []
        heads = wo.shape[0]
        qn = half // quarter
        mine = lambda i, s: 2 * s[1] + s[2]
        for k in sets:
            q0 = k * half // bq
            kl = (k + 1) * half
            o = call(
                functools.partial(attn_kernel, bq=bq, bk=bk, q_block0=q0, scale=scale), (half // bq,),
                [
                    cols(gw, bq, lambda i, *_, q0=q0: q0 + i), cols(kl, hd, fixed), pl.BlockSpec((hd, kl), lambda i, *_: (gw // hd, 0)),
                    cols(1, bq, lambda i, *_, q0=q0: q0 + i), cols(kl, 1, fixed),
                ],
                pl.BlockSpec((gw, bq), by_col),
                bf(gw, half),
                [vmem(hd, bq2, dtype=F32), vmem(hd, bq2), vmem(1, bq2, dtype=F32), vmem(hd, kl), vmem(8, CH, dtype=F32)],
                prefetch=2, flops=gw * half * kl)(lo_t, full_t, qv, kv, qv, pos_row, pos_col)
            mc = 2 * y + co
            my, myc = 2 * yo + c, 2 * yo + co
            o_c = send(take_cols(o, mc * quarter, quarter), PC)
            o_y = send(take_cols(o, my * quarter, quarter), PY)
            o_yc = send(take_cols(o, myc * quarter, quarter), PYC)
            h, m = call(
                functools.partial(proj_kernel, width=D), (1,),
                [cols(gw, quarter, mine)] + [whole(gw, quarter)] * 3 + [ANY] * 8 + [
                    cols(w4, quarter, lambda i, s, k=k: (2 * s[0] + k) * qn + mine(i, s)), cols(w4, quarter, lambda i, s, k=k: k * qn + mine(i, s)),
                    *[cols(w4, quarter, lambda i, s: s[2])] * 2,
                    whole(D, 4)] + [ANY] * k,
                [whole(D, quarter), pl.BlockSpec((quarter, D), lambda i, s, k=k: (k, 0))],
                [bf(D, quarter), bf(oh, D)],
                [vmem(4 * gw, quarter), vmem(D, quarter), vmem(len(Bs), heads, w4, hd), vmem(4, w4, quarter), vmem(4, w4, quarter, dtype=F32), dma((len(Bs),))],
                flops=D * gw * half, aliases={18: 1} if k else None)(scal, o, o_c, o_y, o_yc, *Bs, xt, own_c, rx[k], rxc[k], gcol, *m_own)
            h_own.append(h)
            m_own = [m]
        h_for = [send(h_own[k], PX) for k in sets]
        m_for = []
        for k in sets:
            m_for = [call(
                functools.partial(renorm_kernel, width=D), (1,), [whole(D, quarter), whole(D, 4)] + [ANY] * k,
                pl.BlockSpec((quarter, D), lambda i, s, k=k: (k, 0)), bf(oh, D), [vmem(D, quarter)],
                flops=D * half, aliases={3: 0} if k else None)(scal, h_for[k], gcol, *m_for)]

        def gated(ms, wsets, ft=128):
            nf = F8 // ft
            groups, sets = len(ms), len(wsets)
            early = lambda i: jnp.minimum(i, nf - 1)
            late = lambda i: jnp.maximum(i - nf, 0)
            specs = [cols(w4, ft, lambda j, i, s, at=at, up=up: up * nf + at(i)) for at in (early, late)[:sets] for up in range(2) for _ in wsets[0]]
            return call(
                functools.partial(gate_up_kernel, groups=groups, sets=sets, steps=nf), (groups, sets * nf),
                [whole(oh, D)] * groups + specs, pl.BlockSpec((oh, ft), lambda j, i, s: (j, i)),
                bf(oh * groups, sets * F8), flops=D * F4 * half * groups * sets)(scal, *ms, *[t for w in wsets for t in w + w])

        gua, gub = gu['a'], gu['b']
        near = [t[0] for t in (gua, gub)]
        zy_own = gated(m_own, near)
        zy_for = gated(m_for, near)
        za_own = gated(m_own, [gua[1]])
        za_for = gated(m_for, [gua[1]])
        zb = gated(m_own + m_for, [gub[1]], 3 * CH)
        w2 = 2 * w4
        chunks = oh // CH
        yt = 2 * CH
        part = call(
            down_y_kernel, (oh // yt,), [pl.BlockSpec((yt, F4), by_row)] * 2 + [ANY] * 4,
            pl.BlockSpec((2, D, yt), lambda i, s: (i, 0, 0)), f32(chunks, D, yt),
            [vmem(D, F4), dma((4,))], flops=D * F4 * half)(scal, zy_own, zy_for, *dn_y)
        out = pl.pallas_call(
            functools.partial(tail_kernel, width=D, chunks=chunks),
            out_shape=bf(w4, rows),
            in_specs=[ANY] * 16,
            out_specs=ANY,
            scratch_shapes=[
                vmem(D, F4), vmem(chunks, yt, F4), vmem(w2, 4, dtype=F32), vmem(3, D, yt, dtype=F32), vmem(chunks, w2, yt, dtype=F32),
                *[vmem(chunks, w2, yt)] * 3, *[vmem(chunks, 2, 8, CH, dtype=F32)] * 2, vmem(2, 8, CH, dtype=F32),
                dma((7,)), dma((chunks, 4)), dma((3,)), *[dma((chunks, 2))] * 6, *[dma((2,))] * 2, *[dma((chunks, 2, 3))] * 2],
            cost_estimate=pl.CostEstimate(flops=D * F4 * S, bytes_accessed=D * rows, transcendentals=0),
            compiler_params=pltpu.CompilerParams(vmem_limit_bytes=VM, collective_id=0, has_side_effects=True),
            name='tail',
        )(part, za_own, za_for, zb, *dn_o, dwb, dwb_c, dw_own, *h_own, *h_for, gcol)
        kv_c = send(kv, PC)
        most = nb - per_half
        kv_sets = jnp.split(kv, [most * tile // 2, most * tile])
        kv_x = [send(t, PX) for t in kv_sets]
        kv_xc = [send(t, PC) for t in kv_x]
        kv_outs = []
        for i, (t, tc, base, last) in enumerate(zip([kv] + kv_x, [kv_c] + kv_xc, (0, 0, most // 2, most), (nb, most // 2, most, nb))):
            extra = i == 3
            cut = 2 if i == 0 else 1
            kt = tile // cut
            n = cut * (last - base)
            kv_spec = pl.BlockSpec((kt, gw), by_row)
            at = lambda j, s, i=i, base=base, cut=cut: (((1 - s[0] if i else s[0]) * nb + base) * cut + j, 0, 0)
            cspec = [cols(w4, rows // n, lambda i, s: i)] * extra
            kv_outs = call(
                functools.partial(kv_out_kernel, extra=int(extra)), (n,), [kv_spec] * 2 + cspec + [ANY] * len(kv_outs),
                [pl.BlockSpec((kt, 2, hd), at)] * 2 + cspec, [bf(rows, 2, hd)] * 2 + [bf(w4, rows)] * extra,
                flops=rows * gw, aliases={3 + extra: 0, 4 + extra: 1} if i else None)(scal, t, tc, *[out] * extra, *kv_outs)
        k_out, v_out, out = kv_outs
        return out.T, k_out, v_out

    width_spec = P('dm')
    in_specs = (P('dp', 'dm'), P('dp', None), width_spec, P('dm', 'tp', None), P('dm', 'tp', None), P('dm', 'tp', None), P('tp', None, 'dm'), width_spec, width_spec, P('dm', 'tp'), P('dm', 'tp'), P('tp', 'dm'), width_spec)
    out_specs = (P('dp', 'dm'), P('dp', 'tp', None), P('dp', 'tp', None))
    return jax.shard_map(layer, mesh=mesh, in_specs=in_specs, out_specs=out_specs, check_vma=False)
```
